32 devices in a mesh: grp: 2 (over y), seq: 16 (over z, x, core).
Axes of the slice: x: 2, y: 2, z: 4, core: 2. Of those that a mesh axis runs over, the one named last changes fastest.
Arguments:
- frames: bfloat16 [4, 10240, 1280], P('grp', 'seq'), parts along dimension 0, may hold values from -120 to 120
- dec_states: bfloat16 [2, 256, 1280], P(None, 'grp'), parts along dimension 1, may hold values from -6 to 6
- w_query: bfloat16 [1280, 1280], P(None, 'seq'), may hold values from -0.15625 to 0.15625
- w_keyval: bfloat16 [1280, 2560], replicated, may hold values from -0.15625 to 0.15625
- w_output: bfloat16 [1280, 1280], P(None, 'seq'), may hold values from -0.15625 to 0.15625
- head_slope: float32 [20], replicated, may hold values from 0.3 to 12
- lengths: int32 [4, 16], P('grp'), parts along dimension 0, may hold values from 128 to 640, as said below
- positions: int32 [2, 256], P(None, 'grp'), parts along dimension 1, may hold values from 0 to 15
Outputs:
- attended: bfloat16 [2, 256, 1280], P(None, 'grp', 'seq'), parts along dimension 1
The draws below stay inside these ranges and needn't reach their ends.
There are 2 independent parts, one for each index of `grp`. The reference program is written for one: setup_inputs(seed, part) draws one part's arguments, and reference() takes and returns one part's arrays. A program takes and returns all parts, laid end to end along the dimension named above; an argument that names none is the same for every part. Nothing has to cross between parts.
Inputs may be any that keep to these rules, and one draw needn't show every extreme that they name: `lengths`: every step has one block of exactly 640 valid frames.
All inputs are finite; a program needn't handle non-finite values.
Results may differ from the reference program's by a relative error of at most 0.005.
The reference program's roundings to bfloat16 on the way count: a program that leaves them out, or rounds other values in their place, can miss the bound.
Values may be sent and summed in bfloat16 or wider, within the bound.
A program may use at most 128 MiB of HBM per device.

```python
import math
import jax
import jax.numpy as jnp
from jax import lax

D = 1280
H = 20
FR = 640
STEPS = 2
QROWS = 128
N_SEQ = 16


def draw_frames(key, part):
    key_base = jax.random.fold_in(key, 11)
    base = jax.random.normal(key_base, (STEPS, N_SEQ * FR, D), jnp.float32)
    base = jnp.clip(base, -6.0, 6.0)
    return base.astype(jnp.bfloat16)


def draw_lengths(key, part):
    key_pick = jax.random.fold_in(key, 21)
    key_long = jax.random.fold_in(key, 22)
    lowest = FR // 5
    spread = FR - lowest
    picked = jax.random.randint(key_pick, (STEPS, N_SEQ), 0, spread + 1)
    frame_counts = lowest + picked * picked // spread
    longest = jax.random.randint(key_long, (STEPS,), 0, N_SEQ)
    longest_at = jnp.arange(N_SEQ, dtype=jnp.int32)[None, :] == longest[:, None]
    return jnp.where(longest_at, FR, frame_counts).astype(jnp.int32)


def plant(values, own_key, smallest, high):
    spot = [jax.random.randint(jax.random.fold_in(own_key, axis), (), 0, length) for axis, length in enumerate(values.shape)]
    main_axis = values.shape.index(max(values.shape))
    neighbour = spot[:main_axis] + [(spot[main_axis] + 1) % values.shape[main_axis]] + spot[main_axis + 1:]
    return values.at[tuple(spot)].set(smallest).at[tuple(neighbour)].set(high)


def block_levels(own_key, extent, split, least, largest):
    level, own = 1.0, jax.random.fold_in(own_key, 6)
    for axis_at, shards_of in split:
        draws = jnp.exp(jax.random.uniform(jax.random.fold_in(own, axis_at), (shards_of,), jnp.float32, least / len(split), largest / len(split)))
        level = level * jnp.repeat(draws, extent[axis_at] // shards_of).reshape([-1 if axis == axis_at else 1 for axis in range(len(extent))])
    return level


def noise(rng, shape, scale, most, pieces=(), kind=jnp.bfloat16):
    result = jax.random.normal(rng, shape, jnp.float32) * scale
    if len(pieces) > 0:
        result = block_levels(rng, shape, pieces, -0.22, 0.18) * result
    return jnp.clip(result, min=-most, max=most).astype(kind)


def setup_inputs(seed: int = 0, part: int = 0) -> dict:
    splits = jax.random.split(jax.random.key(seed), 9)
    part_splits = jax.random.split(jax.random.fold_in(splits[8], part), 9)
    return {
        "frames": draw_frames(jax.random.fold_in(jax.random.fold_in(splits[8], part), 71), part),
        "dec_states": noise(part_splits[1], (STEPS, QROWS, D), 1.0, 6.0),
        "w_query": noise(splits[2], (D, D), D ** -0.5, 0.15625, ((1, 16),)),
        "w_keyval": noise(splits[3], (D, 2 * D), D ** -0.5, 0.15625),
        "w_output": noise(splits[4], (D, D), D ** -0.5, 0.15625, ((1, 16),)),
        "head_slope": jnp.clip(jnp.exp(jax.random.uniform(splits[5], (H,), jnp.float32, math.log(0.3), math.log(12.0))), 0.3, 12.0),
        "lengths": draw_lengths(jax.random.fold_in(jax.random.fold_in(splits[8], part), 71), part),
        "positions": plant(jax.random.randint(part_splits[7], (STEPS, QROWS), 0, N_SEQ), jax.random.fold_in(part_splits[7], 1), 0, N_SEQ - 1).astype(jnp.int32),
    }


def reference(frames, dec_states, w_query, w_keyval, w_output, head_slope, lengths, positions):
    step_count, total_frames, model_width = frames.shape
    query_rows = dec_states.shape[1]
    head_count = head_slope.shape[0]
    head_size = model_width // head_count
    block_count = N_SEQ
    frame_count = total_frames // block_count
    keyval = jnp.dot(frames.reshape(step_count * total_frames, model_width), w_keyval, preferred_element_type=jnp.float32).astype(jnp.bfloat16)
    all_keys = keyval[:, :model_width].reshape(step_count, block_count, frame_count, head_count, head_size)
    all_values = keyval[:, model_width:].reshape(step_count, block_count, frame_count, head_count, head_size)
    queries = jnp.dot(dec_states.reshape(step_count * query_rows, model_width), w_query, preferred_element_type=jnp.float32).astype(jnp.bfloat16)
    queries = queries.reshape(step_count, query_rows, head_count, head_size)
    results = []
    for step_now in range(step_count):
        query_now = queries[step_now].astype(jnp.float32)
        row_positions = positions[step_now].astype(jnp.float32)

        def one_block(flat_index):
            older_step = flat_index // block_count
            block_index = flat_index % block_count
            block_keys = all_keys[older_step, block_index].astype(jnp.float32)
            block_values = all_values[older_step, block_index].astype(jnp.float32)
            scores = jnp.einsum('qhd,jhd->hqj', query_now, block_keys) / math.sqrt(head_size)
            slot_place = ((block_index + 1) % block_count).astype(jnp.float32)
            age_steps = (step_now - older_step).astype(jnp.float32)
            distance = jnp.abs(row_positions - slot_place) / block_count + age_steps
            scores = scores - head_slope[:, None, None] * distance[None, :, None]
            length_now = lengths[older_step, block_index]
            valid = jnp.arange(frame_count, dtype=jnp.int32)[None, None, :] < length_now
            scores = jnp.where(valid, scores, -jnp.inf)
            row_peak = lax.optimization_barrier(jnp.max(scores, axis=2))
            weights = jnp.exp(scores - row_peak[:, :, None]).astype(jnp.bfloat16).astype(jnp.float32)
            row_total = lax.optimization_barrier(jnp.sum(weights, axis=2))
            row_context = jnp.einsum('hqj,jhd->hqd', weights, block_values)
            return (row_peak, row_total, row_context)
        peaks, totals, contexts = lax.map(one_block, jnp.arange((step_now + 1) * block_count, dtype=jnp.int32))
        row_top = lax.optimization_barrier(jnp.max(peaks, axis=0))
        factors = jnp.exp(peaks - row_top[None])
        row_total = lax.optimization_barrier(jnp.sum(factors * totals, axis=0))
        row_context = lax.optimization_barrier(jnp.sum(factors[..., None] * contexts, axis=0))
        context = (row_context / row_total[..., None]).transpose(1, 0, 2).reshape(query_rows, model_width)
        context = context.astype(jnp.bfloat16)
        results.append(jnp.dot(context, w_output, preferred_element_type=jnp.float32).astype(jnp.bfloat16))
    return jnp.stack(results)
```

```python
import functools
import math

import jax
import jax.numpy as jnp
from jax import lax
from jax.experimental import pallas as pl
from jax.experimental.pallas import tpu as pltpu
from jax.sharding import PartitionSpec as P

MESH = pl.DeviceIdType.MESH
EXTRA = 16
MASKED = -1e30


def rows_together(ref, first, count):
    parts = [ref[first + index].astype(jnp.float32) for index in range(count)]
    return jnp.concatenate(parts, axis=0)


def await_bytes(ref, count, sem):
    part = ref.at[pl.ds(0, count)]
    pltpu.make_async_copy(part, part, sem).wait()


def plain_kernel(
    n,
    dec_ref,
    wq_ref,
    wout_ref,
    pos_ref,
    slope_ref,
    len_ref,
    frames_hbm,
    wkv_hbm,
    out_ref,
    frames_ref,
    wkv_ref,
    k_ref,
    vt_ref,
    q_ref,
    ctx_ref,
    stat_ref,
    got_ctx,
    got_stat,
    pair_ctx,
    pair_stat,
    sum_ctx,
    sum_stat,
    fin_ref,
    frame_sem,
    weight_sem,
    send_sem,
    recv_sem,
    hop_sem,
    pair_sem,
):
    me = lax.axis_index("seq")
    steps, frame_count, width = frames_hbm.shape
    tokens = dec_ref.shape[0]
    per_step = tokens // steps
    heads = k_ref.shape[0]
    size = width // heads
    rows = wq_ref.shape[0]
    groups = math.gcd(heads, n)
    group_chunks = n // groups
    group_heads = heads // groups
    tile = frames_ref.shape[1]
    half = wkv_ref.shape[2]
    tiles = frames_ref.shape[0]
    per_block = frame_count // tile
    scale = 1.0 / math.sqrt(size)

    def frame_copy(index):
        return pltpu.make_async_copy(
            frames_hbm.at[index // per_block, pl.ds((index % per_block) * tile, tile)],
            frames_ref.at[index],
            frame_sem.at[index],
        )

    def weight_copy(index):
        return pltpu.make_async_copy(
            wkv_hbm.at[:, pl.ds(pl.multiple_of(index * half, half), half)], wkv_ref.at[index], weight_sem.at[index]
        )

    frame_copy(0).start()
    weight_copy(0).start()
    for index in range(1, tiles):
        frame_copy(index).start()
    for index in range(1, wkv_ref.shape[0]):
        weight_copy(index).start()

    barrier = pltpu.get_barrier_semaphore()

    @pl.loop(1, n)
    def _(step):
        peer = lax.rem(me + step, n)
        pl.semaphore_signal(barrier, inc=1, device_id={"seq": peer}, device_id_type=MESH)

    own_query = lax.dot_general(
        wq_ref[...], dec_ref[...], (((1,), (1,)), ((), ())), preferred_element_type=jnp.float32
    )
    q_ref[me] = own_query.astype(jnp.bfloat16)
    pl.semaphore_wait(barrier, n - 1)

    def send(src, dst, sem, peer):
        pltpu.make_async_remote_copy(
            src_ref=src,
            dst_ref=dst,
            send_sem=send_sem.at[sem],
            recv_sem=recv_sem.at[sem],
            device_id={"seq": peer},
            device_id_type=MESH,
        ).start()

    partner = me + 1 - 2 * lax.rem(me, 2)
    chips = n // 2

    def pass_on(ref, chunk, sem):
        send(ref.at[chunk], ref.at[chunk], sem, partner)

    def hop(ref, step, sem, level):
        return pltpu.make_async_remote_copy(
            src_ref=ref.at[me],
            dst_ref=ref.at[me],
            send_sem=send_sem.at[sem],
            recv_sem=hop_sem.at[level, step],
            device_id={"seq": lax.rem(me + 2 * step, n)},
            device_id_type=MESH,
        )

    def spread(ref, sem, level):
        @pl.loop(1, chips)
        def _(step):
            hop(ref, step, sem, level).start()

        pass_on(ref, me, level)

    def relay(ref, sem, level):
        @pl.loop(1, chips)
        def _(step):
            hop(ref, step, sem, level).wait_recv()
            pass_on(ref, lax.rem(me - 2 * step + n, n), level)

    def settle(ref, sem, level):
        await_bytes(ref, chips - 1, send_sem.at[sem])
        await_bytes(ref, chips, recv_sem.at[level])
        await_bytes(ref, chips, send_sem.at[level])

    spread(q_ref, 2, 0)

    column = lax.broadcasted_iota(jnp.int32, (frame_count, size + EXTRA), 1)
    place = lax.broadcasted_iota(jnp.int32, (frame_count, size + EXTRA), 0)
    masks = []
    for older in range(steps):
        hidden = (place >= len_ref[older, me]) & (column == size)
        masks.append(jnp.where(hidden, MASKED, 0.0).astype(jnp.bfloat16))
    mask = jnp.concatenate(masks, axis=0)
    ones = jnp.ones((EXTRA, steps * frame_count), jnp.bfloat16)

    @pl.loop(0, heads)
    def _(head):
        k_ref[head] = mask
        vt_ref[head, size:, :] = ones

    parts = wkv_ref.shape[0] // 2
    part_heads = half // size

    def project(part, index):
        at = pl.ds(pl.multiple_of(index * tile, tile), tile)
        keyval = jnp.dot(frames_ref[index], wkv_ref[part], preferred_element_type=jnp.float32)
        return at, keyval.astype(jnp.bfloat16)

    for index in range(tiles):
        frame_copy(index).wait()

    @pl.loop(0, parts)
    def _(part):
        weight_copy(part).wait()
        for index in range(tiles):
            at, keyval = project(part, index)
            for local_head in range(part_heads):
                lanes = slice(local_head * size, (local_head + 1) * size)
                k_ref[part * part_heads + local_head, at, 0:size] = keyval[:, lanes]

    def project_values(part):
        weight_copy(parts + part).wait()
        for index in range(tiles):
            at, keyval = project(parts + part, index)
            turned = keyval.T
            for local_head in range(part_heads):
                lanes = slice(local_head * size, (local_head + 1) * size)
                vt_ref[part * part_heads + local_head, 0:size, at] = turned[lanes]

    pl.loop(0, parts - 2)(project_values)
    relay(q_ref, 2, 0)
    pl.loop(parts - 2, parts)(project_values)
    settle(q_ref, 2, 0)

    slot_place = lax.rem(me + 1, n).astype(jnp.float32)
    distance = jnp.abs(pos_ref[...].astype(jnp.float32) - slot_place) / n
    first_row = lax.broadcasted_iota(jnp.int32, (EXTRA, tokens), 0) == 0
    query_tail = jnp.where(first_row, 1.0, 0.0).astype(jnp.bfloat16)
    token_step = lax.broadcasted_iota(jnp.int32, (1, tokens), 1) // per_step

    row = lax.broadcasted_iota(jnp.int32, (rows, tokens), 0)

    def pass_sums(turn):
        group = lax.rem(me // group_chunks + 1 + turn, groups)
        await_bytes(pair_stat, group_chunks // 2, pair_sem.at[0, turn])
        await_bytes(pair_ctx, group_chunks // 2, pair_sem.at[1, turn])

        @pl.loop(0, group_chunks // 2)
        def _(index):
            chunk = group * group_chunks + 2 * index + lax.rem(me, 2)
            slot = chunk // 2
            one, two = stat_ref[chunk], pair_stat[slot]
            top = jnp.maximum(one[0:2], two[0:2])
            one_factor = jnp.exp(one[0:2] - top)
            two_factor = jnp.exp(two[0:2] - top)
            stat = jnp.concatenate([top, one[2:4] * one_factor + two[2:4] * two_factor], axis=0)
            is_one = row + lax.rem(chunk * rows, size) < size
            context = ctx_ref[chunk].astype(jnp.float32) * jnp.where(
                is_one, one_factor[0:1], one_factor[1:2]
            ) + pair_ctx[slot].astype(jnp.float32) * jnp.where(
                is_one, two_factor[0:1], two_factor[1:2]
            )
            context = context.astype(jnp.bfloat16)

            @pl.when(chunk != me)
            def _():
                sum_stat[slot] = stat
                sum_ctx[slot] = context
                send(sum_stat.at[slot], got_stat.at[me // 2], 4, chunk)
                send(sum_ctx.at[slot], got_ctx.at[me // 2], 5, chunk)

            @pl.when(chunk == me)
            def _():
                got_stat[slot] = stat
                got_ctx[slot] = context

    @pl.loop(0, groups)
    def _(turn):
        group = lax.rem(me // group_chunks + 1 + turn, groups)
        query_rows = rows_together(q_ref, group * group_chunks, group_chunks).astype(jnp.bfloat16)
        peaks, totals, contexts = [], [], []

        def scores(local_head):
            query = jnp.concatenate(
                [query_rows[local_head * size : (local_head + 1) * size], query_tail], axis=0
            )
            return [
                jnp.dot(
                    k_ref[
                        group * group_heads + local_head,
                        pl.ds(older * frame_count, frame_count),
                        :,
                    ],
                    query[:, older * per_step :],
                    preferred_element_type=jnp.float32,
                )
                for older in range(steps)
            ]

        ready = scores(0)
        for local_head in range(group_heads):
            head = group * group_heads + local_head
            raws = ready
            if local_head + 1 < group_heads:
                ready = scores(local_head + 1)
            slope = slope_ref[head]
            peak = context = None
            for older in range(steps):
                first = older * per_step
                block = pl.ds(older * frame_count, frame_count)
                raw = raws[older]
                raw_peak = jnp.max(raw, axis=0, keepdims=True)
                weights = jnp.exp2((raw - raw_peak) * (scale * math.log2(math.e)))
                part_context = jnp.dot(
                    vt_ref[head, :, block],
                    weights.astype(jnp.bfloat16),
                    preferred_element_type=jnp.float32,
                )
                age = (token_step[:, first:] - older).astype(jnp.float32)
                part_peak = raw_peak * scale - slope * (distance[:, first:] + age)
                if peak is None:
                    peak, context = part_peak, part_context
                    continue
                top = jnp.maximum(peak[:, first:], part_peak)
                old_factor = jnp.exp(peak[:, first:] - top)
                new_factor = jnp.exp(part_peak - top)
                merged = context[:, first:] * old_factor + part_context * new_factor
                peak = jnp.concatenate([peak[:, :first], top], axis=1)
                context = jnp.concatenate([context[:, :first], merged], axis=1)
            peaks.append(peak)
            totals.append(context[size : size + 1])
            contexts.append(context[:size])
        stacked = jnp.concatenate(contexts, axis=0)
        for index in range(group_chunks):
            low, high = index * rows, (index + 1) * rows
            one, two = low // size, (high - 1) // size
            chunk = group * group_chunks + index
            ctx_ref[chunk] = stacked[low:high].astype(jnp.bfloat16)
            stat_ref[chunk] = jnp.concatenate(
                [peaks[one], peaks[two], totals[one], totals[two]], axis=0
            )

        @pl.loop(0, group_chunks // 2)
        def _(index):
            chunk = group * group_chunks + 2 * index + 1 - lax.rem(me, 2)
            for kind, (src, dst) in enumerate(((stat_ref, pair_stat), (ctx_ref, pair_ctx))):
                pltpu.make_async_remote_copy(
                    src_ref=src.at[chunk],
                    dst_ref=dst.at[chunk // 2],
                    send_sem=send_sem.at[kind],
                    recv_sem=pair_sem.at[kind, turn],
                    device_id={"seq": partner},
                    device_id_type=MESH,
                ).start()

        @pl.when(turn > 0)
        def _():
            pass_sums(turn - 1)

    pass_sums(groups - 1)
    await_bytes(got_stat, chips - 1, recv_sem.at[4])
    await_bytes(got_ctx, chips - 1, recv_sem.at[5])
    await_bytes(sum_stat, chips - 1, send_sem.at[4])
    await_bytes(sum_ctx, chips - 1, send_sem.at[5])
    await_bytes(stat_ref, chips, send_sem.at[0])
    await_bytes(ctx_ref, chips, send_sem.at[1])

    top = lax.fori_loop(
        1, chips, lambda at, best: jnp.maximum(best, got_stat[at][0:2]), got_stat[0][0:2]
    )
    is_one = row + lax.rem(me * rows, size) < size

    def add(at, state):
        total, acc = state
        stat = got_stat[at]
        factor = jnp.exp(stat[0:2] - top)
        spread = jnp.where(is_one, factor[0:1], factor[1:2])
        return total + stat[2:4] * factor, acc + got_ctx[at].astype(jnp.float32) * spread

    total, acc = lax.fori_loop(
        0,
        chips,
        add,
        (jnp.zeros((2, tokens), jnp.float32), jnp.zeros((rows, tokens), jnp.float32)),
    )
    fin_ref[me] = (acc / jnp.where(is_one, total[0:1], total[1:2])).astype(jnp.bfloat16)

    spread(fin_ref, 3, 1)
    relay(fin_ref, 3, 1)
    settle(fin_ref, 3, 1)
    context = rows_together(fin_ref, 0, n).astype(jnp.bfloat16)
    attended = jnp.dot(wout_ref[...], context, preferred_element_type=jnp.float32)
    attended = attended.astype(jnp.bfloat16)
    for step in range(steps):
        out_ref[step] = attended[:, step * per_step : (step + 1) * per_step]


def plain_local(n, frames, dec_states, w_query, w_keyval, w_output, head_slope, lengths, positions):
    steps, frame_count, width = frames.shape
    per_step = dec_states.shape[1]
    tokens = steps * per_step
    heads = head_slope.shape[0]
    size = width // heads
    rows = w_query.shape[1]
    keys = steps * frame_count
    tile = frame_count
    part = math.gcd(width, 256)
    vmem = pl.BlockSpec(memory_space=pltpu.VMEM)
    smem = pl.BlockSpec(memory_space=pltpu.SMEM)
    hbm = pl.BlockSpec(memory_space=pl.ANY)
    out = pl.pallas_call(
        functools.partial(plain_kernel, n),
        out_shape=jax.ShapeDtypeStruct((steps, rows, per_step), jnp.bfloat16),
        in_specs=[vmem, vmem, vmem, vmem, smem, smem, hbm, hbm],
        out_specs=vmem,
        scratch_shapes=[
            pltpu.VMEM((keys // tile, tile, width), jnp.bfloat16),
            pltpu.VMEM((2 * width // part, width, part), jnp.bfloat16),
            pltpu.VMEM((heads, keys, size + EXTRA), jnp.bfloat16),
            pltpu.VMEM((heads, size + EXTRA, keys), jnp.bfloat16),
            pltpu.VMEM((n, rows, tokens), jnp.bfloat16),
            pltpu.VMEM((n, rows, tokens), jnp.bfloat16),
            pltpu.VMEM((n, 4, tokens), jnp.float32),
            pltpu.VMEM((n // 2, rows, tokens), jnp.bfloat16),
            pltpu.VMEM((n // 2, 4, tokens), jnp.float32),
            pltpu.VMEM((n // 2, rows, tokens), jnp.bfloat16),
            pltpu.VMEM((n // 2, 4, tokens), jnp.float32),
            pltpu.VMEM((n // 2, rows, tokens), jnp.bfloat16),
            pltpu.VMEM((n // 2, 4, tokens), jnp.float32),
            pltpu.VMEM((n, rows, tokens), jnp.bfloat16),
            pltpu.SemaphoreType.DMA((keys // tile,)),
            pltpu.SemaphoreType.DMA((2 * width // part,)),
            pltpu.SemaphoreType.DMA((6,)),
            pltpu.SemaphoreType.DMA((6,)),
            pltpu.SemaphoreType.DMA((2, n // 2)),
            pltpu.SemaphoreType.DMA((2, math.gcd(heads, n))),
        ],
        compiler_params=pltpu.CompilerParams(
            collective_id=0, has_side_effects=True, vmem_limit_bytes=60 * 1024 * 1024
        ),
    )(
        dec_states.reshape(tokens, width),
        w_query.T,
        w_output.T,
        positions.reshape(1, tokens),
        head_slope,
        lengths,
        frames,
        w_keyval,
    )
    return out.transpose(0, 2, 1)


GROUPS = ((3, 2), (5, 2), (0, 2), (2, 1), (7, 1), (8, 1), (9, 1))
PLAN = (
    ("K1", "B0", "Q0", "V1", "K2", "V2", "Q1", "K3", "V3", "W0", "K0", "Y0", "A0", "V0", "M0", "A1", "W1", "K4")
    + ("M1", "S0", "Y1", "A2", "S1", "A3", "M2", "C0", "A4", "M3", "V4", "S2", "M4", "C1", "A5", "X0", "A6", "M5")
    + ("C3", "M6", "C4", "X1", "C2", "C5", "R0", "C6", "R3", "R1", "R4", "R2", "R5")
)
SUMS = ("near", "near", "near", "far", "far", "far", "far")
SHARES = ("column", "column", "relay", "relay", "relay", "relay", "direct")


def paired_kernel(
    n,
    pos_ref,
    slope_ref,
    len_ref,
    dec_hbm,
    wq_hbm,
    wout_hbm,
    frames_hbm,
    wkv_hbm,
    out_ref,
    dec_ref,
    wq_ref,
    wout_ref,
    frames_ref,
    wkv_ref,
    k_ref,
    mask_ref,
    vt_ref,
    q_ref,
    ctx_ref,
    stat_ref,
    pair_ctx,
    pair_stat,
    chip_ctx,
    chip_stat,
    got_ctx,
    got_stat,
    near_stat,
    side_stat,
    side_ctx,
    fin_ref,
    small_sem,
    frame_sem,
    weight_sem,
    send_sem,
    hop_sem,
    relay_sem,
    pair_sem,
    got_sem,
    near_sem,
    fin_sem,
    both_sem,
    side_sem,
):
    me = lax.axis_index("seq")
    core, chip = lax.rem(me, 2), me // 2
    partner = me + 1 - 2 * core
    chips = n // 2
    steps, frame_count, width = frames_hbm.shape
    tokens = dec_hbm.shape[0]
    per_step = tokens // steps
    pairs, lanes = vt_ref.shape[0], vt_ref.shape[1]
    size = lanes // 2
    rows = wq_hbm.shape[0]
    half = wkv_ref.shape[2]
    parts = wkv_ref.shape[0] // 2
    part_pairs = half // lanes
    scale = 1.0 / math.sqrt(size)
    groups = GROUPS
    side, level, levels = lax.rem(chip, 2), chip // 2, chips // 2

    small = [
        pltpu.make_async_copy(src, dst, small_sem.at[at])
        for at, (src, dst) in enumerate(((dec_hbm, dec_ref), (wq_hbm, wq_ref), (wout_hbm, wout_ref)))
    ]

    def frame_copy(index):
        return pltpu.make_async_copy(frames_hbm.at[index], frames_ref.at[index], frame_sem.at[index])

    def weight_copy(index):
        return pltpu.make_async_copy(
            wkv_hbm.at[:, pl.ds(pl.multiple_of(index * half, half), half)], wkv_ref.at[index], weight_sem.at[index]
        )

    small[1].start()
    small[0].start()
    weight_order = [int(stage[1:]) + parts * (stage[0] == "V") for stage in PLAN if stage[0] in "KV"]
    weight_copy(weight_order[0]).start(priority=1)
    for step in range(steps):
        frame_copy(step).start(priority=1)

    barrier = pltpu.get_barrier_semaphore()

    @pl.loop(1, n)
    def _(step):
        peer = lax.rem(me + step, n)
        pl.semaphore_signal(barrier, inc=1, device_id={"seq": peer}, device_id_type=MESH)

    def remote(src, dst, sent, got, peer):
        return pltpu.make_async_remote_copy(
            src_ref=src,
            dst_ref=dst,
            send_sem=sent,
            recv_sem=got,
            device_id={"seq": peer},
            device_id_type=MESH,
        )

    def await_copy(ref, sem):
        pltpu.make_async_copy(ref, ref, sem).wait()

    def query_rows(device):
        return q_ref.at[pl.ds(pl.multiple_of(device * rows, 16), rows)]

    def await_small():
        small[1].wait()
        small[0].wait()

    def project_query():
        own_query = lax.dot_general(
            wq_ref[...], dec_ref[...], (((1,), (1,)), ((), ())), preferred_element_type=jnp.float32
        )
        q_ref[pl.ds(pl.multiple_of(me * rows, 16), rows), :] = own_query.astype(jnp.bfloat16)

    def await_barrier(_):
        for index in weight_order[4:]:
            weight_copy(index).start(priority=1)
        small[2].start(priority=1)
        pl.semaphore_wait(barrier, n - 1)

    await_small()
    project_query()

    middle = chips // 4
    wave_chips = (
        list(range(middle, chips - middle)),
        list(range(middle)) + list(range(chips - middle, chips)),
    )
    is_middle = (chip >= middle) & (chip < chips - middle)

    def query_relay(device, wave):
        block = query_rows(device)
        remote(block, block, send_sem.at[1], relay_sem.at[wave], partner).start()

    def spread_queries(wave):
        @pl.when(is_middle if wave == 0 else jnp.logical_not(is_middle))
        def _():
            own = query_rows(me)

            @pl.loop(1, chips)
            def _(step):
                remote(own, own, send_sem.at[0], hop_sem.at[chip], lax.rem(me + 2 * step, n)).start()

            query_relay(me, wave)

    def relay_queries(wave):
        for source in wave_chips[wave]:

            @pl.when(source != chip)
            def _():
                await_copy(query_rows(me), hop_sem.at[source])
                query_relay(2 * source + core, wave)

    def await_queries(wave):
        await_copy(q_ref.at[pl.ds(0, rows * len(wave_chips[wave]))], relay_sem.at[wave])

    place = lax.broadcasted_iota(jnp.int32, (frame_count, lanes), 0)
    column = lax.broadcasted_iota(jnp.int32, (frame_count, lanes), 1)
    for older in range(steps):
        hidden = (place >= len_ref[older, me]) & (column == 0)
        mask_ref[older * frame_count : (older + 1) * frame_count, :] = jnp.where(hidden, MASKED, 0.0).astype(
            jnp.bfloat16
        )

    def project_keys(part):
        weight_copy(part).wait()
        for step in range(steps):
            at = slice(step * frame_count, (step + 1) * frame_count)
            keys = jnp.dot(frames_ref[step], wkv_ref[part], preferred_element_type=jnp.float32)
            keys = keys.astype(jnp.bfloat16)
            for index in range(part_pairs):
                k_ref[part * part_pairs + index, at, :] = keys[:, index * lanes : (index + 1) * lanes]

    def project_values(part):
        weight_copy(parts + part).wait()
        for step in range(steps):
            at = slice(step * frame_count, (step + 1) * frame_count)
            values = jnp.dot(frames_ref[step], wkv_ref[parts + part], preferred_element_type=jnp.float32)
            turned = values.astype(jnp.bfloat16).T
            for index in range(part_pairs):
                vt_ref[part * part_pairs + index, :, at] = turned[index * lanes : (index + 1) * lanes]

    def await_frames():
        for step in range(steps):
            frame_copy(step).wait()

    for index in weight_order[1:4]:
        weight_copy(index).start(priority=1)
    await_frames()

    slot_place = lax.rem(me + 1, n).astype(jnp.float32)
    distance = jnp.abs(pos_ref[...].astype(jnp.float32) - slot_place) / n
    tail_row = lax.broadcasted_iota(jnp.int32, (lanes, tokens), 0) == 0
    tail = jnp.where(tail_row, 1.0, 0.0).astype(jnp.bfloat16)
    blank = jnp.zeros((size, tokens), jnp.bfloat16)
    ones = jnp.ones((EXTRA, frame_count), jnp.bfloat16)
    first, second = slice(0, frame_count), slice(frame_count, 2 * frame_count)
    early, late = slice(0, per_step), slice(per_step, tokens)

    def attend_scores(pair):
        query = q_ref[pl.ds(pl.multiple_of(pair * lanes, lanes), lanes), :]
        one = jnp.concatenate([query[:size], blank, tail], axis=0)
        two = jnp.concatenate([blank, query[size:], tail], axis=0)
        both = jnp.concatenate([one[:, late], two[:, late]], axis=1)
        old = jnp.concatenate([k_ref[pair, first, :], mask_ref[first, :]], axis=1)
        new = jnp.concatenate([k_ref[pair, second, :], mask_ref[second, :]], axis=1)
        return [
            functools.partial(jnp.dot, keys, queries, preferred_element_type=jnp.float32)
            for keys, queries in ((old, one), (old, two), (new, both))
        ]

    def soften(raw):
        peak = jnp.max(raw, axis=0, keepdims=True)
        weights = jnp.exp2((raw - peak) * (scale * math.log2(math.e)))
        return peak * scale, weights.astype(jnp.bfloat16)

    def attend_values(pair, kind):
        if kind == 2:
            stack = [vt_ref[pair, :, second], ones]
        else:
            stack = [vt_ref[pair, kind * size : (kind + 1) * size, first], ones]
        return jnp.concatenate(stack, axis=0)

    def attend(group):
        first_pair, count = groups[group]
        dots = []
        for local_pair in range(count):
            dots += [(local_pair, kind, call) for kind, call in enumerate(attend_scores(first_pair + local_pair))]
        results = {}
        ready = [dots[0][2](), dots[1][2]()]
        for at, (local_pair, kind, _) in enumerate(dots):
            raw = ready.pop(0)
            if at + 2 < len(dots):
                ready.append(dots[at + 2][2]())
            peak, weights = soften(raw)
            values = attend_values(first_pair + local_pair, kind)
            results[local_pair, kind] = peak, jnp.dot(values, weights, preferred_element_type=jnp.float32)
        peaks = [[], []]
        totals = [[], []]
        for local_pair in range(count):
            pair = first_pair + local_pair
            new_peaks, new_context = results[local_pair, 2]
            for which in range(2):
                slope = slope_ref[2 * pair + which]
                at = pl.ds(pl.multiple_of(pair * lanes + which * size, size), size)
                peak, context = results[local_pair, which]
                peaks[0].append(peak[:, early] - slope * distance[:, early])
                totals[0].append(context[size : size + 1, early])
                ctx_ref[0, at, :] = context[:size, early].astype(jnp.bfloat16)
                span = slice(which * per_step, (which + 1) * per_step)
                old_peak = peak[:, late] - slope * (distance[:, late] + 1.0)
                new_peak = new_peaks[:, span] - slope * distance[:, late]
                top = jnp.maximum(old_peak, new_peak)
                old_factor, new_factor = jnp.exp(old_peak - top), jnp.exp(new_peak - top)
                own = slice(which * size, (which + 1) * size)
                merged = context[:size, late] * old_factor + new_context[own, span] * new_factor
                ctx_ref[1, at, :] = merged.astype(jnp.bfloat16)
                peaks[1].append(top)
                old_total = context[size : size + 1, late] * old_factor
                totals[1].append(old_total + new_context[lanes : lanes + 1, span] * new_factor)
        for step in range(2):
            stat_ref[step, group, 0 : 4 * count, :] = jnp.concatenate(peaks[step] + totals[step], axis=0)
        block = pl.ds(pl.multiple_of(first_pair * lanes, lanes), count * lanes)
        other = 1 - core
        remote(
            stat_ref.at[other, group], pair_stat.at[group], send_sem.at[2], pair_sem.at[0, group], partner
        ).start()
        remote(
            ctx_ref.at[other, block], pair_ctx.at[block], send_sem.at[3], pair_sem.at[1, group], partner
        ).start()

    def slices(first_pair, count):
        part_rows = count * lanes // chips
        base = first_pair * lanes

        def block(owner):
            place = lax.rem(owner, 2) * (chips // 2) + owner // 2
            return pl.ds(pl.multiple_of(base + place * part_rows, 16), part_rows)

        slot = pl.ds(pl.multiple_of(base // chips, 16), part_rows)
        return part_rows, block, slot

    def mix(one, two, heads):
        top = jnp.maximum(one[:heads], two[:heads])
        one_factor, two_factor = jnp.exp(one[:heads] - top), jnp.exp(two[:heads] - top)
        total = one[heads : 2 * heads] * one_factor + two[heads : 2 * heads] * two_factor
        return top, total, one_factor, two_factor

    def merge_cores(group):
        first_pair, count = groups[group]
        part_rows, block, slot = slices(first_pair, count)
        heads = 2 * count
        await_copy(pair_stat.at[group], pair_sem.at[0, group])
        await_copy(pair_ctx.at[pl.ds(0, count * lanes)], pair_sem.at[1, group])
        top, total, one_factor, two_factor = mix(stat_ref[core, group], pair_stat[group], heads)
        for head in range(heads):
            at = slice(first_pair * lanes + head * size, first_pair * lanes + (head + 1) * size)
            merged = (
                ctx_ref[core, at, :].astype(jnp.float32) * one_factor[head : head + 1]
                + pair_ctx[at, :].astype(jnp.float32) * two_factor[head : head + 1]
            )
            chip_ctx[at, :] = merged.astype(jnp.bfloat16)
        if SUMS[group] == "near":
            near_stat[group] = jnp.concatenate([top, total], axis=0)
            block = side_rows(group, 1 - side)
            peer = me + 2 - 4 * side
            remote(
                near_stat.at[group], side_stat.at[group], send_sem.at[12], near_sem.at[0, group], peer
            ).start()
            remote(
                chip_ctx.at[block], side_ctx.at[block], send_sem.at[11], near_sem.at[1, group], peer
            ).start()
            return
        for owner in range(chips):
            head = (owner % 2 * levels + owner // 2) * part_rows // size
            chip_stat[group, owner] = jnp.concatenate([top[head : head + 1], total[head : head + 1]], axis=0)

        @pl.loop(1, chips)
        def _(step):
            owner = lax.rem(chip + step, chips)
            peer = 2 * owner + core
            remote(
                chip_stat.at[group, owner], got_stat.at[group, chip], send_sem.at[4], got_sem.at[0, group], peer
            ).start()
            remote(
                chip_ctx.at[block(owner)], got_ctx.at[chip, slot], send_sem.at[5], got_sem.at[1, group], peer
            ).start()

        got_stat[group, chip] = chip_stat[group, chip]
        got_ctx[chip, slot, :] = chip_ctx[block(chip), :]

    def side_rows(group, which):
        first_pair, count = groups[group]
        span = count * lanes // 2
        return pl.ds(pl.multiple_of(first_pair * lanes + which * span, 16), span)

    def merge_sides(group):
        first_pair, count = groups[group]
        part_rows, block, slot = slices(first_pair, count)
        await_copy(side_stat.at[group], near_sem.at[0, group])
        await_copy(side_ctx.at[pl.ds(0, count * lanes // 2)], near_sem.at[1, group])
        stats = mix(near_stat[group], side_stat[group], 2 * count)
        top, total, one_factor, two_factor = (
            jnp.where(side == 0, stat[:count], stat[count:]) for stat in stats
        )
        base = first_pair * lanes + side * (count * lanes // 2)
        for head in range(count):
            at = pl.ds(pl.multiple_of(base + head * size, size), size)
            merged = (
                chip_ctx[at, :].astype(jnp.float32) * one_factor[head : head + 1]
                + side_ctx[at, :].astype(jnp.float32) * two_factor[head : head + 1]
            )
            chip_ctx[at, :] = merged.astype(jnp.bfloat16)
        for owner in range(levels):
            head = owner * part_rows // size
            chip_stat[group, owner] = jnp.concatenate([top[head : head + 1], total[head : head + 1]], axis=0)

        @pl.loop(1, levels)
        def _(step):
            owner = lax.rem(level + step, levels)
            peer = lax.rem(me + 4 * step, n)
            remote(
                chip_stat.at[group, owner], got_stat.at[group, level], send_sem.at[13], got_sem.at[0, group], peer
            ).start()
            remote(
                chip_ctx.at[block(2 * owner + side)],
                got_ctx.at[level, slot],
                send_sem.at[10],
                got_sem.at[1, group],
                peer,
            ).start()

        got_stat[group, level] = chip_stat[group, level]
        got_ctx[level, slot, :] = chip_ctx[block(chip), :]

    def merge_chips(group):
        first_pair, count = groups[group]
        mode = SHARES[group]
        sources = levels if SUMS[group] == "near" else chips
        part_rows, block, slot = slices(first_pair, count)
        await_copy(got_stat.at[group, pl.ds(0, sources - 1)], got_sem.at[0, group])
        await_copy(got_ctx.at[pl.ds(0, sources - 1), pl.ds(0, part_rows)], got_sem.at[1, group])
        stats = [got_stat[group, source] for source in range(sources)]
        top = stats[0][0:1]
        for stat in stats[1:]:
            top = jnp.maximum(top, stat[0:1])
        total = context = None
        for source, stat in enumerate(stats):
            factor = jnp.exp(stat[0:1] - top)
            part_total = stat[1:2] * factor
            part_context = got_ctx[source, slot, :].astype(jnp.float32) * factor
            total = part_total if total is None else total + part_total
            context = part_context if context is None else context + part_context
        fin_ref[core, block(chip), :] = (context / total).astype(jnp.bfloat16)
        own = fin_ref.at[core, block(chip)]
        if mode == "direct":

            @pl.loop(1, n)
            def _(step):
                remote(own, own, send_sem.at[7], fin_sem.at[group], lax.rem(me + step, n)).start()

        else:
            stride = 4 if mode == "column" else 2

            @pl.loop(1, n // stride)
            def _(step):
                remote(
                    own, own, send_sem.at[6], fin_sem.at[group], lax.rem(me + stride * step, n)
                ).start()

    def group_rows(group):
        first_pair, count = groups[group]
        return slice(first_pair * lanes, (first_pair + count) * lanes)

    def await_slices(group, amount):
        await_copy(fin_ref.at[0, pl.ds(0, amount * groups[group][1] * lanes // chips)], fin_sem.at[group])

    def cross(group):
        await_slices(group, levels - 1)
        block = fin_ref.at[core, side_rows(group, side)]
        remote(block, block, send_sem.at[9], side_sem.at[group], me + 2 - 4 * side).start()

    def relay(group):
        if SHARES[group] == "column":
            await_copy(fin_ref.at[0, pl.ds(0, groups[group][1] * lanes // 2)], side_sem.at[group])
        else:
            await_slices(group, chips - 1)
        block = fin_ref.at[core, group_rows(group)]
        remote(block, block, send_sem.at[8], both_sem.at[group], partner).start()

    stages = {
        "K": project_keys,
        "V": project_values,
        "B": await_barrier,
        "Q": spread_queries,
        "W": relay_queries,
        "Y": await_queries,
        "A": attend,
        "M": merge_cores,
        "S": merge_sides,
        "C": merge_chips,
        "X": cross,
        "R": relay,
    }
    for stage in PLAN:
        stages[stage[0]](int(stage[1:]))

    def await_both(group):
        await_copy(fin_ref.at[0, group_rows(group)], both_sem.at[group])

    small[2].wait()
    direct = [group for group, mode in enumerate(SHARES) if mode == "direct"]
    for group in range(direct[0]):
        await_both(group)

    def attended(begin, stop):
        context = jnp.concatenate([fin_ref[0, begin:stop, :], fin_ref[1, begin:stop, :]], axis=1)
        return jnp.dot(wout_ref[:, begin:stop], context, preferred_element_type=jnp.float32)

    late_row = groups[direct[0]][0] * lanes
    total = attended(0, late_row)
    for group in direct:
        await_slices(group, n - 1)
    total = total + attended(late_row, width)
    total = total.astype(jnp.bfloat16)
    for step in range(steps):
        out_ref[step] = total[:, step * per_step : (step + 1) * per_step]

    def sent(amount, sem):
        await_copy(fin_ref.at[0, pl.ds(0, amount)], send_sem.at[sem])

    share_rows = {mode: 0 for mode in SHARES}
    sum_rows = {mode: 0 for mode in SUMS}
    sum_count = {mode: 0 for mode in SUMS}
    for (_, count), shared, summed in zip(groups, SHARES, SUMS):
        share_rows[shared] += count * lanes // chips
        sum_rows[summed] += count * lanes // chips
        sum_count[summed] += 1
    await_copy(q_ref.at[pl.ds(0, rows * (chips - 1))], send_sem.at[0])
    await_copy(q_ref.at[pl.ds(0, rows * chips)], send_sem.at[1])
    await_copy(stat_ref.at[0], send_sem.at[2])
    await_copy(ctx_ref.at[0], send_sem.at[3])
    await_copy(got_stat.at[pl.ds(0, sum_count["far"]), pl.ds(0, chips - 1)], send_sem.at[4])
    sent((chips - 1) * sum_rows["far"], 5)
    sent((levels - 1) * share_rows["column"] + (chips - 1) * share_rows["relay"], 6)
    sent((n - 1) * share_rows["direct"], 7)
    sent(late_row, 8)
    sent(levels * share_rows["column"], 9)
    sent((levels - 1) * sum_rows["near"], 10)
    sent(levels * sum_rows["near"], 11)
    await_copy(side_stat.at[pl.ds(0, sum_count["near"])], send_sem.at[12])
    await_copy(got_stat.at[pl.ds(0, sum_count["near"]), pl.ds(0, levels - 1)], send_sem.at[13])


def paired_local(n, frames, dec_states, w_query, w_keyval, w_output, head_slope, lengths, positions):
    steps, frame_count, width = frames.shape
    per_step = dec_states.shape[1]
    tokens = steps * per_step
    heads = head_slope.shape[0]
    lanes = 2 * (width // heads)
    pairs = heads // 2
    rows = w_query.shape[1]
    keys = steps * frame_count
    part = 2 * lanes
    chips = n // 2
    groups = len(GROUPS)
    vmem = pl.BlockSpec(memory_space=pltpu.VMEM)
    smem = pl.BlockSpec(memory_space=pltpu.SMEM)
    hbm = pl.BlockSpec(memory_space=pl.ANY)
    out = pl.pallas_call(
        functools.partial(paired_kernel, n),
        out_shape=jax.ShapeDtypeStruct((steps, rows, per_step), jnp.bfloat16),
        in_specs=[vmem, smem, smem, hbm, hbm, hbm, hbm, hbm],
        out_specs=vmem,
        scratch_shapes=[
            pltpu.VMEM((tokens, width), jnp.bfloat16),
            pltpu.VMEM((rows, width), jnp.bfloat16),
            pltpu.VMEM((rows, width), jnp.bfloat16),
            pltpu.VMEM((steps, frame_count, width), jnp.bfloat16),
            pltpu.VMEM((2 * width // part, width, part), jnp.bfloat16),
            pltpu.VMEM((pairs, keys, lanes), jnp.bfloat16),
            pltpu.VMEM((keys, lanes), jnp.bfloat16),
            pltpu.VMEM((pairs, lanes, keys), jnp.bfloat16),
            pltpu.VMEM((width, tokens), jnp.bfloat16),
            pltpu.VMEM((2, width, per_step), jnp.bfloat16),
            pltpu.VMEM((2, groups, 8, per_step), jnp.float32),
            pltpu.VMEM((width, per_step), jnp.bfloat16),
            pltpu.VMEM((groups, 8, per_step), jnp.float32),
            pltpu.VMEM((width, per_step), jnp.bfloat16),
            pltpu.VMEM((groups, chips, 2, per_step), jnp.float32),
            pltpu.VMEM((chips, width // chips, per_step), jnp.bfloat16),
            pltpu.VMEM((groups, chips, 2, per_step), jnp.float32),
            pltpu.VMEM((groups, 8, per_step), jnp.float32),
            pltpu.VMEM((groups, 8, per_step), jnp.float32),
            pltpu.VMEM((width, per_step), jnp.bfloat16),
            pltpu.VMEM((2, width, per_step), jnp.bfloat16),
            pltpu.SemaphoreType.DMA((3,)),
            pltpu.SemaphoreType.DMA((steps,)),
            pltpu.SemaphoreType.DMA((2 * width // part,)),
            pltpu.SemaphoreType.DMA((14,)),
            pltpu.SemaphoreType.DMA((chips,)),
            pltpu.SemaphoreType.DMA((2,)),
            pltpu.SemaphoreType.DMA((2, groups)),
            pltpu.SemaphoreType.DMA((2, groups)),
            pltpu.SemaphoreType.DMA((2, groups)),
            pltpu.SemaphoreType.DMA((groups,)),
            pltpu.SemaphoreType.DMA((groups,)),
            pltpu.SemaphoreType.DMA((groups,)),
        ],
        compiler_params=pltpu.CompilerParams(
            collective_id=0, has_side_effects=True, vmem_limit_bytes=60 * 1024 * 1024
        ),
    )(
        positions.reshape(1, tokens),
        head_slope,
        lengths,
        dec_states.reshape(tokens, width),
        w_query.T,
        w_output.T,
        frames,
        w_keyval,
    )
    return out.transpose(0, 2, 1)


def fits_pairs(n, frames, dec_states, w_query, head_slope):
    steps, frame_count, width = frames.shape
    per_step, heads = dec_states.shape[1], head_slope.shape[0]
    size = width // heads
    chips = n // 2
    return (
        steps == 2
        and n % 4 == 0
        and heads % 4 == 0
        and heads // 2 == sum(count for _, count in GROUPS)
        and n % 8 == 0
        and size == 64
        and per_step == 2 * size
        and frame_count % 128 == 0
        and w_query.shape[1] % 16 == 0
        and (2 * size) % (16 * chips) == 0
    )


def local(n, frames, dec_states, w_query, w_keyval, w_output, head_slope, lengths, positions):
    paired = fits_pairs(n, frames, dec_states, w_query, head_slope)
    run = paired_local if paired else plain_local
    return run(n, frames, dec_states, w_query, w_keyval, w_output, head_slope, lengths, positions)


def solution(mesh):
    return jax.shard_map(
        functools.partial(local, mesh.shape["seq"]),
        mesh=mesh,
        in_specs=(
            P("grp", "seq", None),
            P(None, "grp", None),
            P(None, "seq"),
            P(),
            P(None, "seq"),
            P(),
            P("grp", None),
            P(None, "grp"),
        ),
        out_specs=P(None, "grp", "seq"),
        check_vma=False,
    )
```

```python
import functools
import math

import jax
import jax.numpy as jnp
from jax import lax
from jax.experimental import pallas as pl
from jax.experimental.pallas import tpu as pltpu
from jax.sharding import PartitionSpec as P

MESH = pl.DeviceIdType.MESH
EXTRA = 16
MASKED = -1e30


def rows_together(ref, first, count):
    parts = [ref[first + index].astype(jnp.float32) for index in range(count)]
    return jnp.concatenate(parts, axis=0)


def await_bytes(ref, count, sem):
    part = ref.at[pl.ds(0, count)]
    pltpu.make_async_copy(part, part, sem).wait()


def plain_kernel(
    n,
    dec_ref,
    wq_ref,
    wout_ref,
    pos_ref,
    slope_ref,
    len_ref,
    frames_hbm,
    wkv_hbm,
    out_ref,
    frames_ref,
    wkv_ref,
    k_ref,
    vt_ref,
    q_ref,
    ctx_ref,
    stat_ref,
    got_ctx,
    got_stat,
    pair_ctx,
    pair_stat,
    sum_ctx,
    sum_stat,
    fin_ref,
    frame_sem,
    weight_sem,
    send_sem,
    recv_sem,
    hop_sem,
    pair_sem,
):
    me = lax.axis_index("seq")
    steps, frame_count, width = frames_hbm.shape
    tokens = dec_ref.shape[0]
    per_step = tokens // steps
    heads = k_ref.shape[0]
    size = width // heads
    rows = wq_ref.shape[0]
    groups = math.gcd(heads, n)
    group_chunks = n // groups
    group_heads = heads // groups
    tile = frames_ref.shape[1]
    half = wkv_ref.shape[2]
    tiles = frames_ref.shape[0]
    per_block = frame_count // tile
    scale = 1.0 / math.sqrt(size)

    def frame_copy(index):
        return pltpu.make_async_copy(
            frames_hbm.at[index // per_block, pl.ds((index % per_block) * tile, tile)],
            frames_ref.at[index],
            frame_sem.at[index],
        )

    def weight_copy(index):
        return pltpu.make_async_copy(
            wkv_hbm.at[:, pl.ds(pl.multiple_of(index * half, half), half)], wkv_ref.at[index], weight_sem.at[index]
        )

    frame_copy(0).start()
    weight_copy(0).start()
    for index in range(1, tiles):
        frame_copy(index).start()
    for index in range(1, wkv_ref.shape[0]):
        weight_copy(index).start()

    barrier = pltpu.get_barrier_semaphore()

    @pl.loop(1, n)
    def _(step):
        peer = lax.rem(me + step, n)
        pl.semaphore_signal(barrier, inc=1, device_id={"seq": peer}, device_id_type=MESH)

    own_query = lax.dot_general(
        wq_ref[...], dec_ref[...], (((1,), (1,)), ((), ())), preferred_element_type=jnp.float32
    )
    q_ref[me] = own_query.astype(jnp.bfloat16)
    pl.semaphore_wait(barrier, n - 1)

    def send(src, dst, sem, peer):
        pltpu.make_async_remote_copy(
            src_ref=src,
            dst_ref=dst,
            send_sem=send_sem.at[sem],
            recv_sem=recv_sem.at[sem],
            device_id={"seq": peer},
            device_id_type=MESH,
        ).start()

    partner = me + 1 - 2 * lax.rem(me, 2)
    chips = n // 2

    def pass_on(ref, chunk, sem):
        send(ref.at[chunk], ref.at[chunk], sem, partner)

    def hop(ref, step, sem, level):
        return pltpu.make_async_remote_copy(
            src_ref=ref.at[me],
            dst_ref=ref.at[me],
            send_sem=send_sem.at[sem],
            recv_sem=hop_sem.at[level, step],
            device_id={"seq": lax.rem(me + 2 * step, n)},
            device_id_type=MESH,
        )

    def spread(ref, sem, level):
        @pl.loop(1, chips)
        def _(step):
            hop(ref, step, sem, level).start()

        pass_on(ref, me, level)

    def relay(ref, sem, level):
        @pl.loop(1, chips)
        def _(step):
            hop(ref, step, sem, level).wait_recv()
            pass_on(ref, lax.rem(me - 2 * step + n, n), level)

    def settle(ref, sem, level):
        await_bytes(ref, chips - 1, send_sem.at[sem])
        await_bytes(ref, chips, recv_sem.at[level])
        await_bytes(ref, chips, send_sem.at[level])

    spread(q_ref, 2, 0)

    column = lax.broadcasted_iota(jnp.int32, (frame_count, size + EXTRA), 1)
    place = lax.broadcasted_iota(jnp.int32, (frame_count, size + EXTRA), 0)
    masks = []
    for older in range(steps):
        hidden = (place >= len_ref[older, me]) & (column == size)
        masks.append(jnp.where(hidden, MASKED, 0.0).astype(jnp.bfloat16))
    mask = jnp.concatenate(masks, axis=0)
    ones = jnp.ones((EXTRA, steps * frame_count), jnp.bfloat16)

    @pl.loop(0, heads)
    def _(head):
        k_ref[head] = mask
        vt_ref[head, size:, :] = ones

    parts = wkv_ref.shape[0] // 2
    part_heads = half // size

    def project(part, index):
        at = pl.ds(pl.multiple_of(index * tile, tile), tile)
        keyval = jnp.dot(frames_ref[index], wkv_ref[part], preferred_element_type=jnp.float32)
        return at, keyval.astype(jnp.bfloat16)

    for index in range(tiles):
        frame_copy(index).wait()

    @pl.loop(0, parts)
    def _(part):
        weight_copy(part).wait()
        for index in range(tiles):
            at, keyval = project(part, index)
            for local_head in range(part_heads):
                lanes = slice(local_head * size, (local_head + 1) * size)
                k_ref[part * part_heads + local_head, at, 0:size] = keyval[:, lanes]

    def project_values(part):
        weight_copy(parts + part).wait()
        for index in range(tiles):
            at, keyval = project(parts + part, index)
            turned = keyval.T
            for local_head in range(part_heads):
                lanes = slice(local_head * size, (local_head + 1) * size)
                vt_ref[part * part_heads + local_head, 0:size, at] = turned[lanes]

    pl.loop(0, parts - 2)(project_values)
    relay(q_ref, 2, 0)
    pl.loop(parts - 2, parts)(project_values)
    settle(q_ref, 2, 0)

    slot_place = lax.rem(me + 1, n).astype(jnp.float32)
    distance = jnp.abs(pos_ref[...].astype(jnp.float32) - slot_place) / n
    first_row = lax.broadcasted_iota(jnp.int32, (EXTRA, tokens), 0) == 0
    query_tail = jnp.where(first_row, 1.0, 0.0).astype(jnp.bfloat16)
    token_step = lax.broadcasted_iota(jnp.int32, (1, tokens), 1) // per_step

    row = lax.broadcasted_iota(jnp.int32, (rows, tokens), 0)

    def pass_sums(turn):
        group = lax.rem(me // group_chunks + 1 + turn, groups)
        await_bytes(pair_stat, group_chunks // 2, pair_sem.at[0, turn])
        await_bytes(pair_ctx, group_chunks // 2, pair_sem.at[1, turn])

        @pl.loop(0, group_chunks // 2)
        def _(index):
            chunk = group * group_chunks + 2 * index + lax.rem(me, 2)
            slot = chunk // 2
            one, two = stat_ref[chunk], pair_stat[slot]
            top = jnp.maximum(one[0:2], two[0:2])
            one_factor = jnp.exp(one[0:2] - top)
            two_factor = jnp.exp(two[0:2] - top)
            stat = jnp.concatenate([top, one[2:4] * one_factor + two[2:4] * two_factor], axis=0)
            is_one = row + lax.rem(chunk * rows, size) < size
            context = ctx_ref[chunk].astype(jnp.float32) * jnp.where(
                is_one, one_factor[0:1], one_factor[1:2]
            ) + pair_ctx[slot].astype(jnp.float32) * jnp.where(
                is_one, two_factor[0:1], two_factor[1:2]
            )
            context = context.astype(jnp.bfloat16)

            @pl.when(chunk != me)
            def _():
                sum_stat[slot] = stat
                sum_ctx[slot] = context
                send(sum_stat.at[slot], got_stat.at[me // 2], 4, chunk)
                send(sum_ctx.at[slot], got_ctx.at[me // 2], 5, chunk)

            @pl.when(chunk == me)
            def _():
                got_stat[slot] = stat
                got_ctx[slot] = context

    @pl.loop(0, groups)
    def _(turn):
        group = lax.rem(me // group_chunks + 1 + turn, groups)
        query_rows = rows_together(q_ref, group * group_chunks, group_chunks).astype(jnp.bfloat16)
        peaks, totals, contexts = [], [], []

        def scores(local_head):
            query = jnp.concatenate(
                [query_rows[local_head * size : (local_head + 1) * size], query_tail], axis=0
            )
            return [
                jnp.dot(
                    k_ref[
                        group * group_heads + local_head,
                        pl.ds(older * frame_count, frame_count),
                        :,
                    ],
                    query[:, older * per_step :],
                    preferred_element_type=jnp.float32,
                )
                for older in range(steps)
            ]

        ready = scores(0)
        for local_head in range(group_heads):
            head = group * group_heads + local_head
            raws = ready
            if local_head + 1 < group_heads:
                ready = scores(local_head + 1)
            slope = slope_ref[head]
            peak = context = None
            for older in range(steps):
                first = older * per_step
                block = pl.ds(older * frame_count, frame_count)
                raw = raws[older]
                raw_peak = jnp.max(raw, axis=0, keepdims=True)
                weights = jnp.exp2((raw - raw_peak) * (scale * math.log2(math.e)))
                part_context = jnp.dot(
                    vt_ref[head, :, block],
                    weights.astype(jnp.bfloat16),
                    preferred_element_type=jnp.float32,
                )
                age = (token_step[:, first:] - older).astype(jnp.float32)
                part_peak = raw_peak * scale - slope * (distance[:, first:] + age)
                if peak is None:
                    peak, context = part_peak, part_context
                    continue
                top = jnp.maximum(peak[:, first:], part_peak)
                old_factor = jnp.exp(peak[:, first:] - top)
                new_factor = jnp.exp(part_peak - top)
                merged = context[:, first:] * old_factor + part_context * new_factor
                peak = jnp.concatenate([peak[:, :first], top], axis=1)
                context = jnp.concatenate([context[:, :first], merged], axis=1)
            peaks.append(peak)
            totals.append(context[size : size + 1])
            contexts.append(context[:size])
        stacked = jnp.concatenate(contexts, axis=0)
        for index in range(group_chunks):
            low, high = index * rows, (index + 1) * rows
            one, two = low // size, (high - 1) // size
            chunk = group * group_chunks + index
            ctx_ref[chunk] = stacked[low:high].astype(jnp.bfloat16)
            stat_ref[chunk] = jnp.concatenate(
                [peaks[one], peaks[two], totals[one], totals[two]], axis=0
            )

        @pl.loop(0, group_chunks // 2)
        def _(index):
            chunk = group * group_chunks + 2 * index + 1 - lax.rem(me, 2)
            for kind, (src, dst) in enumerate(((stat_ref, pair_stat), (ctx_ref, pair_ctx))):
                pltpu.make_async_remote_copy(
                    src_ref=src.at[chunk],
                    dst_ref=dst.at[chunk // 2],
                    send_sem=send_sem.at[kind],
                    recv_sem=pair_sem.at[kind, turn],
                    device_id={"seq": partner},
                    device_id_type=MESH,
                ).start()

        @pl.when(turn > 0)
        def _():
            pass_sums(turn - 1)

    pass_sums(groups - 1)
    await_bytes(got_stat, chips - 1, recv_sem.at[4])
    await_bytes(got_ctx, chips - 1, recv_sem.at[5])
    await_bytes(sum_stat, chips - 1, send_sem.at[4])
    await_bytes(sum_ctx, chips - 1, send_sem.at[5])
    await_bytes(stat_ref, chips, send_sem.at[0])
    await_bytes(ctx_ref, chips, send_sem.at[1])

    top = lax.fori_loop(
        1, chips, lambda at, best: jnp.maximum(best, got_stat[at][0:2]), got_stat[0][0:2]
    )
    is_one = row + lax.rem(me * rows, size) < size

    def add(at, state):
        total, acc = state
        stat = got_stat[at]
        factor = jnp.exp(stat[0:2] - top)
        spread = jnp.where(is_one, factor[0:1], factor[1:2])
        return total + stat[2:4] * factor, acc + got_ctx[at].astype(jnp.float32) * spread

    total, acc = lax.fori_loop(
        0,
        chips,
        add,
        (jnp.zeros((2, tokens), jnp.float32), jnp.zeros((rows, tokens), jnp.float32)),
    )
    fin_ref[me] = (acc / jnp.where(is_one, total[0:1], total[1:2])).astype(jnp.bfloat16)

    spread(fin_ref, 3, 1)
    relay(fin_ref, 3, 1)
    settle(fin_ref, 3, 1)
    context = rows_together(fin_ref, 0, n).astype(jnp.bfloat16)
    attended = jnp.dot(wout_ref[...], context, preferred_element_type=jnp.float32)
    attended = attended.astype(jnp.bfloat16)
    for step in range(steps):
        out_ref[step] = attended[:, step * per_step : (step + 1) * per_step]


def plain_local(n, frames, dec_states, w_query, w_keyval, w_output, head_slope, lengths, positions):
    steps, frame_count, width = frames.shape
    per_step = dec_states.shape[1]
    tokens = steps * per_step
    heads = head_slope.shape[0]
    size = width // heads
    rows = w_query.shape[1]
    keys = steps * frame_count
    tile = frame_count
    part = math.gcd(width, 256)
    vmem = pl.BlockSpec(memory_space=pltpu.VMEM)
    smem = pl.BlockSpec(memory_space=pltpu.SMEM)
    hbm = pl.BlockSpec(memory_space=pl.ANY)
    out = pl.pallas_call(
        functools.partial(plain_kernel, n),
        out_shape=jax.ShapeDtypeStruct((steps, rows, per_step), jnp.bfloat16),
        in_specs=[vmem, vmem, vmem, vmem, smem, smem, hbm, hbm],
        out_specs=vmem,
        scratch_shapes=[
            pltpu.VMEM((keys // tile, tile, width), jnp.bfloat16),
            pltpu.VMEM((2 * width // part, width, part), jnp.bfloat16),
            pltpu.VMEM((heads, keys, size + EXTRA), jnp.bfloat16),
            pltpu.VMEM((heads, size + EXTRA, keys), jnp.bfloat16),
            pltpu.VMEM((n, rows, tokens), jnp.bfloat16),
            pltpu.VMEM((n, rows, tokens), jnp.bfloat16),
            pltpu.VMEM((n, 4, tokens), jnp.float32),
            pltpu.VMEM((n // 2, rows, tokens), jnp.bfloat16),
            pltpu.VMEM((n // 2, 4, tokens), jnp.float32),
            pltpu.VMEM((n // 2, rows, tokens), jnp.bfloat16),
            pltpu.VMEM((n // 2, 4, tokens), jnp.float32),
            pltpu.VMEM((n // 2, rows, tokens), jnp.bfloat16),
            pltpu.VMEM((n // 2, 4, tokens), jnp.float32),
            pltpu.VMEM((n, rows, tokens), jnp.bfloat16),
            pltpu.SemaphoreType.DMA((keys // tile,)),
            pltpu.SemaphoreType.DMA((2 * width // part,)),
            pltpu.SemaphoreType.DMA((6,)),
            pltpu.SemaphoreType.DMA((6,)),
            pltpu.SemaphoreType.DMA((2, n // 2)),
            pltpu.SemaphoreType.DMA((2, math.gcd(heads, n))),
        ],
        compiler_params=pltpu.CompilerParams(
            collective_id=0, has_side_effects=True, vmem_limit_bytes=60 * 1024 * 1024
        ),
    )(
        dec_states.reshape(tokens, width),
        w_query.T,
        w_output.T,
        positions.reshape(1, tokens),
        head_slope,
        lengths,
        frames,
        w_keyval,
    )
    return out.transpose(0, 2, 1)


GROUPS = ((3, 2), (5, 2), (0, 2), (2, 1), (7, 1), (8, 1), (9, 1))
PLAN = (
    ("K1", "B0", "Q0", "V1", "K2", "V2", "K3", "Q1", "V3", "W0", "K0", "Y0", "A0", "A1", "M0", "W1", "K4", "M1")
    + ("Y1", "A2", "A3", "M2", "C0", "A4", "M3", "C1", "A5", "M4", "A6", "M5", "M6", "C2", "X0", "C3", "X1", "C4")
    + ("R0", "C5", "C6", "R1", "R2", "R3", "R4", "R5")
)
BESIDE = {0: "V0", 2: "V4"}
SUMS = ("far", "far", "far", "far", "far", "far", "far")
SHARES = ("column", "column", "relay", "relay", "relay", "relay", "direct")


def paired_kernel(
    n,
    pos_hbm,
    slope_hbm,
    len_hbm,
    dec_hbm,
    wq_hbm,
    wout_hbm,
    frames_hbm,
    wkv_hbm,
    out_ref,
    pos_ref,
    slope_ref,
    len_ref,
    dec_ref,
    wq_ref,
    wout_ref,
    frames_ref,
    wkv_ref,
    k_ref,
    mask_ref,
    vt_ref,
    q_ref,
    ctx_ref,
    stat_ref,
    pair_ctx,
    pair_stat,
    chip_ctx,
    chip_stat,
    got_ctx,
    got_stat,
    near_stat,
    side_stat,
    side_ctx,
    fin_ref,
    small_sem,
    frame_sem,
    weight_sem,
    send_sem,
    hop_sem,
    relay_sem,
    pair_sem,
    got_sem,
    near_sem,
    fin_sem,
    both_sem,
    side_sem,
):
    me = lax.axis_index("seq")
    core, chip = lax.rem(me, 2), me // 2
    partner = me + 1 - 2 * core
    chips = n // 2
    steps, frame_count, width = frames_hbm.shape
    tokens = dec_hbm.shape[0]
    per_step = tokens // steps
    pairs, lanes = vt_ref.shape[0], vt_ref.shape[1]
    size = lanes // 2
    rows = wq_hbm.shape[0]
    half = wkv_ref.shape[2]
    parts = wkv_ref.shape[0] // 2
    part_pairs = half // lanes
    scale = 1.0 / math.sqrt(size)
    groups = GROUPS
    side, level, levels = lax.rem(chip, 2), chip // 2, chips // 2

    small = [
        pltpu.make_async_copy(src, dst, small_sem.at[at])
        for at, (src, dst) in enumerate(
            (
                (dec_hbm, dec_ref),
                (wq_hbm, wq_ref),
                (wout_hbm, wout_ref),
                (pos_hbm, pos_ref),
                (slope_hbm, slope_ref),
                (len_hbm, len_ref),
            )
        )
    ]

    def frame_copy(index):
        return pltpu.make_async_copy(frames_hbm.at[index], frames_ref.at[index], frame_sem.at[index])

    def weight_copy(index):
        return pltpu.make_async_copy(
            wkv_hbm.at[:, pl.ds(pl.multiple_of(index * half, half), half)], wkv_ref.at[index], weight_sem.at[index]
        )

    for at in (1, 0, 5, 4, 3):
        small[at].start()
    ordered = [stage if stage[0] in "KV" else BESIDE.get(int(stage[1:]), "B") for stage in PLAN if stage[0] in "KVA"]
    weight_order = [int(stage[1:]) + parts * (stage[0] == "V") for stage in ordered if stage != "B"]
    weight_copy(weight_order[0]).start(priority=1)
    for step in range(steps):
        frame_copy(step).start(priority=1)

    barrier = pltpu.get_barrier_semaphore()

    @pl.loop(1, n)
    def _(step):
        peer = lax.rem(me + step, n)
        pl.semaphore_signal(barrier, inc=1, device_id={"seq": peer}, device_id_type=MESH)

    def remote(src, dst, sent, got, peer):
        return pltpu.make_async_remote_copy(
            src_ref=src,
            dst_ref=dst,
            send_sem=sent,
            recv_sem=got,
            device_id={"seq": peer},
            device_id_type=MESH,
        )

    def await_copy(ref, sem):
        pltpu.make_async_copy(ref, ref, sem).wait()

    def query_rows(device):
        return q_ref.at[pl.ds(pl.multiple_of(device * rows, 16), rows)]

    def await_small():
        for at in (1, 0, 5, 4, 3):
            small[at].wait()

    def project_query():
        own_query = lax.dot_general(
            wq_ref[...], dec_ref[...], (((1,), (1,)), ((), ())), preferred_element_type=jnp.float32
        )
        q_ref[pl.ds(pl.multiple_of(me * rows, 16), rows), :] = own_query.astype(jnp.bfloat16)

    def await_barrier(_):
        for index in weight_order[4:]:
            weight_copy(index).start(priority=1)
        small[2].start(priority=1)
        pl.semaphore_wait(barrier, n - 1)

    await_small()
    project_query()

    middle = chips // 4
    wave_chips = (
        list(range(middle, chips - middle)),
        list(range(middle)) + list(range(chips - middle, chips)),
    )
    is_middle = (chip >= middle) & (chip < chips - middle)

    def query_relay(device, wave):
        block = query_rows(device)
        remote(block, block, send_sem.at[1], relay_sem.at[wave], partner).start()

    def spread_queries(wave):
        @pl.when(is_middle if wave == 0 else jnp.logical_not(is_middle))
        def _():
            own = query_rows(me)

            @pl.loop(1, chips)
            def _(step):
                remote(own, own, send_sem.at[0], hop_sem.at[chip], lax.rem(me + 2 * step, n)).start()

            query_relay(me, wave)

    def relay_queries(wave):
        for source in wave_chips[wave]:

            @pl.when(source != chip)
            def _():
                await_copy(query_rows(me), hop_sem.at[source])
                query_relay(2 * source + core, wave)

    def await_queries(wave):
        await_copy(q_ref.at[pl.ds(0, rows * len(wave_chips[wave]))], relay_sem.at[wave])

    place = lax.broadcasted_iota(jnp.int32, (frame_count, lanes), 0)
    column = lax.broadcasted_iota(jnp.int32, (frame_count, lanes), 1)
    for older in range(steps):
        hidden = (place >= len_ref[older, me]) & (column == 0)
        mask_ref[older * frame_count : (older + 1) * frame_count, :] = jnp.where(hidden, MASKED, 0.0).astype(
            jnp.bfloat16
        )

    def keys_piece(part, step, begin, stop):
        keys = jnp.dot(
            frames_ref[step, begin:stop, :], wkv_ref[part], preferred_element_type=jnp.float32
        ).astype(jnp.bfloat16)
        at = slice(step * frame_count + begin, step * frame_count + stop)
        for index in range(part_pairs):
            k_ref[part * part_pairs + index, at, :] = keys[:, index * lanes : (index + 1) * lanes]

    def values_piece(part, step, begin, stop):
        values = jnp.dot(
            frames_ref[step, begin:stop, :], wkv_ref[parts + part], preferred_element_type=jnp.float32
        )
        turned = values.astype(jnp.bfloat16).T
        at = slice(step * frame_count + begin, step * frame_count + stop)
        for index in range(part_pairs):
            vt_ref[part * part_pairs + index, :, at] = turned[index * lanes : (index + 1) * lanes]

    def project(kind, part, cuts):
        piece = keys_piece if kind == "K" else values_piece
        return [
            functools.partial(piece, part, step, begin, stop)
            for step in range(steps)
            for begin, stop in zip(cuts, cuts[1:])
        ]

    def project_keys(part):
        weight_copy(part).wait()
        for piece in project("K", part, (0, frame_count)):
            piece()

    def project_values(part):
        weight_copy(parts + part).wait()
        for piece in project("V", part, (0, frame_count)):
            piece()

    def await_frames():
        for step in range(steps):
            frame_copy(step).wait()

    for index in weight_order[1:4]:
        weight_copy(index).start(priority=1)
    await_frames()

    slot_place = lax.rem(me + 1, n).astype(jnp.float32)
    distance = jnp.abs(pos_ref[...].astype(jnp.float32) - slot_place) / n
    tail_row = lax.broadcasted_iota(jnp.int32, (lanes, tokens), 0) == 0
    tail = jnp.where(tail_row, 1.0, 0.0).astype(jnp.bfloat16)
    blank = jnp.zeros((size, tokens), jnp.bfloat16)
    ones = jnp.ones((EXTRA, frame_count), jnp.bfloat16)
    first, second = slice(0, frame_count), slice(frame_count, 2 * frame_count)
    early, late = slice(0, per_step), slice(per_step, tokens)

    def attend_scores(pair):
        query = q_ref[pl.ds(pl.multiple_of(pair * lanes, lanes), lanes), :]
        one = jnp.concatenate([query[:size], blank, tail], axis=0)
        two = jnp.concatenate([blank, query[size:], tail], axis=0)
        both = jnp.concatenate([one[:, late], two[:, late]], axis=1)
        old = jnp.concatenate([k_ref[pair, first, :], mask_ref[first, :]], axis=1)
        new = jnp.concatenate([k_ref[pair, second, :], mask_ref[second, :]], axis=1)
        return [
            functools.partial(jnp.dot, keys, queries, preferred_element_type=jnp.float32)
            for keys, queries in ((old, one), (old, two), (new, both))
        ]

    def soften(raw):
        peak = jnp.max(raw, axis=0, keepdims=True)
        weights = jnp.exp2((raw - peak) * (scale * math.log2(math.e)))
        return peak * scale, weights.astype(jnp.bfloat16)

    def attend_values(pair, kind):
        if kind == 2:
            stack = [vt_ref[pair, :, second], ones]
        else:
            stack = [vt_ref[pair, kind * size : (kind + 1) * size, first], ones]
        return jnp.concatenate(stack, axis=0)

    def attend(group):
        first_pair, count = groups[group]
        beside = []
        if group in BESIDE:
            kind, part = BESIDE[group][0], int(BESIDE[group][1:])
            weight_copy(part + parts * (kind == "V")).wait()
            half_frames = frame_count // 256 * 128
            beside = project(kind, part, (0, half_frames, frame_count))
        dots = []
        for local_pair in range(count):
            dots += [(local_pair, kind, call) for kind, call in enumerate(attend_scores(first_pair + local_pair))]
        results = {}
        ready = [dots[0][2](), dots[1][2]()]
        for at, (local_pair, kind, _) in enumerate(dots):
            raw = ready.pop(0)
            if at + 2 < len(dots):
                ready.append(dots[at + 2][2]())
            if beside:
                beside.pop(0)()
            peak, weights = soften(raw)
            values = attend_values(first_pair + local_pair, kind)
            results[local_pair, kind] = peak, jnp.dot(values, weights, preferred_element_type=jnp.float32)
        for piece in beside:
            piece()
        peaks = [[], []]
        totals = [[], []]
        for local_pair in range(count):
            pair = first_pair + local_pair
            new_peaks, new_context = results[local_pair, 2]
            for which in range(2):
                slope = slope_ref[2 * pair + which]
                at = pl.ds(pl.multiple_of(pair * lanes + which * size, size), size)
                peak, context = results[local_pair, which]
                peaks[0].append(peak[:, early] - slope * distance[:, early])
                totals[0].append(context[size : size + 1, early])
                ctx_ref[0, at, :] = context[:size, early].astype(jnp.bfloat16)
                span = slice(which * per_step, (which + 1) * per_step)
                old_peak = peak[:, late] - slope * (distance[:, late] + 1.0)
                new_peak = new_peaks[:, span] - slope * distance[:, late]
                top = jnp.maximum(old_peak, new_peak)
                old_factor, new_factor = jnp.exp(old_peak - top), jnp.exp(new_peak - top)
                own = slice(which * size, (which + 1) * size)
                merged = context[:size, late] * old_factor + new_context[own, span] * new_factor
                ctx_ref[1, at, :] = merged.astype(jnp.bfloat16)
                peaks[1].append(top)
                old_total = context[size : size + 1, late] * old_factor
                totals[1].append(old_total + new_context[lanes : lanes + 1, span] * new_factor)
        for step in range(2):
            stat_ref[step, group, 0 : 4 * count, :] = jnp.concatenate(peaks[step] + totals[step], axis=0)
        block = pl.ds(pl.multiple_of(first_pair * lanes, lanes), count * lanes)
        other = 1 - core
        remote(
            stat_ref.at[other, group], pair_stat.at[group], send_sem.at[2], pair_sem.at[0, group], partner
        ).start()
        remote(
            ctx_ref.at[other, block], pair_ctx.at[block], send_sem.at[3], pair_sem.at[1, group], partner
        ).start()

    def slices(first_pair, count):
        part_rows = count * lanes // chips
        base = first_pair * lanes

        def block(owner):
            place = lax.rem(owner, 2) * (chips // 2) + owner // 2
            return pl.ds(pl.multiple_of(base + place * part_rows, 16), part_rows)

        slot = pl.ds(pl.multiple_of(base // chips, 16), part_rows)
        return part_rows, block, slot

    def mix(one, two, heads):
        top = jnp.maximum(one[:heads], two[:heads])
        one_factor, two_factor = jnp.exp(one[:heads] - top), jnp.exp(two[:heads] - top)
        total = one[heads : 2 * heads] * one_factor + two[heads : 2 * heads] * two_factor
        return top, total, one_factor, two_factor

    def merge_cores(group):
        first_pair, count = groups[group]
        part_rows, block, slot = slices(first_pair, count)
        heads = 2 * count
        await_copy(pair_stat.at[group], pair_sem.at[0, group])
        await_copy(pair_ctx.at[pl.ds(0, count * lanes)], pair_sem.at[1, group])
        top, total, one_factor, two_factor = mix(stat_ref[core, group], pair_stat[group], heads)
        for head in range(heads):
            at = slice(first_pair * lanes + head * size, first_pair * lanes + (head + 1) * size)
            merged = (
                ctx_ref[core, at, :].astype(jnp.float32) * one_factor[head : head + 1]
                + pair_ctx[at, :].astype(jnp.float32) * two_factor[head : head + 1]
            )
            chip_ctx[at, :] = merged.astype(jnp.bfloat16)
        if SUMS[group] == "near":
            near_stat[group] = jnp.concatenate([top, total], axis=0)
            block = side_rows(group, 1 - side)
            peer = me + 2 - 4 * side
            remote(
                near_stat.at[group], side_stat.at[group], send_sem.at[12], near_sem.at[0, group], peer
            ).start()
            remote(
                chip_ctx.at[block], side_ctx.at[block], send_sem.at[11], near_sem.at[1, group], peer
            ).start()
            return
        for owner in range(chips):
            head = (owner % 2 * levels + owner // 2) * part_rows // size
            chip_stat[group, owner] = jnp.concatenate([top[head : head + 1], total[head : head + 1]], axis=0)

        @pl.loop(1, chips)
        def _(step):
            owner = lax.rem(chip + step, chips)
            peer = 2 * owner + core
            remote(
                chip_stat.at[group, owner], got_stat.at[group, chip], send_sem.at[4], got_sem.at[0, group], peer
            ).start()
            remote(
                chip_ctx.at[block(owner)], got_ctx.at[chip, slot], send_sem.at[5], got_sem.at[1, group], peer
            ).start()

        got_stat[group, chip] = chip_stat[group, chip]
        got_ctx[chip, slot, :] = chip_ctx[block(chip), :]

    def side_rows(group, which):
        first_pair, count = groups[group]
        span = count * lanes // 2
        return pl.ds(pl.multiple_of(first_pair * lanes + which * span, 16), span)

    def merge_sides(group):
        first_pair, count = groups[group]
        part_rows, block, slot = slices(first_pair, count)
        await_copy(side_stat.at[group], near_sem.at[0, group])
        await_copy(side_ctx.at[pl.ds(0, count * lanes // 2)], near_sem.at[1, group])
        stats = mix(near_stat[group], side_stat[group], 2 * count)
        top, total, one_factor, two_factor = (
            jnp.where(side == 0, stat[:count], stat[count:]) for stat in stats
        )
        base = first_pair * lanes + side * (count * lanes // 2)
        for head in range(count):
            at = pl.ds(pl.multiple_of(base + head * size, size), size)
            merged = (
                chip_ctx[at, :].astype(jnp.float32) * one_factor[head : head + 1]
                + side_ctx[at, :].astype(jnp.float32) * two_factor[head : head + 1]
            )
            chip_ctx[at, :] = merged.astype(jnp.bfloat16)
        for owner in range(levels):
            head = owner * part_rows // size
            chip_stat[group, owner] = jnp.concatenate([top[head : head + 1], total[head : head + 1]], axis=0)

        @pl.loop(1, levels)
        def _(step):
            owner = lax.rem(level + step, levels)
            peer = lax.rem(me + 4 * step, n)
            remote(
                chip_stat.at[group, owner], got_stat.at[group, level], send_sem.at[13], got_sem.at[0, group], peer
            ).start()
            remote(
                chip_ctx.at[block(2 * owner + side)],
                got_ctx.at[level, slot],
                send_sem.at[10],
                got_sem.at[1, group],
                peer,
            ).start()

        got_stat[group, level] = chip_stat[group, level]
        got_ctx[level, slot, :] = chip_ctx[block(chip), :]

    def merge_chips(group):
        first_pair, count = groups[group]
        mode = SHARES[group]
        sources = levels if SUMS[group] == "near" else chips
        part_rows, block, slot = slices(first_pair, count)
        await_copy(got_stat.at[group, pl.ds(0, sources - 1)], got_sem.at[0, group])
        await_copy(got_ctx.at[pl.ds(0, sources - 1), pl.ds(0, part_rows)], got_sem.at[1, group])
        stats = [got_stat[group, source] for source in range(sources)]
        top = stats[0][0:1]
        for stat in stats[1:]:
            top = jnp.maximum(top, stat[0:1])
        total = context = None
        for source, stat in enumerate(stats):
            factor = jnp.exp(stat[0:1] - top)
            part_total = stat[1:2] * factor
            part_context = got_ctx[source, slot, :].astype(jnp.float32) * factor
            total = part_total if total is None else total + part_total
            context = part_context if context is None else context + part_context
        fin_ref[core, block(chip), :] = (context / total).astype(jnp.bfloat16)
        own = fin_ref.at[core, block(chip)]
        if mode == "direct":

            @pl.loop(1, n)
            def _(step):
                remote(own, own, send_sem.at[7], fin_sem.at[group], lax.rem(me + step, n)).start()

        else:
            stride = 4 if mode == "column" else 2

            @pl.loop(1, n // stride)
            def _(step):
                remote(
                    own, own, send_sem.at[6], fin_sem.at[group], lax.rem(me + stride * step, n)
                ).start()

    def group_rows(group):
        first_pair, count = groups[group]
        return slice(first_pair * lanes, (first_pair + count) * lanes)

    def await_slices(group, amount):
        await_copy(fin_ref.at[0, pl.ds(0, amount * groups[group][1] * lanes // chips)], fin_sem.at[group])

    def cross(group):
        await_slices(group, levels - 1)
        block = fin_ref.at[core, side_rows(group, side)]
        remote(block, block, send_sem.at[9], side_sem.at[group], me + 2 - 4 * side).start()

    def relay(group):
        if SHARES[group] == "column":
            await_copy(fin_ref.at[0, pl.ds(0, groups[group][1] * lanes // 2)], side_sem.at[group])
        else:
            await_slices(group, chips - 1)
        block = fin_ref.at[core, group_rows(group)]
        remote(block, block, send_sem.at[8], both_sem.at[group], partner).start()

    stages = {
        "K": project_keys,
        "V": project_values,
        "B": await_barrier,
        "Q": spread_queries,
        "W": relay_queries,
        "Y": await_queries,
        "A": attend,
        "M": merge_cores,
        "S": merge_sides,
        "C": merge_chips,
        "X": cross,
        "R": relay,
    }
    for stage in PLAN:
        stages[stage[0]](int(stage[1:]))

    def await_both(group):
        await_copy(fin_ref.at[0, group_rows(group)], both_sem.at[group])

    small[2].wait()
    direct = [group for group, mode in enumerate(SHARES) if mode == "direct"]
    for group in range(direct[0]):
        await_both(group)

    def attended(begin, stop):
        context = jnp.concatenate([fin_ref[0, begin:stop, :], fin_ref[1, begin:stop, :]], axis=1)
        return jnp.dot(wout_ref[:, begin:stop], context, preferred_element_type=jnp.float32)

    late_row = groups[direct[0]][0] * lanes
    total = attended(0, late_row)
    for group in direct:
        await_slices(group, n - 1)
    total = total + attended(late_row, width)
    total = total.astype(jnp.bfloat16)
    for step in range(steps):
        out_ref[step] = total[:, step * per_step : (step + 1) * per_step]

    def sent(amount, sem):
        await_copy(fin_ref.at[0, pl.ds(0, amount)], send_sem.at[sem])

    share_rows = {mode: 0 for mode in SHARES}
    sum_rows = {mode: 0 for mode in SUMS}
    sum_count = {mode: 0 for mode in SUMS}
    for (_, count), shared, summed in zip(groups, SHARES, SUMS):
        share_rows[shared] += count * lanes // chips
        sum_rows[summed] += count * lanes // chips
        sum_count[summed] += 1
    await_copy(q_ref.at[pl.ds(0, rows * (chips - 1))], send_sem.at[0])
    await_copy(q_ref.at[pl.ds(0, rows * chips)], send_sem.at[1])
    await_copy(stat_ref.at[0], send_sem.at[2])
    await_copy(ctx_ref.at[0], send_sem.at[3])
    await_copy(got_stat.at[pl.ds(0, sum_count["far"]), pl.ds(0, chips - 1)], send_sem.at[4])
    sent((chips - 1) * sum_rows["far"], 5)
    sent((levels - 1) * share_rows["column"] + (chips - 1) * share_rows["relay"], 6)
    sent((n - 1) * share_rows["direct"], 7)
    sent(late_row, 8)
    sent(levels * share_rows["column"], 9)
    if "near" in SUMS:
        sent((levels - 1) * sum_rows["near"], 10)
        sent(levels * sum_rows["near"], 11)
        await_copy(side_stat.at[pl.ds(0, sum_count["near"])], send_sem.at[12])
        await_copy(got_stat.at[pl.ds(0, sum_count["near"]), pl.ds(0, levels - 1)], send_sem.at[13])


def paired_local(n, frames, dec_states, w_query, w_keyval, w_output, head_slope, lengths, positions):
    steps, frame_count, width = frames.shape
    per_step = dec_states.shape[1]
    tokens = steps * per_step
    heads = head_slope.shape[0]
    lanes = 2 * (width // heads)
    pairs = heads // 2
    rows = w_query.shape[1]
    keys = steps * frame_count
    part = 2 * lanes
    chips = n // 2
    groups = len(GROUPS)
    vmem = pl.BlockSpec(memory_space=pltpu.VMEM)
    hbm = pl.BlockSpec(memory_space=pltpu.HBM)
    out = pl.pallas_call(
        functools.partial(paired_kernel, n),
        out_shape=pltpu.VMEM((steps, rows, per_step), jnp.bfloat16),
        in_specs=[hbm] * 8,
        out_specs=vmem,
        scratch_shapes=[
            pltpu.VMEM((1, tokens), jnp.int32),
            pltpu.SMEM((heads,), jnp.float32),
            pltpu.SMEM(lengths.shape, jnp.int32),
            pltpu.VMEM((tokens, width), jnp.bfloat16),
            pltpu.VMEM((rows, width), jnp.bfloat16),
            pltpu.VMEM((rows, width), jnp.bfloat16),
            pltpu.VMEM((steps, frame_count, width), jnp.bfloat16),
            pltpu.VMEM((2 * width // part, width, part), jnp.bfloat16),
            pltpu.VMEM((pairs, keys, lanes), jnp.bfloat16),
            pltpu.VMEM((keys, lanes), jnp.bfloat16),
            pltpu.VMEM((pairs, lanes, keys), jnp.bfloat16),
            pltpu.VMEM((width, tokens), jnp.bfloat16),
            pltpu.VMEM((2, width, per_step), jnp.bfloat16),
            pltpu.VMEM((2, groups, 8, per_step), jnp.float32),
            pltpu.VMEM((width, per_step), jnp.bfloat16),
            pltpu.VMEM((groups, 8, per_step), jnp.float32),
            pltpu.VMEM((width, per_step), jnp.bfloat16),
            pltpu.VMEM((groups, chips, 2, per_step), jnp.float32),
            pltpu.VMEM((chips, width // chips, per_step), jnp.bfloat16),
            pltpu.VMEM((groups, chips, 2, per_step), jnp.float32),
            pltpu.VMEM((groups, 8, per_step), jnp.float32),
            pltpu.VMEM((groups, 8, per_step), jnp.float32),
            pltpu.VMEM((width, per_step), jnp.bfloat16),
            pltpu.VMEM((2, width, per_step), jnp.bfloat16),
            pltpu.SemaphoreType.DMA((6,)),
            pltpu.SemaphoreType.DMA((steps,)),
            pltpu.SemaphoreType.DMA((2 * width // part,)),
            pltpu.SemaphoreType.DMA((14,)),
            pltpu.SemaphoreType.DMA((chips,)),
            pltpu.SemaphoreType.DMA((2,)),
            pltpu.SemaphoreType.DMA((2, groups)),
            pltpu.SemaphoreType.DMA((2, groups)),
            pltpu.SemaphoreType.DMA((2, groups)),
            pltpu.SemaphoreType.DMA((groups,)),
            pltpu.SemaphoreType.DMA((groups,)),
            pltpu.SemaphoreType.DMA((groups,)),
        ],
        compiler_params=pltpu.CompilerParams(
            collective_id=0, has_side_effects=True, vmem_limit_bytes=40 * 1024 * 1024
        ),
    )(
        *(
            pltpu.with_memory_space_constraint(value, pltpu.HBM)
            for value in (
                positions.reshape(1, tokens),
                head_slope,
                lengths,
                dec_states.reshape(tokens, width),
                w_query.T,
                w_output.T,
                frames,
                w_keyval,
            )
        )
    )
    return out.transpose(0, 2, 1)


def fits_pairs(n, frames, dec_states, w_query, head_slope):
    steps, frame_count, width = frames.shape
    per_step, heads = dec_states.shape[1], head_slope.shape[0]
    size = width // heads
    chips = n // 2
    return (
        steps == 2
        and n % 4 == 0
        and heads % 4 == 0
        and heads // 2 == sum(count for _, count in GROUPS)
        and n % 8 == 0
        and size == 64
        and per_step == 2 * size
        and frame_count % 128 == 0
        and w_query.shape[1] % 16 == 0
        and (2 * size) % (16 * chips) == 0
    )


def local(n, frames, dec_states, w_query, w_keyval, w_output, head_slope, lengths, positions):
    paired = fits_pairs(n, frames, dec_states, w_query, head_slope)
    run = paired_local if paired else plain_local
    return run(n, frames, dec_states, w_query, w_keyval, w_output, head_slope, lengths, positions)


def solution(mesh):
    return jax.shard_map(
        functools.partial(local, mesh.shape["seq"]),
        mesh=mesh,
        in_specs=(
            P("grp", "seq", None),
            P(None, "grp", None),
            P(None, "seq"),
            P(),
            P(None, "seq"),
            P(),
            P("grp", None),
            P(None, "grp"),
        ),
        out_specs=P(None, "grp", "seq"),
        check_vma=False,
    )
```

```python
import functools
import math

import jax
import jax.numpy as jnp
from jax import lax
from jax.experimental import pallas as pl
from jax.experimental.pallas import tpu as pltpu
from jax.sharding import PartitionSpec as P

MESH = pl.DeviceIdType.MESH
EXTRA = 16
MASKED = -1e30


def rows_together(ref, first, count):
    parts = [ref[first + index].astype(jnp.float32) for index in range(count)]
    return jnp.concatenate(parts, axis=0)


def await_bytes(ref, count, sem):
    part = ref.at[pl.ds(0, count)]
    pltpu.make_async_copy(part, part, sem).wait()


def plain_kernel(
    n,
    dec_ref,
    wq_ref,
    wout_ref,
    pos_ref,
    slope_ref,
    len_ref,
    frames_hbm,
    wkv_hbm,
    out_ref,
    frames_ref,
    wkv_ref,
    k_ref,
    vt_ref,
    q_ref,
    ctx_ref,
    stat_ref,
    got_ctx,
    got_stat,
    pair_ctx,
    pair_stat,
    sum_ctx,
    sum_stat,
    fin_ref,
    frame_sem,
    weight_sem,
    send_sem,
    recv_sem,
    hop_sem,
    pair_sem,
):
    me = lax.axis_index("seq")
    steps, frame_count, width = frames_hbm.shape
    tokens = dec_ref.shape[0]
    per_step = tokens // steps
    heads = k_ref.shape[0]
    size = width // heads
    rows = wq_ref.shape[0]
    groups = math.gcd(heads, n)
    group_chunks = n // groups
    group_heads = heads // groups
    tile = frames_ref.shape[1]
    half = wkv_ref.shape[2]
    tiles = frames_ref.shape[0]
    per_block = frame_count // tile
    scale = 1.0 / math.sqrt(size)

    def frame_copy(index):
        return pltpu.make_async_copy(
            frames_hbm.at[index // per_block, pl.ds((index % per_block) * tile, tile)],
            frames_ref.at[index],
            frame_sem.at[index],
        )

    def weight_copy(index):
        return pltpu.make_async_copy(
            wkv_hbm.at[:, pl.ds(pl.multiple_of(index * half, half), half)], wkv_ref.at[index], weight_sem.at[index]
        )

    frame_copy(0).start()
    weight_copy(0).start()
    for index in range(1, tiles):
        frame_copy(index).start()
    for index in range(1, wkv_ref.shape[0]):
        weight_copy(index).start()

    barrier = pltpu.get_barrier_semaphore()

    @pl.loop(1, n)
    def _(step):
        peer = lax.rem(me + step, n)
        pl.semaphore_signal(barrier, inc=1, device_id={"seq": peer}, device_id_type=MESH)

    own_query = lax.dot_general(
        wq_ref[...], dec_ref[...], (((1,), (1,)), ((), ())), preferred_element_type=jnp.float32
    )
    q_ref[me] = own_query.astype(jnp.bfloat16)
    pl.semaphore_wait(barrier, n - 1)

    def send(src, dst, sem, peer):
        pltpu.make_async_remote_copy(
            src_ref=src,
            dst_ref=dst,
            send_sem=send_sem.at[sem],
            recv_sem=recv_sem.at[sem],
            device_id={"seq": peer},
            device_id_type=MESH,
        ).start()

    partner = me + 1 - 2 * lax.rem(me, 2)
    chips = n // 2

    def pass_on(ref, chunk, sem):
        send(ref.at[chunk], ref.at[chunk], sem, partner)

    def hop(ref, step, sem, level):
        return pltpu.make_async_remote_copy(
            src_ref=ref.at[me],
            dst_ref=ref.at[me],
            send_sem=send_sem.at[sem],
            recv_sem=hop_sem.at[level, step],
            device_id={"seq": lax.rem(me + 2 * step, n)},
            device_id_type=MESH,
        )

    def spread(ref, sem, level):
        @pl.loop(1, chips)
        def _(step):
            hop(ref, step, sem, level).start()

        pass_on(ref, me, level)

    def relay(ref, sem, level):
        @pl.loop(1, chips)
        def _(step):
            hop(ref, step, sem, level).wait_recv()
            pass_on(ref, lax.rem(me - 2 * step + n, n), level)

    def settle(ref, sem, level):
        await_bytes(ref, chips - 1, send_sem.at[sem])
        await_bytes(ref, chips, recv_sem.at[level])
        await_bytes(ref, chips, send_sem.at[level])

    spread(q_ref, 2, 0)

    column = lax.broadcasted_iota(jnp.int32, (frame_count, size + EXTRA), 1)
    place = lax.broadcasted_iota(jnp.int32, (frame_count, size + EXTRA), 0)
    masks = []
    for older in range(steps):
        hidden = (place >= len_ref[older, me]) & (column == size)
        masks.append(jnp.where(hidden, MASKED, 0.0).astype(jnp.bfloat16))
    mask = jnp.concatenate(masks, axis=0)
    ones = jnp.ones((EXTRA, steps * frame_count), jnp.bfloat16)

    @pl.loop(0, heads)
    def _(head):
        k_ref[head] = mask
        vt_ref[head, size:, :] = ones

    parts = wkv_ref.shape[0] // 2
    part_heads = half // size

    def project(part, index):
        at = pl.ds(pl.multiple_of(index * tile, tile), tile)
        keyval = jnp.dot(frames_ref[index], wkv_ref[part], preferred_element_type=jnp.float32)
        return at, keyval.astype(jnp.bfloat16)

    for index in range(tiles):
        frame_copy(index).wait()

    @pl.loop(0, parts)
    def _(part):
        weight_copy(part).wait()
        for index in range(tiles):
            at, keyval = project(part, index)
            for local_head in range(part_heads):
                lanes = slice(local_head * size, (local_head + 1) * size)
                k_ref[part * part_heads + local_head, at, 0:size] = keyval[:, lanes]

    def project_values(part):
        weight_copy(parts + part).wait()
        for index in range(tiles):
            at, keyval = project(parts + part, index)
            turned = keyval.T
            for local_head in range(part_heads):
                lanes = slice(local_head * size, (local_head + 1) * size)
                vt_ref[part * part_heads + local_head, 0:size, at] = turned[lanes]

    pl.loop(0, parts - 2)(project_values)
    relay(q_ref, 2, 0)
    pl.loop(parts - 2, parts)(project_values)
    settle(q_ref, 2, 0)

    slot_place = lax.rem(me + 1, n).astype(jnp.float32)
    distance = jnp.abs(pos_ref[...].astype(jnp.float32) - slot_place) / n
    first_row = lax.broadcasted_iota(jnp.int32, (EXTRA, tokens), 0) == 0
    query_tail = jnp.where(first_row, 1.0, 0.0).astype(jnp.bfloat16)
    token_step = lax.broadcasted_iota(jnp.int32, (1, tokens), 1) // per_step

    row = lax.broadcasted_iota(jnp.int32, (rows, tokens), 0)

    def pass_sums(turn):
        group = lax.rem(me // group_chunks + 1 + turn, groups)
        await_bytes(pair_stat, group_chunks // 2, pair_sem.at[0, turn])
        await_bytes(pair_ctx, group_chunks // 2, pair_sem.at[1, turn])

        @pl.loop(0, group_chunks // 2)
        def _(index):
            chunk = group * group_chunks + 2 * index + lax.rem(me, 2)
            slot = chunk // 2
            one, two = stat_ref[chunk], pair_stat[slot]
            top = jnp.maximum(one[0:2], two[0:2])
            one_factor = jnp.exp(one[0:2] - top)
            two_factor = jnp.exp(two[0:2] - top)
            stat = jnp.concatenate([top, one[2:4] * one_factor + two[2:4] * two_factor], axis=0)
            is_one = row + lax.rem(chunk * rows, size) < size
            context = ctx_ref[chunk].astype(jnp.float32) * jnp.where(
                is_one, one_factor[0:1], one_factor[1:2]
            ) + pair_ctx[slot].astype(jnp.float32) * jnp.where(
                is_one, two_factor[0:1], two_factor[1:2]
            )
            context = context.astype(jnp.bfloat16)

            @pl.when(chunk != me)
            def _():
                sum_stat[slot] = stat
                sum_ctx[slot] = context
                send(sum_stat.at[slot], got_stat.at[me // 2], 4, chunk)
                send(sum_ctx.at[slot], got_ctx.at[me // 2], 5, chunk)

            @pl.when(chunk == me)
            def _():
                got_stat[slot] = stat
                got_ctx[slot] = context

    @pl.loop(0, groups)
    def _(turn):
        group = lax.rem(me // group_chunks + 1 + turn, groups)
        query_rows = rows_together(q_ref, group * group_chunks, group_chunks).astype(jnp.bfloat16)
        peaks, totals, contexts = [], [], []

        def scores(local_head):
            query = jnp.concatenate(
                [query_rows[local_head * size : (local_head + 1) * size], query_tail], axis=0
            )
            return [
                jnp.dot(
                    k_ref[
                        group * group_heads + local_head,
                        pl.ds(older * frame_count, frame_count),
                        :,
                    ],
                    query[:, older * per_step :],
                    preferred_element_type=jnp.float32,
                )
                for older in range(steps)
            ]

        ready = scores(0)
        for local_head in range(group_heads):
            head = group * group_heads + local_head
            raws = ready
            if local_head + 1 < group_heads:
                ready = scores(local_head + 1)
            slope = slope_ref[head]
            peak = context = None
            for older in range(steps):
                first = older * per_step
                block = pl.ds(older * frame_count, frame_count)
                raw = raws[older]
                raw_peak = jnp.max(raw, axis=0, keepdims=True)
                weights = jnp.exp2((raw - raw_peak) * (scale * math.log2(math.e)))
                part_context = jnp.dot(
                    vt_ref[head, :, block],
                    weights.astype(jnp.bfloat16),
                    preferred_element_type=jnp.float32,
                )
                age = (token_step[:, first:] - older).astype(jnp.float32)
                part_peak = raw_peak * scale - slope * (distance[:, first:] + age)
                if peak is None:
                    peak, context = part_peak, part_context
                    continue
                top = jnp.maximum(peak[:, first:], part_peak)
                old_factor = jnp.exp(peak[:, first:] - top)
                new_factor = jnp.exp(part_peak - top)
                merged = context[:, first:] * old_factor + part_context * new_factor
                peak = jnp.concatenate([peak[:, :first], top], axis=1)
                context = jnp.concatenate([context[:, :first], merged], axis=1)
            peaks.append(peak)
            totals.append(context[size : size + 1])
            contexts.append(context[:size])
        stacked = jnp.concatenate(contexts, axis=0)
        for index in range(group_chunks):
            low, high = index * rows, (index + 1) * rows
            one, two = low // size, (high - 1) // size
            chunk = group * group_chunks + index
            ctx_ref[chunk] = stacked[low:high].astype(jnp.bfloat16)
            stat_ref[chunk] = jnp.concatenate(
                [peaks[one], peaks[two], totals[one], totals[two]], axis=0
            )

        @pl.loop(0, group_chunks // 2)
        def _(index):
            chunk = group * group_chunks + 2 * index + 1 - lax.rem(me, 2)
            for kind, (src, dst) in enumerate(((stat_ref, pair_stat), (ctx_ref, pair_ctx))):
                pltpu.make_async_remote_copy(
                    src_ref=src.at[chunk],
                    dst_ref=dst.at[chunk // 2],
                    send_sem=send_sem.at[kind],
                    recv_sem=pair_sem.at[kind, turn],
                    device_id={"seq": partner},
                    device_id_type=MESH,
                ).start()

        @pl.when(turn > 0)
        def _():
            pass_sums(turn - 1)

    pass_sums(groups - 1)
    await_bytes(got_stat, chips - 1, recv_sem.at[4])
    await_bytes(got_ctx, chips - 1, recv_sem.at[5])
    await_bytes(sum_stat, chips - 1, send_sem.at[4])
    await_bytes(sum_ctx, chips - 1, send_sem.at[5])
    await_bytes(stat_ref, chips, send_sem.at[0])
    await_bytes(ctx_ref, chips, send_sem.at[1])

    top = lax.fori_loop(
        1, chips, lambda at, best: jnp.maximum(best, got_stat[at][0:2]), got_stat[0][0:2]
    )
    is_one = row + lax.rem(me * rows, size) < size

    def add(at, state):
        total, acc = state
        stat = got_stat[at]
        factor = jnp.exp(stat[0:2] - top)
        spread = jnp.where(is_one, factor[0:1], factor[1:2])
        return total + stat[2:4] * factor, acc + got_ctx[at].astype(jnp.float32) * spread

    total, acc = lax.fori_loop(
        0,
        chips,
        add,
        (jnp.zeros((2, tokens), jnp.float32), jnp.zeros((rows, tokens), jnp.float32)),
    )
    fin_ref[me] = (acc / jnp.where(is_one, total[0:1], total[1:2])).astype(jnp.bfloat16)

    spread(fin_ref, 3, 1)
    relay(fin_ref, 3, 1)
    settle(fin_ref, 3, 1)
    context = rows_together(fin_ref, 0, n).astype(jnp.bfloat16)
    attended = jnp.dot(wout_ref[...], context, preferred_element_type=jnp.float32)
    attended = attended.astype(jnp.bfloat16)
    for step in range(steps):
        out_ref[step] = attended[:, step * per_step : (step + 1) * per_step]


def plain_local(n, frames, dec_states, w_query, w_keyval, w_output, head_slope, lengths, positions):
    steps, frame_count, width = frames.shape
    per_step = dec_states.shape[1]
    tokens = steps * per_step
    heads = head_slope.shape[0]
    size = width // heads
    rows = w_query.shape[1]
    keys = steps * frame_count
    tile = frame_count
    part = math.gcd(width, 256)
    vmem = pl.BlockSpec(memory_space=pltpu.VMEM)
    smem = pl.BlockSpec(memory_space=pltpu.SMEM)
    hbm = pl.BlockSpec(memory_space=pl.ANY)
    out = pl.pallas_call(
        functools.partial(plain_kernel, n),
        out_shape=jax.ShapeDtypeStruct((steps, rows, per_step), jnp.bfloat16),
        in_specs=[vmem, vmem, vmem, vmem, smem, smem, hbm, hbm],
        out_specs=vmem,
        scratch_shapes=[
            pltpu.VMEM((keys // tile, tile, width), jnp.bfloat16),
            pltpu.VMEM((2 * width // part, width, part), jnp.bfloat16),
            pltpu.VMEM((heads, keys, size + EXTRA), jnp.bfloat16),
            pltpu.VMEM((heads, size + EXTRA, keys), jnp.bfloat16),
            pltpu.VMEM((n, rows, tokens), jnp.bfloat16),
            pltpu.VMEM((n, rows, tokens), jnp.bfloat16),
            pltpu.VMEM((n, 4, tokens), jnp.float32),
            pltpu.VMEM((n // 2, rows, tokens), jnp.bfloat16),
            pltpu.VMEM((n // 2, 4, tokens), jnp.float32),
            pltpu.VMEM((n // 2, rows, tokens), jnp.bfloat16),
            pltpu.VMEM((n // 2, 4, tokens), jnp.float32),
            pltpu.VMEM((n // 2, rows, tokens), jnp.bfloat16),
            pltpu.VMEM((n // 2, 4, tokens), jnp.float32),
            pltpu.VMEM((n, rows, tokens), jnp.bfloat16),
            pltpu.SemaphoreType.DMA((keys // tile,)),
            pltpu.SemaphoreType.DMA((2 * width // part,)),
            pltpu.SemaphoreType.DMA((6,)),
            pltpu.SemaphoreType.DMA((6,)),
            pltpu.SemaphoreType.DMA((2, n // 2)),
            pltpu.SemaphoreType.DMA((2, math.gcd(heads, n))),
        ],
        compiler_params=pltpu.CompilerParams(
            collective_id=0, has_side_effects=True, vmem_limit_bytes=60 * 1024 * 1024
        ),
    )(
        dec_states.reshape(tokens, width),
        w_query.T,
        w_output.T,
        positions.reshape(1, tokens),
        head_slope,
        lengths,
        frames,
        w_keyval,
    )
    return out.transpose(0, 2, 1)


GROUPS = ((3, 2), (5, 2), (0, 2), (2, 1), (7, 1), (8, 1), (9, 1))
PLAN = (
    ("K1", "B0", "Q0", "V1", "K2", "V2", "K3", "Q1", "V3", "W0", "K0", "Y0", "A0", "A1", "M0", "W1", "K4", "M1")
    + ("Y1", "A2", "A3", "M2", "C0", "A4", "M3", "C1", "A5", "M4", "A6", "M5", "M6", "C2", "X0", "C3", "X1", "C4")
    + ("R0", "C5", "C6", "R1", "R2", "R3", "R4", "R5")
)
BESIDE = {0: "V0", 2: "V4"}
SHARES = ("column", "column", "relay", "relay", "relay", "relay", "direct")


def paired_kernel(
    n,
    pos_hbm,
    slope_hbm,
    len_hbm,
    dec_hbm,
    wq_hbm,
    wout_hbm,
    frames_hbm,
    wkv_hbm,
    out_ref,
    pos_ref,
    slope_ref,
    len_ref,
    dec_ref,
    wq_ref,
    wout_ref,
    frames_ref,
    wkv_ref,
    k_ref,
    mask_ref,
    vt_ref,
    q_ref,
    ctx_ref,
    stat_ref,
    pair_ctx,
    pair_stat,
    chip_ctx,
    chip_stat,
    got_ctx,
    got_stat,
    fin_ref,
    small_sem,
    frame_sem,
    weight_sem,
    send_sem,
    hop_sem,
    relay_sem,
    pair_sem,
    got_sem,
    fin_sem,
    both_sem,
    side_sem,
):
    me = lax.axis_index("seq")
    core, chip = lax.rem(me, 2), me // 2
    partner = me + 1 - 2 * core
    chips = n // 2
    steps, frame_count, width = frames_hbm.shape
    tokens = dec_hbm.shape[0]
    per_step = tokens // steps
    pairs, lanes = vt_ref.shape[0], vt_ref.shape[1]
    size = lanes // 2
    rows = wq_hbm.shape[0]
    half = wkv_ref.shape[2]
    parts = wkv_ref.shape[0] // 2
    part_pairs = half // lanes
    scale = 1.0 / math.sqrt(size)
    groups = GROUPS
    side, levels = lax.rem(chip, 2), chips // 2
    owners = list(range(chips // 4, chips - chips // 4))

    small = [
        pltpu.make_async_copy(src, dst, small_sem.at[at])
        for at, (src, dst) in enumerate(
            (
                (dec_hbm, dec_ref),
                (wq_hbm, wq_ref),
                (wout_hbm, wout_ref),
                (pos_hbm, pos_ref),
                (slope_hbm, slope_ref),
                (len_hbm, len_ref),
            )
        )
    ]

    def frame_copy(index):
        return pltpu.make_async_copy(frames_hbm.at[index], frames_ref.at[index], frame_sem.at[index])

    def weight_copy(index):
        return pltpu.make_async_copy(
            wkv_hbm.at[:, pl.ds(pl.multiple_of(index * half, half), half)], wkv_ref.at[index], weight_sem.at[index]
        )

    for at in (1, 0, 5, 4, 3):
        small[at].start()
    ordered = [stage if stage[0] in "KV" else BESIDE.get(int(stage[1:]), "B") for stage in PLAN if stage[0] in "KVA"]
    weight_order = [int(stage[1:]) + parts * (stage[0] == "V") for stage in ordered if stage != "B"]
    weight_copy(weight_order[0]).start(priority=1)
    for step in range(steps):
        frame_copy(step).start(priority=1)

    barrier = pltpu.get_barrier_semaphore()

    @pl.loop(1, n)
    def _(step):
        peer = lax.rem(me + step, n)
        pl.semaphore_signal(barrier, inc=1, device_id={"seq": peer}, device_id_type=MESH)

    def remote(src, dst, sent, got, peer):
        return pltpu.make_async_remote_copy(
            src_ref=src,
            dst_ref=dst,
            send_sem=sent,
            recv_sem=got,
            device_id={"seq": peer},
            device_id_type=MESH,
        )

    def await_copy(ref, sem):
        pltpu.make_async_copy(ref, ref, sem).wait()

    def query_rows(device):
        return q_ref.at[pl.ds(pl.multiple_of(device * rows, 16), rows)]

    def await_small():
        for at in (1, 0, 5, 4, 3):
            small[at].wait()

    def project_query():
        own_query = lax.dot_general(
            wq_ref[...], dec_ref[...], (((1,), (1,)), ((), ())), preferred_element_type=jnp.float32
        )
        q_ref[pl.ds(pl.multiple_of(me * rows, 16), rows), :] = own_query.astype(jnp.bfloat16)

    def await_barrier(_):
        for index in weight_order[4:]:
            weight_copy(index).start(priority=1)
        small[2].start(priority=1)
        pl.semaphore_wait(barrier, n - 1)

    await_small()
    project_query()

    middle = chips // 4
    wave_chips = (
        list(range(middle, chips - middle)),
        list(range(middle)) + list(range(chips - middle, chips)),
    )
    is_middle = (chip >= middle) & (chip < chips - middle)

    def query_relay(device, wave):
        block = query_rows(device)
        remote(block, block, send_sem.at[1], relay_sem.at[wave], partner).start()

    def spread_queries(wave):
        @pl.when(is_middle if wave == 0 else jnp.logical_not(is_middle))
        def _():
            own = query_rows(me)

            @pl.loop(1, chips)
            def _(step):
                remote(own, own, send_sem.at[0], hop_sem.at[chip], lax.rem(me + 2 * step, n)).start()

            query_relay(me, wave)

    def relay_queries(wave):
        for source in wave_chips[wave]:

            @pl.when(source != chip)
            def _():
                await_copy(query_rows(me), hop_sem.at[source])
                query_relay(2 * source + core, wave)

    def await_queries(wave):
        await_copy(q_ref.at[pl.ds(0, rows * len(wave_chips[wave]))], relay_sem.at[wave])

    place = lax.broadcasted_iota(jnp.int32, (frame_count, lanes), 0)
    column = lax.broadcasted_iota(jnp.int32, (frame_count, lanes), 1)
    for older in range(steps):
        hidden = (place >= len_ref[older, me]) & (column == 0)
        mask_ref[older * frame_count : (older + 1) * frame_count, :] = jnp.where(hidden, MASKED, 0.0).astype(
            jnp.bfloat16
        )

    def keys_piece(part, step, begin, stop):
        keys = jnp.dot(
            frames_ref[step, begin:stop, :], wkv_ref[part], preferred_element_type=jnp.float32
        ).astype(jnp.bfloat16)
        at = slice(step * frame_count + begin, step * frame_count + stop)
        for index in range(part_pairs):
            k_ref[part * part_pairs + index, at, :] = keys[:, index * lanes : (index + 1) * lanes]

    def values_piece(part, step, begin, stop):
        values = jnp.dot(
            frames_ref[step, begin:stop, :], wkv_ref[parts + part], preferred_element_type=jnp.float32
        )
        turned = values.astype(jnp.bfloat16).T
        at = slice(step * frame_count + begin, step * frame_count + stop)
        for index in range(part_pairs):
            vt_ref[part * part_pairs + index, :, at] = turned[index * lanes : (index + 1) * lanes]

    def project(kind, part, cuts):
        piece = keys_piece if kind == "K" else values_piece
        return [
            functools.partial(piece, part, step, begin, stop)
            for step in range(steps)
            for begin, stop in zip(cuts, cuts[1:])
        ]

    def project_keys(part):
        weight_copy(part).wait()
        for piece in project("K", part, (0, frame_count)):
            piece()

    def project_values(part):
        weight_copy(parts + part).wait()
        for piece in project("V", part, (0, frame_count)):
            piece()

    def await_frames():
        for step in range(steps):
            frame_copy(step).wait()

    for index in weight_order[1:4]:
        weight_copy(index).start(priority=1)
    await_frames()

    slot_place = lax.rem(me + 1, n).astype(jnp.float32)
    distance = jnp.abs(pos_ref[...].astype(jnp.float32) - slot_place) / n
    tail_row = lax.broadcasted_iota(jnp.int32, (lanes, tokens), 0) == 0
    tail = jnp.where(tail_row, 1.0, 0.0).astype(jnp.bfloat16)
    blank = jnp.zeros((size, tokens), jnp.bfloat16)
    ones = jnp.ones((EXTRA, frame_count), jnp.bfloat16)
    first, second = slice(0, frame_count), slice(frame_count, 2 * frame_count)
    early, late = slice(0, per_step), slice(per_step, tokens)

    def attend_scores(pair):
        query = q_ref[pl.ds(pl.multiple_of(pair * lanes, lanes), lanes), :]
        one = jnp.concatenate([query[:size], blank, tail], axis=0)
        two = jnp.concatenate([blank, query[size:], tail], axis=0)
        both = jnp.concatenate([one[:, late], two[:, late]], axis=1)
        old = jnp.concatenate([k_ref[pair, first, :], mask_ref[first, :]], axis=1)
        new = jnp.concatenate([k_ref[pair, second, :], mask_ref[second, :]], axis=1)
        return [
            functools.partial(jnp.dot, keys, queries, preferred_element_type=jnp.float32)
            for keys, queries in ((old, one), (old, two), (new, both))
        ]

    def soften(raw):
        peak = jnp.max(raw, axis=0, keepdims=True)
        weights = jnp.exp2((raw - peak) * (scale * math.log2(math.e)))
        return peak * scale, weights.astype(jnp.bfloat16)

    def attend_values(pair, kind):
        if kind == 2:
            stack = [vt_ref[pair, :, second], ones]
        else:
            stack = [vt_ref[pair, kind * size : (kind + 1) * size, first], ones]
        return jnp.concatenate(stack, axis=0)

    def attend(group):
        first_pair, count = groups[group]
        beside = []
        if group in BESIDE:
            kind, part = BESIDE[group][0], int(BESIDE[group][1:])
            weight_copy(part + parts * (kind == "V")).wait()
            half_frames = frame_count // 256 * 128
            beside = project(kind, part, (0, half_frames, frame_count))
        dots = []
        for local_pair in range(count):
            dots += [(local_pair, kind, call) for kind, call in enumerate(attend_scores(first_pair + local_pair))]
        results = {}
        ready = [dots[0][2](), dots[1][2]()]
        for at, (local_pair, kind, _) in enumerate(dots):
            raw = ready.pop(0)
            if at + 2 < len(dots):
                ready.append(dots[at + 2][2]())
            if beside:
                beside.pop(0)()
            peak, weights = soften(raw)
            values = attend_values(first_pair + local_pair, kind)
            results[local_pair, kind] = peak, jnp.dot(values, weights, preferred_element_type=jnp.float32)
        for piece in beside:
            piece()
        peaks = [[], []]
        totals = [[], []]
        for local_pair in range(count):
            pair = first_pair + local_pair
            new_peaks, new_context = results[local_pair, 2]
            for which in range(2):
                slope = slope_ref[2 * pair + which]
                at = pl.ds(pl.multiple_of(pair * lanes + which * size, size), size)
                peak, context = results[local_pair, which]
                peaks[0].append(peak[:, early] - slope * distance[:, early])
                totals[0].append(context[size : size + 1, early])
                ctx_ref[0, at, :] = context[:size, early].astype(jnp.bfloat16)
                span = slice(which * per_step, (which + 1) * per_step)
                old_peak = peak[:, late] - slope * (distance[:, late] + 1.0)
                new_peak = new_peaks[:, span] - slope * distance[:, late]
                top = jnp.maximum(old_peak, new_peak)
                old_factor, new_factor = jnp.exp(old_peak - top), jnp.exp(new_peak - top)
                own = slice(which * size, (which + 1) * size)
                merged = context[:size, late] * old_factor + new_context[own, span] * new_factor
                ctx_ref[1, at, :] = merged.astype(jnp.bfloat16)
                peaks[1].append(top)
                old_total = context[size : size + 1, late] * old_factor
                totals[1].append(old_total + new_context[lanes : lanes + 1, span] * new_factor)
        for step in range(2):
            stat_ref[step, group, 0 : 4 * count, :] = jnp.concatenate(peaks[step] + totals[step], axis=0)
        block = pl.ds(pl.multiple_of(first_pair * lanes, lanes), count * lanes)
        other = 1 - core
        remote(
            stat_ref.at[other, group], pair_stat.at[group], send_sem.at[2], pair_sem.at[0, group], partner
        ).start()
        remote(
            ctx_ref.at[other, block], pair_ctx.at[block], send_sem.at[3], pair_sem.at[1, group], partner
        ).start()

    def slices(first_pair, count):
        part_rows = count * lanes // len(owners)
        base = first_pair * lanes

        def place(owner):
            return owner % 2 * (levels // 2) + owner // 2 - levels // 4

        def block(owner):
            return pl.ds(pl.multiple_of(base + place(owner) * part_rows, 16), part_rows)

        slot = pl.ds(pl.multiple_of(base // len(owners), 16), part_rows)
        return part_rows, place, block, slot

    def mix(one, two, heads):
        top = jnp.maximum(one[:heads], two[:heads])
        one_factor, two_factor = jnp.exp(one[:heads] - top), jnp.exp(two[:heads] - top)
        total = one[heads : 2 * heads] * one_factor + two[heads : 2 * heads] * two_factor
        return top, total, one_factor, two_factor

    def merge_cores(group):
        first_pair, count = groups[group]
        part_rows, place, block, slot = slices(first_pair, count)
        heads = 2 * count
        await_copy(pair_stat.at[group], pair_sem.at[0, group])
        await_copy(pair_ctx.at[pl.ds(0, count * lanes)], pair_sem.at[1, group])
        top, total, one_factor, two_factor = mix(stat_ref[core, group], pair_stat[group], heads)
        for head in range(heads):
            at = slice(first_pair * lanes + head * size, first_pair * lanes + (head + 1) * size)
            merged = (
                ctx_ref[core, at, :].astype(jnp.float32) * one_factor[head : head + 1]
                + pair_ctx[at, :].astype(jnp.float32) * two_factor[head : head + 1]
            )
            chip_ctx[at, :] = merged.astype(jnp.bfloat16)
        for owner in owners:
            head = place(owner) * part_rows // size
            chip_stat[group, owner] = jnp.concatenate([top[head : head + 1], total[head : head + 1]], axis=0)

            @pl.when(owner != chip)
            def _():
                peer = 2 * owner + core
                remote(
                    chip_stat.at[group, owner],
                    got_stat.at[group, chip],
                    send_sem.at[4],
                    got_sem.at[0, group],
                    peer,
                ).start()
                remote(
                    chip_ctx.at[block(owner)], got_ctx.at[chip, slot], send_sem.at[5], got_sem.at[1, group], peer
                ).start()

        @pl.when(is_middle)
        def _():
            got_stat[group, chip] = chip_stat[group, chip]
            got_ctx[chip, slot, :] = chip_ctx[block(chip), :]

    def merge_chips(group):
        pl.when(is_middle)(functools.partial(own_rows, group))

    def own_rows(group):
        first_pair, count = groups[group]
        mode = SHARES[group]
        part_rows, _, block, slot = slices(first_pair, count)
        await_copy(got_stat.at[group, pl.ds(0, chips - 1)], got_sem.at[0, group])
        await_copy(got_ctx.at[pl.ds(0, chips - 1), pl.ds(0, part_rows)], got_sem.at[1, group])
        stats = [got_stat[group, source] for source in range(chips)]
        top = stats[0][0:1]
        for stat in stats[1:]:
            top = jnp.maximum(top, stat[0:1])
        total = context = None
        for source, stat in enumerate(stats):
            factor = jnp.exp(stat[0:1] - top)
            part_total = stat[1:2] * factor
            part_context = got_ctx[source, slot, :].astype(jnp.float32) * factor
            total = part_total if total is None else total + part_total
            context = part_context if context is None else context + part_context
        fin_ref[core, block(chip), :] = (context / total).astype(jnp.bfloat16)
        own = fin_ref.at[core, block(chip)]
        if mode == "direct":

            @pl.loop(1, n)
            def _(step):
                remote(own, own, send_sem.at[7], fin_sem.at[group], lax.rem(me + step, n)).start()

        else:
            stride = 4 if mode == "column" else 2

            @pl.loop(1, n // stride)
            def _(step):
                remote(
                    own, own, send_sem.at[6], fin_sem.at[group], lax.rem(me + stride * step, n)
                ).start()

    def group_rows(group):
        first_pair, count = groups[group]
        return slice(first_pair * lanes, (first_pair + count) * lanes)

    def await_middle(ref, unit, amount, sem):
        @pl.when(is_middle)
        def _():
            await_copy(ref.at[pl.ds(0, unit * (amount - 1))], sem)

        @pl.when(jnp.logical_not(is_middle))
        def _():
            await_copy(ref.at[pl.ds(0, unit * amount)], sem)

    def await_slices(group, amount):
        unit = groups[group][1] * lanes // len(owners)
        await_middle(fin_ref.at[0], unit, amount, fin_sem.at[group])

    def side_rows(group, which):
        first_pair, count = groups[group]
        span = count * lanes // 2
        return pl.ds(pl.multiple_of(first_pair * lanes + which * span, 16), span)

    def cross(group):
        await_slices(group, levels // 2)
        block = fin_ref.at[core, side_rows(group, side)]
        remote(block, block, send_sem.at[9], side_sem.at[group], me + 2 - 4 * side).start()

    def relay(group):
        if SHARES[group] == "column":
            await_copy(fin_ref.at[0, pl.ds(0, groups[group][1] * lanes // 2)], side_sem.at[group])
        else:
            await_slices(group, len(owners))
        block = fin_ref.at[core, group_rows(group)]
        remote(block, block, send_sem.at[8], both_sem.at[group], partner).start()

    stages = {
        "K": project_keys,
        "V": project_values,
        "B": await_barrier,
        "Q": spread_queries,
        "W": relay_queries,
        "Y": await_queries,
        "A": attend,
        "M": merge_cores,
        "C": merge_chips,
        "X": cross,
        "R": relay,
    }
    for stage in PLAN:
        stages[stage[0]](int(stage[1:]))

    def await_both(group):
        await_copy(fin_ref.at[0, group_rows(group)], both_sem.at[group])

    small[2].wait()
    direct = [group for group, mode in enumerate(SHARES) if mode == "direct"]
    for group in range(direct[0]):
        await_both(group)

    def attended(begin, stop):
        context = jnp.concatenate([fin_ref[0, begin:stop, :], fin_ref[1, begin:stop, :]], axis=1)
        return jnp.dot(wout_ref[:, begin:stop], context, preferred_element_type=jnp.float32)

    late_row = groups[direct[0]][0] * lanes
    total = attended(0, late_row)
    for group in direct:
        await_slices(group, 2 * len(owners))
    total = total + attended(late_row, width)
    total = total.astype(jnp.bfloat16)
    for step in range(steps):
        out_ref[step] = total[:, step * per_step : (step + 1) * per_step]

    def sent(amount, sem):
        await_copy(q_ref.at[pl.ds(0, amount // 2)], send_sem.at[sem])

    share_rows = {mode: 0 for mode in SHARES}
    for (_, count), shared in zip(groups, SHARES):
        share_rows[shared] += count * lanes // len(owners)
    await_copy(q_ref.at[pl.ds(0, rows * (chips - 1))], send_sem.at[0])
    await_copy(q_ref.at[pl.ds(0, rows * chips)], send_sem.at[1])
    await_copy(stat_ref.at[0], send_sem.at[2])
    await_copy(ctx_ref.at[0], send_sem.at[3])
    @pl.when(is_middle)
    def _():
        await_copy(chip_stat.at[:, pl.ds(0, len(owners) - 1)], send_sem.at[4])

    @pl.when(jnp.logical_not(is_middle))
    def _():
        await_copy(chip_stat.at[:, pl.ds(0, len(owners))], send_sem.at[4])

    await_middle(fin_ref.at[0], width // len(owners), len(owners), send_sem.at[5])

    @pl.when(is_middle)
    def _():
        sent((levels - 1) * share_rows["column"] + (chips - 1) * share_rows["relay"], 6)
        sent((n - 1) * share_rows["direct"], 7)

    sent(late_row, 8)
    sent(share_rows["column"] * len(owners) // 2, 9)


def paired_local(n, frames, dec_states, w_query, w_keyval, w_output, head_slope, lengths, positions):
    steps, frame_count, width = frames.shape
    per_step = dec_states.shape[1]
    tokens = steps * per_step
    heads = head_slope.shape[0]
    lanes = 2 * (width // heads)
    pairs = heads // 2
    rows = w_query.shape[1]
    keys = steps * frame_count
    part = 2 * lanes
    chips = n // 2
    groups = len(GROUPS)
    vmem = pl.BlockSpec(memory_space=pltpu.VMEM)
    hbm = pl.BlockSpec(memory_space=pltpu.HBM)
    out = pl.pallas_call(
        functools.partial(paired_kernel, n),
        out_shape=pltpu.VMEM((steps, rows, per_step), jnp.bfloat16),
        in_specs=[hbm] * 8,
        out_specs=vmem,
        scratch_shapes=[
            pltpu.VMEM((1, tokens), jnp.int32),
            pltpu.SMEM((heads,), jnp.float32),
            pltpu.SMEM(lengths.shape, jnp.int32),
            pltpu.VMEM((tokens, width), jnp.bfloat16),
            pltpu.VMEM((rows, width), jnp.bfloat16),
            pltpu.VMEM((rows, width), jnp.bfloat16),
            pltpu.VMEM((steps, frame_count, width), jnp.bfloat16),
            pltpu.VMEM((2 * width // part, width, part), jnp.bfloat16),
            pltpu.VMEM((pairs, keys, lanes), jnp.bfloat16),
            pltpu.VMEM((keys, lanes), jnp.bfloat16),
            pltpu.VMEM((pairs, lanes, keys), jnp.bfloat16),
            pltpu.VMEM((width, tokens), jnp.bfloat16),
            pltpu.VMEM((2, width, per_step), jnp.bfloat16),
            pltpu.VMEM((2, groups, 8, per_step), jnp.float32),
            pltpu.VMEM((width, per_step), jnp.bfloat16),
            pltpu.VMEM((groups, 8, per_step), jnp.float32),
            pltpu.VMEM((width, per_step), jnp.bfloat16),
            pltpu.VMEM((groups, chips, 2, per_step), jnp.float32),
            pltpu.VMEM((chips, 2 * width // chips, per_step), jnp.bfloat16),
            pltpu.VMEM((groups, chips, 2, per_step), jnp.float32),
            pltpu.VMEM((2, width, per_step), jnp.bfloat16),
            pltpu.SemaphoreType.DMA((6,)),
            pltpu.SemaphoreType.DMA((steps,)),
            pltpu.SemaphoreType.DMA((2 * width // part,)),
            pltpu.SemaphoreType.DMA((10,)),
            pltpu.SemaphoreType.DMA((chips,)),
            pltpu.SemaphoreType.DMA((2,)),
            pltpu.SemaphoreType.DMA((2, groups)),
            pltpu.SemaphoreType.DMA((2, groups)),
            pltpu.SemaphoreType.DMA((groups,)),
            pltpu.SemaphoreType.DMA((groups,)),
            pltpu.SemaphoreType.DMA((groups,)),
        ],
        compiler_params=pltpu.CompilerParams(
            collective_id=0, has_side_effects=True, vmem_limit_bytes=40 * 1024 * 1024
        ),
    )(
        *(
            pltpu.with_memory_space_constraint(value, pltpu.HBM)
            for value in (
                positions.reshape(1, tokens),
                head_slope,
                lengths,
                dec_states.reshape(tokens, width),
                w_query.T,
                w_output.T,
                frames,
                w_keyval,
            )
        )
    )
    return out.transpose(0, 2, 1)


def fits_pairs(n, frames, dec_states, w_query, head_slope):
    steps, frame_count, width = frames.shape
    per_step, heads = dec_states.shape[1], head_slope.shape[0]
    size = width // heads
    chips = n // 2
    return (
        steps == 2
        and n % 4 == 0
        and heads % 4 == 0
        and heads // 2 == sum(count for _, count in GROUPS)
        and n % 16 == 0
        and size == 64
        and per_step == 2 * size
        and frame_count % 128 == 0
        and w_query.shape[1] % 16 == 0
        and (2 * size) % (16 * chips) == 0
    )


def local(n, frames, dec_states, w_query, w_keyval, w_output, head_slope, lengths, positions):
    paired = fits_pairs(n, frames, dec_states, w_query, head_slope)
    run = paired_local if paired else plain_local
    return run(n, frames, dec_states, w_query, w_keyval, w_output, head_slope, lengths, positions)


def solution(mesh):
    return jax.shard_map(
        functools.partial(local, mesh.shape["seq"]),
        mesh=mesh,
        in_specs=(
            P("grp", "seq", None),
            P(None, "grp", None),
            P(None, "seq"),
            P(),
            P(None, "seq"),
            P(),
            P("grp", None),
            P(None, "grp"),
        ),
        out_specs=P(None, "grp", "seq"),
        check_vma=False,
    )
```

```python
import functools
import math

import jax
import jax.numpy as jnp
from jax import lax
from jax.experimental import pallas as pl
from jax.experimental.pallas import tpu as pltpu
from jax.sharding import PartitionSpec as P

MESH = pl.DeviceIdType.MESH
EXTRA = 16
MASKED = -1e30


def rows_together(ref, first, count):
    parts = [ref[first + index].astype(jnp.float32) for index in range(count)]
    return jnp.concatenate(parts, axis=0)


def await_bytes(ref, count, sem):
    part = ref.at[pl.ds(0, count)]
    pltpu.make_async_copy(part, part, sem).wait()


def plain_kernel(
    n,
    dec_ref,
    wq_ref,
    wout_ref,
    pos_ref,
    slope_ref,
    len_ref,
    frames_hbm,
    wkv_hbm,
    out_ref,
    frames_ref,
    wkv_ref,
    k_ref,
    vt_ref,
    q_ref,
    ctx_ref,
    stat_ref,
    got_ctx,
    got_stat,
    pair_ctx,
    pair_stat,
    sum_ctx,
    sum_stat,
    fin_ref,
    frame_sem,
    weight_sem,
    send_sem,
    recv_sem,
    hop_sem,
    pair_sem,
):
    me = lax.axis_index("seq")
    steps, frame_count, width = frames_hbm.shape
    tokens = dec_ref.shape[0]
    per_step = tokens // steps
    heads = k_ref.shape[0]
    size = width // heads
    rows = wq_ref.shape[0]
    groups = math.gcd(heads, n)
    group_chunks = n // groups
    group_heads = heads // groups
    tile = frames_ref.shape[1]
    half = wkv_ref.shape[2]
    tiles = frames_ref.shape[0]
    per_block = frame_count // tile
    scale = 1.0 / math.sqrt(size)

    def frame_copy(index):
        return pltpu.make_async_copy(
            frames_hbm.at[index // per_block, pl.ds((index % per_block) * tile, tile)],
            frames_ref.at[index],
            frame_sem.at[index],
        )

    def weight_copy(index):
        return pltpu.make_async_copy(
            wkv_hbm.at[:, pl.ds(pl.multiple_of(index * half, half), half)], wkv_ref.at[index], weight_sem.at[index]
        )

    frame_copy(0).start()
    weight_copy(0).start()
    for index in range(1, tiles):
        frame_copy(index).start()
    for index in range(1, wkv_ref.shape[0]):
        weight_copy(index).start()

    barrier = pltpu.get_barrier_semaphore()

    @pl.loop(1, n)
    def _(step):
        peer = lax.rem(me + step, n)
        pl.semaphore_signal(barrier, inc=1, device_id={"seq": peer}, device_id_type=MESH)

    own_query = lax.dot_general(
        wq_ref[...], dec_ref[...], (((1,), (1,)), ((), ())), preferred_element_type=jnp.float32
    )
    q_ref[me] = own_query.astype(jnp.bfloat16)
    pl.semaphore_wait(barrier, n - 1)

    def send(src, dst, sem, peer):
        pltpu.make_async_remote_copy(
            src_ref=src,
            dst_ref=dst,
            send_sem=send_sem.at[sem],
            recv_sem=recv_sem.at[sem],
            device_id={"seq": peer},
            device_id_type=MESH,
        ).start()

    partner = me + 1 - 2 * lax.rem(me, 2)
    chips = n // 2

    def pass_on(ref, chunk, sem):
        send(ref.at[chunk], ref.at[chunk], sem, partner)

    def hop(ref, step, sem, level):
        return pltpu.make_async_remote_copy(
            src_ref=ref.at[me],
            dst_ref=ref.at[me],
            send_sem=send_sem.at[sem],
            recv_sem=hop_sem.at[level, step],
            device_id={"seq": lax.rem(me + 2 * step, n)},
            device_id_type=MESH,
        )

    def spread(ref, sem, level):
        @pl.loop(1, chips)
        def _(step):
            hop(ref, step, sem, level).start()

        pass_on(ref, me, level)

    def relay(ref, sem, level):
        @pl.loop(1, chips)
        def _(step):
            hop(ref, step, sem, level).wait_recv()
            pass_on(ref, lax.rem(me - 2 * step + n, n), level)

    def settle(ref, sem, level):
        await_bytes(ref, chips - 1, send_sem.at[sem])
        await_bytes(ref, chips, recv_sem.at[level])
        await_bytes(ref, chips, send_sem.at[level])

    spread(q_ref, 2, 0)

    column = lax.broadcasted_iota(jnp.int32, (frame_count, size + EXTRA), 1)
    place = lax.broadcasted_iota(jnp.int32, (frame_count, size + EXTRA), 0)
    masks = []
    for older in range(steps):
        hidden = (place >= len_ref[older, me]) & (column == size)
        masks.append(jnp.where(hidden, MASKED, 0.0).astype(jnp.bfloat16))
    mask = jnp.concatenate(masks, axis=0)
    ones = jnp.ones((EXTRA, steps * frame_count), jnp.bfloat16)

    @pl.loop(0, heads)
    def _(head):
        k_ref[head] = mask
        vt_ref[head, size:, :] = ones

    parts = wkv_ref.shape[0] // 2
    part_heads = half // size

    def project(part, index):
        at = pl.ds(pl.multiple_of(index * tile, tile), tile)
        keyval = jnp.dot(frames_ref[index], wkv_ref[part], preferred_element_type=jnp.float32)
        return at, keyval.astype(jnp.bfloat16)

    for index in range(tiles):
        frame_copy(index).wait()

    @pl.loop(0, parts)
    def _(part):
        weight_copy(part).wait()
        for index in range(tiles):
            at, keyval = project(part, index)
            for local_head in range(part_heads):
                lanes = slice(local_head * size, (local_head + 1) * size)
                k_ref[part * part_heads + local_head, at, 0:size] = keyval[:, lanes]

    def project_values(part):
        weight_copy(parts + part).wait()
        for index in range(tiles):
            at, keyval = project(parts + part, index)
            turned = keyval.T
            for local_head in range(part_heads):
                lanes = slice(local_head * size, (local_head + 1) * size)
                vt_ref[part * part_heads + local_head, 0:size, at] = turned[lanes]

    pl.loop(0, parts - 2)(project_values)
    relay(q_ref, 2, 0)
    pl.loop(parts - 2, parts)(project_values)
    settle(q_ref, 2, 0)

    slot_place = lax.rem(me + 1, n).astype(jnp.float32)
    distance = jnp.abs(pos_ref[...].astype(jnp.float32) - slot_place) / n
    first_row = lax.broadcasted_iota(jnp.int32, (EXTRA, tokens), 0) == 0
    query_tail = jnp.where(first_row, 1.0, 0.0).astype(jnp.bfloat16)
    token_step = lax.broadcasted_iota(jnp.int32, (1, tokens), 1) // per_step

    row = lax.broadcasted_iota(jnp.int32, (rows, tokens), 0)

    def pass_sums(turn):
        group = lax.rem(me // group_chunks + 1 + turn, groups)
        await_bytes(pair_stat, group_chunks // 2, pair_sem.at[0, turn])
        await_bytes(pair_ctx, group_chunks // 2, pair_sem.at[1, turn])

        @pl.loop(0, group_chunks // 2)
        def _(index):
            chunk = group * group_chunks + 2 * index + lax.rem(me, 2)
            slot = chunk // 2
            one, two = stat_ref[chunk], pair_stat[slot]
            top = jnp.maximum(one[0:2], two[0:2])
            one_factor = jnp.exp(one[0:2] - top)
            two_factor = jnp.exp(two[0:2] - top)
            stat = jnp.concatenate([top, one[2:4] * one_factor + two[2:4] * two_factor], axis=0)
            is_one = row + lax.rem(chunk * rows, size) < size
            context = ctx_ref[chunk].astype(jnp.float32) * jnp.where(
                is_one, one_factor[0:1], one_factor[1:2]
            ) + pair_ctx[slot].astype(jnp.float32) * jnp.where(
                is_one, two_factor[0:1], two_factor[1:2]
            )
            context = context.astype(jnp.bfloat16)

            @pl.when(chunk != me)
            def _():
                sum_stat[slot] = stat
                sum_ctx[slot] = context
                send(sum_stat.at[slot], got_stat.at[me // 2], 4, chunk)
                send(sum_ctx.at[slot], got_ctx.at[me // 2], 5, chunk)

            @pl.when(chunk == me)
            def _():
                got_stat[slot] = stat
                got_ctx[slot] = context

    @pl.loop(0, groups)
    def _(turn):
        group = lax.rem(me // group_chunks + 1 + turn, groups)
        query_rows = rows_together(q_ref, group * group_chunks, group_chunks).astype(jnp.bfloat16)
        peaks, totals, contexts = [], [], []

        def scores(local_head):
            query = jnp.concatenate(
                [query_rows[local_head * size : (local_head + 1) * size], query_tail], axis=0
            )
            return [
                jnp.dot(
                    k_ref[
                        group * group_heads + local_head,
                        pl.ds(older * frame_count, frame_count),
                        :,
                    ],
                    query[:, older * per_step :],
                    preferred_element_type=jnp.float32,
                )
                for older in range(steps)
            ]

        ready = scores(0)
        for local_head in range(group_heads):
            head = group * group_heads + local_head
            raws = ready
            if local_head + 1 < group_heads:
                ready = scores(local_head + 1)
            slope = slope_ref[head]
            peak = context = None
            for older in range(steps):
                first = older * per_step
                block = pl.ds(older * frame_count, frame_count)
                raw = raws[older]
                raw_peak = jnp.max(raw, axis=0, keepdims=True)
                weights = jnp.exp2((raw - raw_peak) * (scale * math.log2(math.e)))
                part_context = jnp.dot(
                    vt_ref[head, :, block],
                    weights.astype(jnp.bfloat16),
                    preferred_element_type=jnp.float32,
                )
                age = (token_step[:, first:] - older).astype(jnp.float32)
                part_peak = raw_peak * scale - slope * (distance[:, first:] + age)
                if peak is None:
                    peak, context = part_peak, part_context
                    continue
                top = jnp.maximum(peak[:, first:], part_peak)
                old_factor = jnp.exp(peak[:, first:] - top)
                new_factor = jnp.exp(part_peak - top)
                merged = context[:, first:] * old_factor + part_context * new_factor
                peak = jnp.concatenate([peak[:, :first], top], axis=1)
                context = jnp.concatenate([context[:, :first], merged], axis=1)
            peaks.append(peak)
            totals.append(context[size : size + 1])
            contexts.append(context[:size])
        stacked = jnp.concatenate(contexts, axis=0)
        for index in range(group_chunks):
            low, high = index * rows, (index + 1) * rows
            one, two = low // size, (high - 1) // size
            chunk = group * group_chunks + index
            ctx_ref[chunk] = stacked[low:high].astype(jnp.bfloat16)
            stat_ref[chunk] = jnp.concatenate(
                [peaks[one], peaks[two], totals[one], totals[two]], axis=0
            )

        @pl.loop(0, group_chunks // 2)
        def _(index):
            chunk = group * group_chunks + 2 * index + 1 - lax.rem(me, 2)
            for kind, (src, dst) in enumerate(((stat_ref, pair_stat), (ctx_ref, pair_ctx))):
                pltpu.make_async_remote_copy(
                    src_ref=src.at[chunk],
                    dst_ref=dst.at[chunk // 2],
                    send_sem=send_sem.at[kind],
                    recv_sem=pair_sem.at[kind, turn],
                    device_id={"seq": partner},
                    device_id_type=MESH,
                ).start()

        @pl.when(turn > 0)
        def _():
            pass_sums(turn - 1)

    pass_sums(groups - 1)
    await_bytes(got_stat, chips - 1, recv_sem.at[4])
    await_bytes(got_ctx, chips - 1, recv_sem.at[5])
    await_bytes(sum_stat, chips - 1, send_sem.at[4])
    await_bytes(sum_ctx, chips - 1, send_sem.at[5])
    await_bytes(stat_ref, chips, send_sem.at[0])
    await_bytes(ctx_ref, chips, send_sem.at[1])

    top = lax.fori_loop(
        1, chips, lambda at, best: jnp.maximum(best, got_stat[at][0:2]), got_stat[0][0:2]
    )
    is_one = row + lax.rem(me * rows, size) < size

    def add(at, state):
        total, acc = state
        stat = got_stat[at]
        factor = jnp.exp(stat[0:2] - top)
        spread = jnp.where(is_one, factor[0:1], factor[1:2])
        return total + stat[2:4] * factor, acc + got_ctx[at].astype(jnp.float32) * spread

    total, acc = lax.fori_loop(
        0,
        chips,
        add,
        (jnp.zeros((2, tokens), jnp.float32), jnp.zeros((rows, tokens), jnp.float32)),
    )
    fin_ref[me] = (acc / jnp.where(is_one, total[0:1], total[1:2])).astype(jnp.bfloat16)

    spread(fin_ref, 3, 1)
    relay(fin_ref, 3, 1)
    settle(fin_ref, 3, 1)
    context = rows_together(fin_ref, 0, n).astype(jnp.bfloat16)
    attended = jnp.dot(wout_ref[...], context, preferred_element_type=jnp.float32)
    attended = attended.astype(jnp.bfloat16)
    for step in range(steps):
        out_ref[step] = attended[:, step * per_step : (step + 1) * per_step]


def plain_local(n, frames, dec_states, w_query, w_keyval, w_output, head_slope, lengths, positions):
    steps, frame_count, width = frames.shape
    per_step = dec_states.shape[1]
    tokens = steps * per_step
    heads = head_slope.shape[0]
    size = width // heads
    rows = w_query.shape[1]
    keys = steps * frame_count
    tile = frame_count
    part = math.gcd(width, 256)
    vmem = pl.BlockSpec(memory_space=pltpu.VMEM)
    smem = pl.BlockSpec(memory_space=pltpu.SMEM)
    hbm = pl.BlockSpec(memory_space=pl.ANY)
    out = pl.pallas_call(
        functools.partial(plain_kernel, n),
        out_shape=jax.ShapeDtypeStruct((steps, rows, per_step), jnp.bfloat16),
        in_specs=[vmem, vmem, vmem, vmem, smem, smem, hbm, hbm],
        out_specs=vmem,
        scratch_shapes=[
            pltpu.VMEM((keys // tile, tile, width), jnp.bfloat16),
            pltpu.VMEM((2 * width // part, width, part), jnp.bfloat16),
            pltpu.VMEM((heads, keys, size + EXTRA), jnp.bfloat16),
            pltpu.VMEM((heads, size + EXTRA, keys), jnp.bfloat16),
            pltpu.VMEM((n, rows, tokens), jnp.bfloat16),
            pltpu.VMEM((n, rows, tokens), jnp.bfloat16),
            pltpu.VMEM((n, 4, tokens), jnp.float32),
            pltpu.VMEM((n // 2, rows, tokens), jnp.bfloat16),
            pltpu.VMEM((n // 2, 4, tokens), jnp.float32),
            pltpu.VMEM((n // 2, rows, tokens), jnp.bfloat16),
            pltpu.VMEM((n // 2, 4, tokens), jnp.float32),
            pltpu.VMEM((n // 2, rows, tokens), jnp.bfloat16),
            pltpu.VMEM((n // 2, 4, tokens), jnp.float32),
            pltpu.VMEM((n, rows, tokens), jnp.bfloat16),
            pltpu.SemaphoreType.DMA((keys // tile,)),
            pltpu.SemaphoreType.DMA((2 * width // part,)),
            pltpu.SemaphoreType.DMA((6,)),
            pltpu.SemaphoreType.DMA((6,)),
            pltpu.SemaphoreType.DMA((2, n // 2)),
            pltpu.SemaphoreType.DMA((2, math.gcd(heads, n))),
        ],
        compiler_params=pltpu.CompilerParams(
            collective_id=0, has_side_effects=True, vmem_limit_bytes=60 * 1024 * 1024
        ),
    )(
        dec_states.reshape(tokens, width),
        w_query.T,
        w_output.T,
        positions.reshape(1, tokens),
        head_slope,
        lengths,
        frames,
        w_keyval,
    )
    return out.transpose(0, 2, 1)


GROUPS = ((3, 2), (5, 2), (0, 2), (2, 1), (7, 1), (8, 1), (9, 1))
PLAN = (
    ("K1", "B0", "Q0", "V1", "K2", "V2", "K3", "Q1", "V3", "W0", "K0", "Y0", "A0", "A1", "M0", "W1", "K4", "M1")
    + ("Y1", "A2", "A3", "M2", "C0", "A4", "M3", "C1", "A5", "M4", "A6", "M5", "M6", "C2", "X0", "C3", "X1", "C4")
    + ("R0", "C5", "C6", "R1", "R2", "R3", "R4", "R5")
)
BESIDE = {0: "V0", 2: "V4"}
SHARES = ("column", "column", "relay", "relay", "relay", "relay", "direct")


def paired_kernel(
    n,
    pos_hbm,
    slope_hbm,
    len_hbm,
    dec_hbm,
    wq_hbm,
    wout_hbm,
    frames_hbm,
    wkv_hbm,
    out_ref,
    pos_ref,
    slope_ref,
    len_ref,
    dec_ref,
    wq_ref,
    wout_ref,
    frames_ref,
    wkv_ref,
    k_ref,
    mask_ref,
    vt_ref,
    q_ref,
    ctx_ref,
    stat_ref,
    pair_ctx,
    pair_stat,
    chip_ctx,
    chip_stat,
    got_ctx,
    got_stat,
    fin_ref,
    small_sem,
    frame_sem,
    weight_sem,
    send_sem,
    hop_sem,
    relay_sem,
    pair_sem,
    got_sem,
    fin_sem,
    both_sem,
    side_sem,
):
    me = lax.axis_index("seq")
    core, chip = lax.rem(me, 2), me // 2
    partner = me + 1 - 2 * core
    chips = n // 2
    steps, frame_count, width = frames_hbm.shape
    tokens = dec_hbm.shape[0]
    per_step = tokens // steps
    pairs, lanes = vt_ref.shape[0], vt_ref.shape[1]
    size = lanes // 2
    rows = wq_hbm.shape[0]
    half = wkv_ref.shape[2]
    parts = wkv_ref.shape[0] // 2
    part_pairs = half // lanes
    scale = 1.0 / math.sqrt(size)
    groups = GROUPS
    stat_rows = 16
    side, levels = lax.rem(chip, 2), chips // 2
    owners = list(range(chips // 4, chips - chips // 4))

    small = [
        pltpu.make_async_copy(src, dst, small_sem.at[at])
        for at, (src, dst) in enumerate(
            (
                (dec_hbm, dec_ref),
                (wq_hbm, wq_ref),
                (wout_hbm, wout_ref),
                (pos_hbm, pos_ref),
                (slope_hbm, slope_ref),
                (len_hbm, len_ref),
            )
        )
    ]

    def frame_copy(index):
        return pltpu.make_async_copy(frames_hbm.at[index], frames_ref.at[index], frame_sem.at[index])

    def weight_copy(index):
        return pltpu.make_async_copy(
            wkv_hbm.at[:, pl.ds(pl.multiple_of(index * half, half), half)], wkv_ref.at[index], weight_sem.at[index]
        )

    for at in (1, 0, 5, 4, 3):
        small[at].start()
    ordered = [stage if stage[0] in "KV" else BESIDE.get(int(stage[1:]), "B") for stage in PLAN if stage[0] in "KVA"]
    weight_order = [int(stage[1:]) + parts * (stage[0] == "V") for stage in ordered if stage != "B"]
    weight_copy(weight_order[0]).start(priority=1)
    for step in range(steps):
        frame_copy(step).start(priority=1)

    barrier = pltpu.get_barrier_semaphore()

    @pl.loop(1, n)
    def _(step):
        peer = lax.rem(me + step, n)
        pl.semaphore_signal(barrier, inc=1, device_id={"seq": peer}, device_id_type=MESH)

    def remote(src, dst, sent, got, peer):
        return pltpu.make_async_remote_copy(
            src_ref=src,
            dst_ref=dst,
            send_sem=sent,
            recv_sem=got,
            device_id={"seq": peer},
            device_id_type=MESH,
        )

    def await_copy(ref, sem):
        pltpu.make_async_copy(ref, ref, sem).wait()

    def query_rows(device):
        return q_ref.at[pl.ds(pl.multiple_of(device * rows, 16), rows)]

    def await_small():
        for at in (1, 0, 5, 4, 3):
            small[at].wait()

    def project_query():
        own_query = lax.dot_general(
            wq_ref[...], dec_ref[...], (((1,), (1,)), ((), ())), preferred_element_type=jnp.float32
        )
        q_ref[pl.ds(pl.multiple_of(me * rows, 16), rows), :] = own_query.astype(jnp.bfloat16)

    def await_barrier(_):
        for index in weight_order[4:]:
            weight_copy(index).start(priority=1)
        small[2].start(priority=1)
        pl.semaphore_wait(barrier, n - 1)

    await_small()
    project_query()

    middle = chips // 4
    wave_chips = (
        list(range(middle, chips - middle)),
        list(range(middle)) + list(range(chips - middle, chips)),
    )
    is_middle = (chip >= middle) & (chip < chips - middle)

    def query_relay(device, wave):
        block = query_rows(device)
        remote(block, block, send_sem.at[1], relay_sem.at[wave], partner).start()

    def spread_queries(wave):
        @pl.when(is_middle if wave == 0 else jnp.logical_not(is_middle))
        def _():
            own = query_rows(me)

            @pl.loop(1, chips)
            def _(step):
                remote(own, own, send_sem.at[0], hop_sem.at[chip], lax.rem(me + 2 * step, n)).start()

            query_relay(me, wave)

    def relay_queries(wave):
        for source in wave_chips[wave]:

            @pl.when(source != chip)
            def _():
                await_copy(query_rows(me), hop_sem.at[source])
                query_relay(2 * source + core, wave)

    def await_queries(wave):
        await_copy(q_ref.at[pl.ds(0, rows * len(wave_chips[wave]))], relay_sem.at[wave])

    place = lax.broadcasted_iota(jnp.int32, (frame_count, lanes), 0)
    column = lax.broadcasted_iota(jnp.int32, (frame_count, lanes), 1)
    for older in range(steps):
        hidden = (place >= len_ref[older, me]) & (column == 0)
        mask_ref[older * frame_count : (older + 1) * frame_count, :] = jnp.where(hidden, MASKED, 0.0).astype(
            jnp.bfloat16
        )

    def keys_piece(part, step, begin, stop):
        keys = jnp.dot(
            frames_ref[step, begin:stop, :], wkv_ref[part], preferred_element_type=jnp.float32
        ).astype(jnp.bfloat16)
        at = slice(step * frame_count + begin, step * frame_count + stop)
        for index in range(part_pairs):
            k_ref[part * part_pairs + index, at, :] = keys[:, index * lanes : (index + 1) * lanes]

    def values_piece(part, step, begin, stop):
        values = jnp.dot(
            frames_ref[step, begin:stop, :], wkv_ref[parts + part], preferred_element_type=jnp.float32
        )
        turned = values.astype(jnp.bfloat16).T
        at = slice(step * frame_count + begin, step * frame_count + stop)
        for index in range(part_pairs):
            vt_ref[part * part_pairs + index, :, at] = turned[index * lanes : (index + 1) * lanes]

    def project(kind, part, cuts):
        piece = keys_piece if kind == "K" else values_piece
        return [
            functools.partial(piece, part, step, begin, stop)
            for step in range(steps)
            for begin, stop in zip(cuts, cuts[1:])
        ]

    def project_keys(part):
        weight_copy(part).wait()
        for piece in project("K", part, (0, frame_count)):
            piece()

    def project_values(part):
        weight_copy(parts + part).wait()
        for piece in project("V", part, (0, frame_count)):
            piece()

    def await_frames():
        for step in range(steps):
            frame_copy(step).wait()

    for index in weight_order[1:4]:
        weight_copy(index).start(priority=1)
    await_frames()

    slot_place = lax.rem(me + 1, n).astype(jnp.float32)
    distance = jnp.abs(pos_ref[...].astype(jnp.float32) - slot_place) / n
    tail_row = lax.broadcasted_iota(jnp.int32, (lanes, tokens), 0) == 0
    tail = jnp.where(tail_row, 1.0, 0.0).astype(jnp.bfloat16)
    blank = jnp.zeros((size, tokens), jnp.bfloat16)
    ones = jnp.ones((EXTRA, frame_count), jnp.bfloat16)
    first, second = slice(0, frame_count), slice(frame_count, 2 * frame_count)
    early, late = slice(0, per_step), slice(per_step, tokens)

    def attend_scores(pair):
        query = q_ref[pl.ds(pl.multiple_of(pair * lanes, lanes), lanes), :]
        one = jnp.concatenate([query[:size], blank, tail], axis=0)
        two = jnp.concatenate([blank, query[size:], tail], axis=0)
        both = jnp.concatenate([one[:, late], two[:, late]], axis=1)
        old = jnp.concatenate([k_ref[pair, first, :], mask_ref[first, :]], axis=1)
        new = jnp.concatenate([k_ref[pair, second, :], mask_ref[second, :]], axis=1)
        return [
            functools.partial(jnp.dot, keys, queries, preferred_element_type=jnp.float32)
            for keys, queries in ((old, one), (old, two), (new, both))
        ]

    def soften(raw):
        peak = jnp.max(raw, axis=0, keepdims=True)
        weights = jnp.exp2((raw - peak) * (scale * math.log2(math.e)))
        return peak * scale, weights.astype(jnp.bfloat16)

    def attend_values(pair, kind):
        if kind == 2:
            stack = [vt_ref[pair, :, second], ones]
        else:
            stack = [vt_ref[pair, kind * size : (kind + 1) * size, first], ones]
        return jnp.concatenate(stack, axis=0)

    def attend(group):
        first_pair, count = groups[group]
        beside = []
        if group in BESIDE:
            kind, part = BESIDE[group][0], int(BESIDE[group][1:])
            weight_copy(part + parts * (kind == "V")).wait()
            half_frames = frame_count // 256 * 128
            beside = project(kind, part, (0, half_frames, frame_count))
        dots = []
        for local_pair in range(count):
            dots += [(local_pair, kind, call) for kind, call in enumerate(attend_scores(first_pair + local_pair))]
        results = {}
        ready = [dots[0][2](), dots[1][2]()]
        for at, (local_pair, kind, _) in enumerate(dots):
            raw = ready.pop(0)
            if at + 2 < len(dots):
                ready.append(dots[at + 2][2]())
            if beside:
                beside.pop(0)()
            peak, weights = soften(raw)
            values = attend_values(first_pair + local_pair, kind)
            results[local_pair, kind] = peak, jnp.dot(values, weights, preferred_element_type=jnp.float32)
        for piece in beside:
            piece()
        peaks = [[], []]
        totals = [[], []]
        for local_pair in range(count):
            pair = first_pair + local_pair
            new_peaks, new_context = results[local_pair, 2]
            for which in range(2):
                slope = slope_ref[2 * pair + which]
                at = pl.ds(pl.multiple_of(pair * lanes + which * size, size), size)
                peak, context = results[local_pair, which]
                peaks[0].append(peak[:, early] - slope * distance[:, early])
                totals[0].append(context[size : size + 1, early])
                ctx_ref[0, at, :] = context[:size, early].astype(jnp.bfloat16)
                span = slice(which * per_step, (which + 1) * per_step)
                old_peak = peak[:, late] - slope * (distance[:, late] + 1.0)
                new_peak = new_peaks[:, span] - slope * distance[:, late]
                top = jnp.maximum(old_peak, new_peak)
                old_factor, new_factor = jnp.exp(old_peak - top), jnp.exp(new_peak - top)
                own = slice(which * size, (which + 1) * size)
                merged = context[:size, late] * old_factor + new_context[own, span] * new_factor
                ctx_ref[1, at, :] = merged.astype(jnp.bfloat16)
                peaks[1].append(top)
                old_total = context[size : size + 1, late] * old_factor
                totals[1].append(old_total + new_context[lanes : lanes + 1, span] * new_factor)
        for step in range(2):
            stat_ref[step, group, 0 : 4 * count, :] = jnp.concatenate(peaks[step] + totals[step], axis=0)
        block = pl.ds(pl.multiple_of(first_pair * lanes, lanes), count * lanes)
        other = 1 - core
        remote(
            stat_ref.at[other, group], pair_stat.at[group], send_sem.at[2], pair_sem.at[group], partner
        ).start()
        remote(
            ctx_ref.at[other, block], pair_ctx.at[block], send_sem.at[3], pair_sem.at[group], partner
        ).start()

    def slices(first_pair, count):
        part_rows = count * lanes // len(owners)
        base = first_pair * lanes

        def place(owner):
            return owner % 2 * (levels // 2) + owner // 2 - levels // 4

        def block(owner):
            return pl.ds(pl.multiple_of(base + place(owner) * part_rows, 16), part_rows)

        slot = pl.ds(pl.multiple_of(base // len(owners), 16), part_rows)
        return part_rows, place, block, slot

    def mix(one, two, heads):
        top = jnp.maximum(one[:heads], two[:heads])
        one_factor, two_factor = jnp.exp(one[:heads] - top), jnp.exp(two[:heads] - top)
        total = one[heads : 2 * heads] * one_factor + two[heads : 2 * heads] * two_factor
        return top, total, one_factor, two_factor

    def merge_cores(group):
        first_pair, count = groups[group]
        part_rows, place, block, slot = slices(first_pair, count)
        heads = 2 * count
        await_copy(pair_ctx.at[pl.ds(0, count * lanes + stat_rows)], pair_sem.at[group])
        top, total, one_factor, two_factor = mix(stat_ref[core, group], pair_stat[group], heads)
        for head in range(heads):
            at = slice(first_pair * lanes + head * size, first_pair * lanes + (head + 1) * size)
            merged = (
                ctx_ref[core, at, :].astype(jnp.float32) * one_factor[head : head + 1]
                + pair_ctx[at, :].astype(jnp.float32) * two_factor[head : head + 1]
            )
            chip_ctx[at, :] = merged.astype(jnp.bfloat16)
        for owner in owners:
            head = place(owner) * part_rows // size
            chip_stat[group, owner] = jnp.concatenate([top[head : head + 1], total[head : head + 1]], axis=0)

            @pl.when(owner != chip)
            def _():
                peer = 2 * owner + core
                remote(
                    chip_stat.at[group, owner],
                    got_stat.at[group, chip],
                    send_sem.at[4],
                    got_sem.at[group],
                    peer,
                ).start()
                remote(
                    chip_ctx.at[block(owner)], got_ctx.at[chip, slot], send_sem.at[5], got_sem.at[group], peer
                ).start()

        @pl.when(is_middle)
        def _():
            got_stat[group, chip] = chip_stat[group, chip]
            got_ctx[chip, slot, :] = chip_ctx[block(chip), :]

    def merge_chips(group):
        pl.when(is_middle)(functools.partial(own_rows, group))

    def own_rows(group):
        first_pair, count = groups[group]
        mode = SHARES[group]
        part_rows, _, block, slot = slices(first_pair, count)
        each = part_rows + stat_rows // 4
        await_copy(fin_ref.at[0, pl.ds(0, (chips - 1) * each)], got_sem.at[group])
        stats = [got_stat[group, source] for source in range(chips)]
        top = stats[0][0:1]
        for stat in stats[1:]:
            top = jnp.maximum(top, stat[0:1])
        total = context = None
        for source, stat in enumerate(stats):
            factor = jnp.exp(stat[0:1] - top)
            part_total = stat[1:2] * factor
            part_context = got_ctx[source, slot, :].astype(jnp.float32) * factor
            total = part_total if total is None else total + part_total
            context = part_context if context is None else context + part_context
        fin_ref[core, block(chip), :] = (context / total).astype(jnp.bfloat16)
        own = fin_ref.at[core, block(chip)]
        stride = {"direct": 1, "relay": 2, "column": 4}[mode]
        sem = 7 if mode == "direct" else 6
        offset = lax.rem(me, stride)

        @pl.loop(0, n // stride)
        def _(step):
            peer = stride * step + offset

            @pl.when(peer != me)
            def _():
                remote(own, own, send_sem.at[sem], fin_sem.at[group], peer).start()

    def group_rows(group):
        first_pair, count = groups[group]
        return slice(first_pair * lanes, (first_pair + count) * lanes)

    def await_middle(ref, unit, amount, sem):
        @pl.when(is_middle)
        def _():
            await_copy(ref.at[pl.ds(0, unit * (amount - 1))], sem)

        @pl.when(jnp.logical_not(is_middle))
        def _():
            await_copy(ref.at[pl.ds(0, unit * amount)], sem)

    def await_slices(group, amount):
        unit = groups[group][1] * lanes // len(owners)
        await_middle(fin_ref.at[0], unit, amount, fin_sem.at[group])

    def side_rows(group, which):
        first_pair, count = groups[group]
        span = count * lanes // 2
        return pl.ds(pl.multiple_of(first_pair * lanes + which * span, 16), span)

    def cross(group):
        await_slices(group, levels // 2)
        block = fin_ref.at[core, side_rows(group, side)]
        remote(block, block, send_sem.at[9], side_sem.at[group], me + 2 - 4 * side).start()

    def relay(group):
        if SHARES[group] == "column":
            await_copy(fin_ref.at[0, pl.ds(0, groups[group][1] * lanes // 2)], side_sem.at[group])
        else:
            await_slices(group, len(owners))
        block = fin_ref.at[core, group_rows(group)]
        remote(block, block, send_sem.at[8], both_sem.at[group], partner).start()

    stages = {
        "K": project_keys,
        "V": project_values,
        "B": await_barrier,
        "Q": spread_queries,
        "W": relay_queries,
        "Y": await_queries,
        "A": attend,
        "M": merge_cores,
        "C": merge_chips,
        "X": cross,
        "R": relay,
    }
    for stage in PLAN:
        stages[stage[0]](int(stage[1:]))

    def await_both(group):
        await_copy(fin_ref.at[0, group_rows(group)], both_sem.at[group])

    small[2].wait()
    direct = [group for group, mode in enumerate(SHARES) if mode == "direct"]
    for group in range(direct[0]):
        await_both(group)

    def attended(begin, stop):
        context = jnp.concatenate([fin_ref[0, begin:stop, :], fin_ref[1, begin:stop, :]], axis=1)
        return jnp.dot(wout_ref[:, begin:stop], context, preferred_element_type=jnp.float32)

    late_row = groups[direct[0]][0] * lanes
    total = attended(0, late_row)
    for group in direct:
        await_slices(group, 2 * len(owners))
    total = total + attended(late_row, width)
    total = total.astype(jnp.bfloat16)
    for step in range(steps):
        out_ref[step] = total[:, step * per_step : (step + 1) * per_step]

    def sent(amount, sem):
        await_copy(q_ref.at[pl.ds(0, amount // 2)], send_sem.at[sem])

    share_rows = {mode: 0 for mode in SHARES}
    for (_, count), shared in zip(groups, SHARES):
        share_rows[shared] += count * lanes // len(owners)
    await_copy(q_ref.at[pl.ds(0, rows * (chips - 1))], send_sem.at[0])
    await_copy(q_ref.at[pl.ds(0, rows * chips)], send_sem.at[1])
    await_copy(stat_ref.at[0], send_sem.at[2])
    await_copy(ctx_ref.at[0], send_sem.at[3])
    @pl.when(is_middle)
    def _():
        await_copy(chip_stat.at[:, pl.ds(0, len(owners) - 1)], send_sem.at[4])

    @pl.when(jnp.logical_not(is_middle))
    def _():
        await_copy(chip_stat.at[:, pl.ds(0, len(owners))], send_sem.at[4])

    await_middle(fin_ref.at[0], width // len(owners), len(owners), send_sem.at[5])

    @pl.when(is_middle)
    def _():
        sent((levels - 1) * share_rows["column"] + (chips - 1) * share_rows["relay"], 6)
        sent((n - 1) * share_rows["direct"], 7)

    sent(late_row, 8)
    sent(share_rows["column"] * len(owners) // 2, 9)


def paired_local(n, frames, dec_states, w_query, w_keyval, w_output, head_slope, lengths, positions):
    steps, frame_count, width = frames.shape
    per_step = dec_states.shape[1]
    tokens = steps * per_step
    heads = head_slope.shape[0]
    lanes = 2 * (width // heads)
    pairs = heads // 2
    rows = w_query.shape[1]
    keys = steps * frame_count
    part = 2 * lanes
    chips = n // 2
    groups = len(GROUPS)
    vmem = pl.BlockSpec(memory_space=pltpu.VMEM)
    hbm = pl.BlockSpec(memory_space=pltpu.HBM)
    out = pl.pallas_call(
        functools.partial(paired_kernel, n),
        out_shape=pltpu.VMEM((steps, rows, per_step), jnp.bfloat16),
        in_specs=[hbm] * 8,
        out_specs=vmem,
        scratch_shapes=[
            pltpu.VMEM((1, tokens), jnp.int32),
            pltpu.SMEM((heads,), jnp.float32),
            pltpu.SMEM(lengths.shape, jnp.int32),
            pltpu.VMEM((tokens, width), jnp.bfloat16),
            pltpu.VMEM((rows, width), jnp.bfloat16),
            pltpu.VMEM((rows, width), jnp.bfloat16),
            pltpu.VMEM((steps, frame_count, width), jnp.bfloat16),
            pltpu.VMEM((2 * width // part, width, part), jnp.bfloat16),
            pltpu.VMEM((pairs, keys, lanes), jnp.bfloat16),
            pltpu.VMEM((keys, lanes), jnp.bfloat16),
            pltpu.VMEM((pairs, lanes, keys), jnp.bfloat16),
            pltpu.VMEM((width, tokens), jnp.bfloat16),
            pltpu.VMEM((2, width, per_step), jnp.bfloat16),
            pltpu.VMEM((2, groups, 8, per_step), jnp.float32),
            pltpu.VMEM((width, per_step), jnp.bfloat16),
            pltpu.VMEM((groups, 8, per_step), jnp.float32),
            pltpu.VMEM((width, per_step), jnp.bfloat16),
            pltpu.VMEM((groups, chips, 2, per_step), jnp.float32),
            pltpu.VMEM((chips, 2 * width // chips, per_step), jnp.bfloat16),
            pltpu.VMEM((groups, chips, 2, per_step), jnp.float32),
            pltpu.VMEM((2, width, per_step), jnp.bfloat16),
            pltpu.SemaphoreType.DMA((6,)),
            pltpu.SemaphoreType.DMA((steps,)),
            pltpu.SemaphoreType.DMA((2 * width // part,)),
            pltpu.SemaphoreType.DMA((10,)),
            pltpu.SemaphoreType.DMA((chips,)),
            pltpu.SemaphoreType.DMA((2,)),
            pltpu.SemaphoreType.DMA((groups,)),
            pltpu.SemaphoreType.DMA((groups,)),
            pltpu.SemaphoreType.DMA((groups,)),
            pltpu.SemaphoreType.DMA((groups,)),
            pltpu.SemaphoreType.DMA((groups,)),
        ],
        compiler_params=pltpu.CompilerParams(
            collective_id=0, has_side_effects=True, vmem_limit_bytes=40 * 1024 * 1024
        ),
    )(
        *(
            pltpu.with_memory_space_constraint(value, pltpu.HBM)
            for value in (
                positions.reshape(1, tokens),
                head_slope,
                lengths,
                dec_states.reshape(tokens, width),
                w_query.T,
                w_output.T,
                frames,
                w_keyval,
            )
        )
    )
    return out.transpose(0, 2, 1)


def fits_pairs(n, frames, dec_states, w_query, head_slope):
    steps, frame_count, width = frames.shape
    per_step, heads = dec_states.shape[1], head_slope.shape[0]
    size = width // heads
    chips = n // 2
    return (
        steps == 2
        and n % 4 == 0
        and heads % 4 == 0
        and heads // 2 == sum(count for _, count in GROUPS)
        and n % 16 == 0
        and size == 64
        and per_step == 2 * size
        and frame_count % 128 == 0
        and w_query.shape[1] % 16 == 0
        and (2 * size) % (16 * chips) == 0
    )


def local(n, frames, dec_states, w_query, w_keyval, w_output, head_slope, lengths, positions):
    paired = fits_pairs(n, frames, dec_states, w_query, head_slope)
    run = paired_local if paired else plain_local
    return run(n, frames, dec_states, w_query, w_keyval, w_output, head_slope, lengths, positions)


def solution(mesh):
    return jax.shard_map(
        functools.partial(local, mesh.shape["seq"]),
        mesh=mesh,
        in_specs=(
            P("grp", "seq", None),
            P(None, "grp", None),
            P(None, "seq"),
            P(),
            P(None, "seq"),
            P(),
            P("grp", None),
            P(None, "grp"),
        ),
        out_specs=P(None, "grp", "seq"),
        check_vma=False,
    )
```

```python
import functools
import math

import jax
import jax.numpy as jnp
from jax import lax
from jax.experimental import pallas as pl
from jax.experimental.pallas import tpu as pltpu
from jax.sharding import PartitionSpec as P

MESH = pl.DeviceIdType.MESH
EXTRA = 16
MASKED = -1e30


def rows_together(ref, first, count):
    parts = [ref[first + index].astype(jnp.float32) for index in range(count)]
    return jnp.concatenate(parts, axis=0)


def await_bytes(ref, count, sem):
    part = ref.at[pl.ds(0, count)]
    pltpu.make_async_copy(part, part, sem).wait()


def plain_kernel(
    n,
    dec_ref,
    wq_ref,
    wout_ref,
    pos_ref,
    slope_ref,
    len_ref,
    frames_hbm,
    wkv_hbm,
    out_ref,
    frames_ref,
    wkv_ref,
    k_ref,
    vt_ref,
    q_ref,
    ctx_ref,
    stat_ref,
    got_ctx,
    got_stat,
    pair_ctx,
    pair_stat,
    sum_ctx,
    sum_stat,
    fin_ref,
    frame_sem,
    weight_sem,
    send_sem,
    recv_sem,
    hop_sem,
    pair_sem,
):
    me = lax.axis_index("seq")
    steps, frame_count, width = frames_hbm.shape
    tokens = dec_ref.shape[0]
    per_step = tokens // steps
    heads = k_ref.shape[0]
    size = width // heads
    rows = wq_ref.shape[0]
    groups = math.gcd(heads, n)
    group_chunks = n // groups
    group_heads = heads // groups
    tile = frames_ref.shape[1]
    half = wkv_ref.shape[2]
    tiles = frames_ref.shape[0]
    per_block = frame_count // tile
    scale = 1.0 / math.sqrt(size)

    def frame_copy(index):
        return pltpu.make_async_copy(
            frames_hbm.at[index // per_block, pl.ds((index % per_block) * tile, tile)],
            frames_ref.at[index],
            frame_sem.at[index],
        )

    def weight_copy(index):
        return pltpu.make_async_copy(
            wkv_hbm.at[:, pl.ds(pl.multiple_of(index * half, half), half)], wkv_ref.at[index], weight_sem.at[index]
        )

    frame_copy(0).start()
    weight_copy(0).start()
    for index in range(1, tiles):
        frame_copy(index).start()
    for index in range(1, wkv_ref.shape[0]):
        weight_copy(index).start()

    barrier = pltpu.get_barrier_semaphore()

    @pl.loop(1, n)
    def _(step):
        peer = lax.rem(me + step, n)
        pl.semaphore_signal(barrier, inc=1, device_id={"seq": peer}, device_id_type=MESH)

    own_query = lax.dot_general(
        wq_ref[...], dec_ref[...], (((1,), (1,)), ((), ())), preferred_element_type=jnp.float32
    )
    q_ref[me] = own_query.astype(jnp.bfloat16)
    pl.semaphore_wait(barrier, n - 1)

    def send(src, dst, sem, peer):
        pltpu.make_async_remote_copy(
            src_ref=src,
            dst_ref=dst,
            send_sem=send_sem.at[sem],
            recv_sem=recv_sem.at[sem],
            device_id={"seq": peer},
            device_id_type=MESH,
        ).start()

    partner = me + 1 - 2 * lax.rem(me, 2)
    chips = n // 2

    def pass_on(ref, chunk, sem):
        send(ref.at[chunk], ref.at[chunk], sem, partner)

    def hop(ref, step, sem, level):
        return pltpu.make_async_remote_copy(
            src_ref=ref.at[me],
            dst_ref=ref.at[me],
            send_sem=send_sem.at[sem],
            recv_sem=hop_sem.at[level, step],
            device_id={"seq": lax.rem(me + 2 * step, n)},
            device_id_type=MESH,
        )

    def spread(ref, sem, level):
        @pl.loop(1, chips)
        def _(step):
            hop(ref, step, sem, level).start()

        pass_on(ref, me, level)

    def relay(ref, sem, level):
        @pl.loop(1, chips)
        def _(step):
            hop(ref, step, sem, level).wait_recv()
            pass_on(ref, lax.rem(me - 2 * step + n, n), level)

    def settle(ref, sem, level):
        await_bytes(ref, chips - 1, send_sem.at[sem])
        await_bytes(ref, chips, recv_sem.at[level])
        await_bytes(ref, chips, send_sem.at[level])

    spread(q_ref, 2, 0)

    column = lax.broadcasted_iota(jnp.int32, (frame_count, size + EXTRA), 1)
    place = lax.broadcasted_iota(jnp.int32, (frame_count, size + EXTRA), 0)
    masks = []
    for older in range(steps):
        hidden = (place >= len_ref[older, me]) & (column == size)
        masks.append(jnp.where(hidden, MASKED, 0.0).astype(jnp.bfloat16))
    mask = jnp.concatenate(masks, axis=0)
    ones = jnp.ones((EXTRA, steps * frame_count), jnp.bfloat16)

    @pl.loop(0, heads)
    def _(head):
        k_ref[head] = mask
        vt_ref[head, size:, :] = ones

    parts = wkv_ref.shape[0] // 2
    part_heads = half // size

    def project(part, index):
        at = pl.ds(pl.multiple_of(index * tile, tile), tile)
        keyval = jnp.dot(frames_ref[index], wkv_ref[part], preferred_element_type=jnp.float32)
        return at, keyval.astype(jnp.bfloat16)

    for index in range(tiles):
        frame_copy(index).wait()

    @pl.loop(0, parts)
    def _(part):
        weight_copy(part).wait()
        for index in range(tiles):
            at, keyval = project(part, index)
            for local_head in range(part_heads):
                lanes = slice(local_head * size, (local_head + 1) * size)
                k_ref[part * part_heads + local_head, at, 0:size] = keyval[:, lanes]

    def project_values(part):
        weight_copy(parts + part).wait()
        for index in range(tiles):
            at, keyval = project(parts + part, index)
            turned = keyval.T
            for local_head in range(part_heads):
                lanes = slice(local_head * size, (local_head + 1) * size)
                vt_ref[part * part_heads + local_head, 0:size, at] = turned[lanes]

    pl.loop(0, parts - 2)(project_values)
    relay(q_ref, 2, 0)
    pl.loop(parts - 2, parts)(project_values)
    settle(q_ref, 2, 0)

    slot_place = lax.rem(me + 1, n).astype(jnp.float32)
    distance = jnp.abs(pos_ref[...].astype(jnp.float32) - slot_place) / n
    first_row = lax.broadcasted_iota(jnp.int32, (EXTRA, tokens), 0) == 0
    query_tail = jnp.where(first_row, 1.0, 0.0).astype(jnp.bfloat16)
    token_step = lax.broadcasted_iota(jnp.int32, (1, tokens), 1) // per_step

    row = lax.broadcasted_iota(jnp.int32, (rows, tokens), 0)

    def pass_sums(turn):
        group = lax.rem(me // group_chunks + 1 + turn, groups)
        await_bytes(pair_stat, group_chunks // 2, pair_sem.at[0, turn])
        await_bytes(pair_ctx, group_chunks // 2, pair_sem.at[1, turn])

        @pl.loop(0, group_chunks // 2)
        def _(index):
            chunk = group * group_chunks + 2 * index + lax.rem(me, 2)
            slot = chunk // 2
            one, two = stat_ref[chunk], pair_stat[slot]
            top = jnp.maximum(one[0:2], two[0:2])
            one_factor = jnp.exp(one[0:2] - top)
            two_factor = jnp.exp(two[0:2] - top)
            stat = jnp.concatenate([top, one[2:4] * one_factor + two[2:4] * two_factor], axis=0)
            is_one = row + lax.rem(chunk * rows, size) < size
            context = ctx_ref[chunk].astype(jnp.float32) * jnp.where(
                is_one, one_factor[0:1], one_factor[1:2]
            ) + pair_ctx[slot].astype(jnp.float32) * jnp.where(
                is_one, two_factor[0:1], two_factor[1:2]
            )
            context = context.astype(jnp.bfloat16)

            @pl.when(chunk != me)
            def _():
                sum_stat[slot] = stat
                sum_ctx[slot] = context
                send(sum_stat.at[slot], got_stat.at[me // 2], 4, chunk)
                send(sum_ctx.at[slot], got_ctx.at[me // 2], 5, chunk)

            @pl.when(chunk == me)
            def _():
                got_stat[slot] = stat
                got_ctx[slot] = context

    @pl.loop(0, groups)
    def _(turn):
        group = lax.rem(me // group_chunks + 1 + turn, groups)
        query_rows = rows_together(q_ref, group * group_chunks, group_chunks).astype(jnp.bfloat16)
        peaks, totals, contexts = [], [], []

        def scores(local_head):
            query = jnp.concatenate(
                [query_rows[local_head * size : (local_head + 1) * size], query_tail], axis=0
            )
            return [
                jnp.dot(
                    k_ref[
                        group * group_heads + local_head,
                        pl.ds(older * frame_count, frame_count),
                        :,
                    ],
                    query[:, older * per_step :],
                    preferred_element_type=jnp.float32,
                )
                for older in range(steps)
            ]

        ready = scores(0)
        for local_head in range(group_heads):
            head = group * group_heads + local_head
            raws = ready
            if local_head + 1 < group_heads:
                ready = scores(local_head + 1)
            slope = slope_ref[head]
            peak = context = None
            for older in range(steps):
                first = older * per_step
                block = pl.ds(older * frame_count, frame_count)
                raw = raws[older]
                raw_peak = jnp.max(raw, axis=0, keepdims=True)
                weights = jnp.exp2((raw - raw_peak) * (scale * math.log2(math.e)))
                part_context = jnp.dot(
                    vt_ref[head, :, block],
                    weights.astype(jnp.bfloat16),
                    preferred_element_type=jnp.float32,
                )
                age = (token_step[:, first:] - older).astype(jnp.float32)
                part_peak = raw_peak * scale - slope * (distance[:, first:] + age)
                if peak is None:
                    peak, context = part_peak, part_context
                    continue
                top = jnp.maximum(peak[:, first:], part_peak)
                old_factor = jnp.exp(peak[:, first:] - top)
                new_factor = jnp.exp(part_peak - top)
                merged = context[:, first:] * old_factor + part_context * new_factor
                peak = jnp.concatenate([peak[:, :first], top], axis=1)
                context = jnp.concatenate([context[:, :first], merged], axis=1)
            peaks.append(peak)
            totals.append(context[size : size + 1])
            contexts.append(context[:size])
        stacked = jnp.concatenate(contexts, axis=0)
        for index in range(group_chunks):
            low, high = index * rows, (index + 1) * rows
            one, two = low // size, (high - 1) // size
            chunk = group * group_chunks + index
            ctx_ref[chunk] = stacked[low:high].astype(jnp.bfloat16)
            stat_ref[chunk] = jnp.concatenate(
                [peaks[one], peaks[two], totals[one], totals[two]], axis=0
            )

        @pl.loop(0, group_chunks // 2)
        def _(index):
            chunk = group * group_chunks + 2 * index + 1 - lax.rem(me, 2)
            for kind, (src, dst) in enumerate(((stat_ref, pair_stat), (ctx_ref, pair_ctx))):
                pltpu.make_async_remote_copy(
                    src_ref=src.at[chunk],
                    dst_ref=dst.at[chunk // 2],
                    send_sem=send_sem.at[kind],
                    recv_sem=pair_sem.at[kind, turn],
                    device_id={"seq": partner},
                    device_id_type=MESH,
                ).start()

        @pl.when(turn > 0)
        def _():
            pass_sums(turn - 1)

    pass_sums(groups - 1)
    await_bytes(got_stat, chips - 1, recv_sem.at[4])
    await_bytes(got_ctx, chips - 1, recv_sem.at[5])
    await_bytes(sum_stat, chips - 1, send_sem.at[4])
    await_bytes(sum_ctx, chips - 1, send_sem.at[5])
    await_bytes(stat_ref, chips, send_sem.at[0])
    await_bytes(ctx_ref, chips, send_sem.at[1])

    top = lax.fori_loop(
        1, chips, lambda at, best: jnp.maximum(best, got_stat[at][0:2]), got_stat[0][0:2]
    )
    is_one = row + lax.rem(me * rows, size) < size

    def add(at, state):
        total, acc = state
        stat = got_stat[at]
        factor = jnp.exp(stat[0:2] - top)
        spread = jnp.where(is_one, factor[0:1], factor[1:2])
        return total + stat[2:4] * factor, acc + got_ctx[at].astype(jnp.float32) * spread

    total, acc = lax.fori_loop(
        0,
        chips,
        add,
        (jnp.zeros((2, tokens), jnp.float32), jnp.zeros((rows, tokens), jnp.float32)),
    )
    fin_ref[me] = (acc / jnp.where(is_one, total[0:1], total[1:2])).astype(jnp.bfloat16)

    spread(fin_ref, 3, 1)
    relay(fin_ref, 3, 1)
    settle(fin_ref, 3, 1)
    context = rows_together(fin_ref, 0, n).astype(jnp.bfloat16)
    attended = jnp.dot(wout_ref[...], context, preferred_element_type=jnp.float32)
    attended = attended.astype(jnp.bfloat16)
    for step in range(steps):
        out_ref[step] = attended[:, step * per_step : (step + 1) * per_step]


def plain_local(n, frames, dec_states, w_query, w_keyval, w_output, head_slope, lengths, positions):
    steps, frame_count, width = frames.shape
    per_step = dec_states.shape[1]
    tokens = steps * per_step
    heads = head_slope.shape[0]
    size = width // heads
    rows = w_query.shape[1]
    keys = steps * frame_count
    tile = frame_count
    part = math.gcd(width, 256)
    vmem = pl.BlockSpec(memory_space=pltpu.VMEM)
    smem = pl.BlockSpec(memory_space=pltpu.SMEM)
    hbm = pl.BlockSpec(memory_space=pl.ANY)
    out = pl.pallas_call(
        functools.partial(plain_kernel, n),
        out_shape=jax.ShapeDtypeStruct((steps, rows, per_step), jnp.bfloat16),
        in_specs=[vmem, vmem, vmem, vmem, smem, smem, hbm, hbm],
        out_specs=vmem,
        scratch_shapes=[
            pltpu.VMEM((keys // tile, tile, width), jnp.bfloat16),
            pltpu.VMEM((2 * width // part, width, part), jnp.bfloat16),
            pltpu.VMEM((heads, keys, size + EXTRA), jnp.bfloat16),
            pltpu.VMEM((heads, size + EXTRA, keys), jnp.bfloat16),
            pltpu.VMEM((n, rows, tokens), jnp.bfloat16),
            pltpu.VMEM((n, rows, tokens), jnp.bfloat16),
            pltpu.VMEM((n, 4, tokens), jnp.float32),
            pltpu.VMEM((n // 2, rows, tokens), jnp.bfloat16),
            pltpu.VMEM((n // 2, 4, tokens), jnp.float32),
            pltpu.VMEM((n // 2, rows, tokens), jnp.bfloat16),
            pltpu.VMEM((n // 2, 4, tokens), jnp.float32),
            pltpu.VMEM((n // 2, rows, tokens), jnp.bfloat16),
            pltpu.VMEM((n // 2, 4, tokens), jnp.float32),
            pltpu.VMEM((n, rows, tokens), jnp.bfloat16),
            pltpu.SemaphoreType.DMA((keys // tile,)),
            pltpu.SemaphoreType.DMA((2 * width // part,)),
            pltpu.SemaphoreType.DMA((6,)),
            pltpu.SemaphoreType.DMA((6,)),
            pltpu.SemaphoreType.DMA((2, n // 2)),
            pltpu.SemaphoreType.DMA((2, math.gcd(heads, n))),
        ],
        compiler_params=pltpu.CompilerParams(
            collective_id=0, has_side_effects=True, vmem_limit_bytes=60 * 1024 * 1024
        ),
    )(
        dec_states.reshape(tokens, width),
        w_query.T,
        w_output.T,
        positions.reshape(1, tokens),
        head_slope,
        lengths,
        frames,
        w_keyval,
    )
    return out.transpose(0, 2, 1)


GROUPS = ((3, 2), (5, 2), (0, 2), (2, 1), (7, 1), (8, 1), (9, 1))
PLAN = (
    ("K1", "B0", "Q0", "V1", "K2", "V2", "K3", "Q1", "V3", "W0", "K0", "Y0", "A0", "A1", "M0", "W1", "K4", "M1")
    + ("Y1", "A2", "A3", "M2", "C0", "A4", "M3", "C1", "A5", "M4", "A6", "M5", "M6", "C2", "X0", "C3", "X1", "C4")
    + ("R0", "C5", "C6", "R1", "R2", "R3", "R4", "R5")
)
BESIDE = {0: "V0", 2: "V4"}
SHARES = ("column", "column", "relay", "relay", "relay", "relay", "direct")


def paired_kernel(
    n,
    pos_hbm,
    slope_hbm,
    len_hbm,
    dec_hbm,
    wq_hbm,
    wout_hbm,
    frames_hbm,
    wkv_hbm,
    out_ref,
    pos_ref,
    slope_ref,
    len_ref,
    dec_ref,
    wq_ref,
    wout_ref,
    frames_ref,
    wkv_ref,
    k_ref,
    mask_ref,
    vt_ref,
    q_ref,
    ctx_ref,
    stat_ref,
    pair_ctx,
    pair_stat,
    chip_ctx,
    chip_stat,
    got_ctx,
    got_stat,
    fin_ref,
    small_sem,
    frame_sem,
    weight_sem,
    send_sem,
    hop_sem,
    relay_sem,
    pair_sem,
    got_sem,
    fin_sem,
    both_sem,
    side_sem,
):
    me = lax.axis_index("seq")
    core, chip = lax.rem(me, 2), me // 2
    partner = me + 1 - 2 * core
    chips = n // 2
    steps, frame_count, width = frames_hbm.shape
    tokens = dec_hbm.shape[0]
    per_step = tokens // steps
    pairs, lanes = vt_ref.shape[0], vt_ref.shape[1]
    size = lanes // 2
    rows = wq_hbm.shape[0]
    half = wkv_ref.shape[2]
    parts = wkv_ref.shape[0] // 2
    part_pairs = half // lanes
    scale = 1.0 / math.sqrt(size)
    groups = GROUPS
    stat_rows = 16
    side, levels = lax.rem(chip, 2), chips // 2
    owners = list(range(chips // 4, chips - chips // 4))

    small = [
        pltpu.make_async_copy(src, dst, small_sem.at[at])
        for at, (src, dst) in enumerate(
            (
                (dec_hbm, dec_ref),
                (wq_hbm, wq_ref),
                (wout_hbm, wout_ref),
                (pos_hbm, pos_ref),
                (slope_hbm, slope_ref),
                (len_hbm, len_ref),
            )
        )
    ]

    def frame_copy(index):
        return pltpu.make_async_copy(frames_hbm.at[index], frames_ref.at[index], frame_sem.at[index])

    def weight_copy(index):
        return pltpu.make_async_copy(
            wkv_hbm.at[:, pl.ds(pl.multiple_of(index * half, half), half)], wkv_ref.at[index], weight_sem.at[index]
        )

    for at in (1, 0, 5, 4, 3):
        small[at].start()
    ordered = [stage if stage[0] in "KV" else BESIDE.get(int(stage[1:]), "B") for stage in PLAN if stage[0] in "KVA"]
    weight_order = [int(stage[1:]) + parts * (stage[0] == "V") for stage in ordered if stage != "B"]
    weight_copy(weight_order[0]).start(priority=1)
    for step in range(steps):
        frame_copy(step).start(priority=1)

    barrier = pltpu.get_barrier_semaphore()

    @pl.loop(1, n)
    def _(step):
        peer = lax.rem(me + step, n)
        pl.semaphore_signal(barrier, inc=1, device_id={"seq": peer}, device_id_type=MESH)

    def remote(src, dst, sent, got, peer):
        return pltpu.make_async_remote_copy(
            src_ref=src,
            dst_ref=dst,
            send_sem=sent,
            recv_sem=got,
            device_id={"seq": peer},
            device_id_type=MESH,
        )

    def await_copy(ref, sem):
        pltpu.make_async_copy(ref, ref, sem).wait()

    def query_rows(device):
        return q_ref.at[pl.ds(pl.multiple_of(device * rows, 16), rows)]

    def await_small():
        for at in (1, 0, 5, 4, 3):
            small[at].wait()

    def project_query():
        own_query = lax.dot_general(
            wq_ref[...], dec_ref[...], (((1,), (1,)), ((), ())), preferred_element_type=jnp.float32
        )
        q_ref[pl.ds(pl.multiple_of(me * rows, 16), rows), :] = own_query.astype(jnp.bfloat16)

    def await_barrier(_):
        for index in weight_order[4:]:
            weight_copy(index).start(priority=1)
        small[2].start(priority=1)
        pl.semaphore_wait(barrier, n - 1)

    await_small()
    project_query()

    middle = chips // 4
    wave_chips = (
        list(range(middle, chips - middle)),
        list(range(middle)) + list(range(chips - middle, chips)),
    )
    is_middle = (chip >= middle) & (chip < chips - middle)

    def query_relay(device, wave):
        block = query_rows(device)
        remote(block, block, send_sem.at[1], relay_sem.at[wave], partner).start()

    def spread_queries(wave):
        @pl.when(is_middle if wave == 0 else jnp.logical_not(is_middle))
        def _():
            own = query_rows(me)

            @pl.loop(1, chips)
            def _(step):
                remote(own, own, send_sem.at[0], hop_sem.at[chip], lax.rem(me + 2 * step, n)).start()

            query_relay(me, wave)

    def relay_queries(wave):
        for source in wave_chips[wave]:

            @pl.when(source != chip)
            def _():
                await_copy(query_rows(me), hop_sem.at[source])
                query_relay(2 * source + core, wave)

    def await_queries(wave):
        await_copy(q_ref.at[pl.ds(0, rows * len(wave_chips[wave]))], relay_sem.at[wave])

    place = lax.broadcasted_iota(jnp.int32, (frame_count, lanes), 0)
    column = lax.broadcasted_iota(jnp.int32, (frame_count, lanes), 1)
    for older in range(steps):
        hidden = (place >= len_ref[older, me]) & (column == 0)
        mask_ref[older * frame_count : (older + 1) * frame_count, :] = jnp.where(hidden, MASKED, 0.0).astype(
            jnp.bfloat16
        )

    def keys_piece(part, step, begin, stop):
        keys = jnp.dot(
            frames_ref[step, begin:stop, :], wkv_ref[part], preferred_element_type=jnp.float32
        ).astype(jnp.bfloat16)
        at = slice(step * frame_count + begin, step * frame_count + stop)
        for index in range(part_pairs):
            k_ref[part * part_pairs + index, at, :] = keys[:, index * lanes : (index + 1) * lanes]

    def values_piece(part, step, begin, stop):
        values = jnp.dot(
            frames_ref[step, begin:stop, :], wkv_ref[parts + part], preferred_element_type=jnp.float32
        )
        turned = values.astype(jnp.bfloat16).T
        at = slice(step * frame_count + begin, step * frame_count + stop)
        for index in range(part_pairs):
            vt_ref[part * part_pairs + index, :, at] = turned[index * lanes : (index + 1) * lanes]

    def project(kind, part, cuts):
        piece = keys_piece if kind == "K" else values_piece
        return [
            functools.partial(piece, part, step, begin, stop)
            for step in range(steps)
            for begin, stop in zip(cuts, cuts[1:])
        ]

    def project_keys(part):
        weight_copy(part).wait()
        for piece in project("K", part, (0, frame_count)):
            piece()

    def project_values(part):
        weight_copy(parts + part).wait()
        for piece in project("V", part, (0, frame_count)):
            piece()

    def await_frames():
        for step in range(steps):
            frame_copy(step).wait()

    for index in weight_order[1:4]:
        weight_copy(index).start(priority=1)
    await_frames()

    slot_place = lax.rem(me + 1, n).astype(jnp.float32)
    distance = jnp.abs(pos_ref[...].astype(jnp.float32) - slot_place) / n
    tail_row = lax.broadcasted_iota(jnp.int32, (lanes, tokens), 0) == 0
    tail = jnp.where(tail_row, 1.0, 0.0).astype(jnp.bfloat16)
    blank = jnp.zeros((size, tokens), jnp.bfloat16)
    ones = jnp.ones((EXTRA, frame_count), jnp.bfloat16)
    first, second = slice(0, frame_count), slice(frame_count, 2 * frame_count)
    early, late = slice(0, per_step), slice(per_step, tokens)

    def attend_scores(pair):
        query = q_ref[pl.ds(pl.multiple_of(pair * lanes, lanes), lanes), :]
        one = jnp.concatenate([query[:size], blank, tail], axis=0)
        two = jnp.concatenate([blank, query[size:], tail], axis=0)
        both = jnp.concatenate([one[:, late], two[:, late]], axis=1)
        old = jnp.concatenate([k_ref[pair, first, :], mask_ref[first, :]], axis=1)
        new = jnp.concatenate([k_ref[pair, second, :], mask_ref[second, :]], axis=1)
        return [
            functools.partial(jnp.dot, keys, queries, preferred_element_type=jnp.float32)
            for keys, queries in ((old, one), (old, two), (new, both))
        ]

    def soften(raw):
        peak = jnp.max(raw, axis=0, keepdims=True)
        weights = jnp.exp2((raw - peak) * (scale * math.log2(math.e)))
        return peak * scale, weights.astype(jnp.bfloat16)

    def attend_values(pair, kind):
        if kind == 2:
            stack = [vt_ref[pair, :, second], ones]
        else:
            stack = [vt_ref[pair, kind * size : (kind + 1) * size, first], ones]
        return jnp.concatenate(stack, axis=0)

    def attend(group):
        first_pair, count = groups[group]
        beside = []
        if group in BESIDE:
            kind, part = BESIDE[group][0], int(BESIDE[group][1:])
            weight_copy(part + parts * (kind == "V")).wait()
            half_frames = frame_count // 256 * 128
            beside = project(kind, part, (0, half_frames, frame_count))
        dots = []
        for local_pair in range(count):
            dots += [(local_pair, kind, call) for kind, call in enumerate(attend_scores(first_pair + local_pair))]
        results = {}
        ready = [dots[0][2](), dots[1][2]()]
        for at, (local_pair, kind, _) in enumerate(dots):
            raw = ready.pop(0)
            if at + 2 < len(dots):
                ready.append(dots[at + 2][2]())
            if beside:
                beside.pop(0)()
            peak, weights = soften(raw)
            values = attend_values(first_pair + local_pair, kind)
            results[local_pair, kind] = peak, jnp.dot(values, weights, preferred_element_type=jnp.float32)
        for piece in beside:
            piece()
        peaks = [[], []]
        totals = [[], []]
        for local_pair in range(count):
            pair = first_pair + local_pair
            new_peaks, new_context = results[local_pair, 2]
            for which in range(2):
                slope = slope_ref[2 * pair + which]
                at = pl.ds(pl.multiple_of(pair * lanes + which * size, size), size)
                peak, context = results[local_pair, which]
                peaks[0].append(peak[:, early] - slope * distance[:, early])
                totals[0].append(context[size : size + 1, early])
                ctx_ref[0, at, :] = context[:size, early].astype(jnp.bfloat16)
                span = slice(which * per_step, (which + 1) * per_step)
                old_peak = peak[:, late] - slope * (distance[:, late] + 1.0)
                new_peak = new_peaks[:, span] - slope * distance[:, late]
                top = jnp.maximum(old_peak, new_peak)
                old_factor, new_factor = jnp.exp(old_peak - top), jnp.exp(new_peak - top)
                own = slice(which * size, (which + 1) * size)
                merged = context[:size, late] * old_factor + new_context[own, span] * new_factor
                ctx_ref[1, at, :] = merged.astype(jnp.bfloat16)
                peaks[1].append(top)
                old_total = context[size : size + 1, late] * old_factor
                totals[1].append(old_total + new_context[lanes : lanes + 1, span] * new_factor)
        for step in range(2):
            stat_ref[step, group, 0 : 4 * count, :] = jnp.concatenate(peaks[step] + totals[step], axis=0)
        block = pl.ds(pl.multiple_of(first_pair * lanes, lanes), count * lanes)
        other = 1 - core
        remote(
            stat_ref.at[other, group], pair_stat.at[group], send_sem.at[2], pair_sem.at[group], partner
        ).start()
        remote(
            ctx_ref.at[other, block], pair_ctx.at[block], send_sem.at[3], pair_sem.at[group], partner
        ).start()

    def slices(first_pair, count):
        part_rows = count * lanes // len(owners)
        base = first_pair * lanes

        def place(owner):
            return owner % 2 * (levels // 2) + owner // 2 - levels // 4

        def block(owner):
            return pl.ds(pl.multiple_of(base + place(owner) * part_rows, 16), part_rows)

        slot = pl.ds(pl.multiple_of(base // len(owners), 16), part_rows)
        return part_rows, place, block, slot

    def mix(one, two, heads):
        top = jnp.maximum(one[:heads], two[:heads])
        one_factor, two_factor = jnp.exp(one[:heads] - top), jnp.exp(two[:heads] - top)
        total = one[heads : 2 * heads] * one_factor + two[heads : 2 * heads] * two_factor
        return top, total, one_factor, two_factor

    def merge_cores(group):
        first_pair, count = groups[group]
        part_rows, place, block, slot = slices(first_pair, count)
        heads = 2 * count
        await_copy(pair_ctx.at[pl.ds(0, count * lanes + stat_rows)], pair_sem.at[group])
        top, total, one_factor, two_factor = mix(stat_ref[core, group], pair_stat[group], heads)
        for head in range(heads):
            at = slice(first_pair * lanes + head * size, first_pair * lanes + (head + 1) * size)
            merged = (
                ctx_ref[core, at, :].astype(jnp.float32) * one_factor[head : head + 1]
                + pair_ctx[at, :].astype(jnp.float32) * two_factor[head : head + 1]
            )
            chip_ctx[at, :] = merged.astype(jnp.bfloat16)
        for owner in owners:
            head = place(owner) * part_rows // size
            chip_stat[group, owner] = jnp.concatenate([top[head : head + 1], total[head : head + 1]], axis=0)

        for first_owner in owners:
            owner = jnp.where(chip < levels, chips - 1 - first_owner, first_owner)
            rows_at = jnp.where(
                chip < levels, place(chips - 1 - first_owner) * part_rows, place(first_owner) * part_rows
            )
            sent_block = pl.ds(pl.multiple_of(first_pair * lanes + rows_at, 16), part_rows)

            @pl.when(owner != chip)
            def _():
                peer = 2 * owner + core
                remote(
                    chip_stat.at[group, owner], got_stat.at[group, chip], send_sem.at[4], got_sem.at[group], peer
                ).start()
                remote(
                    chip_ctx.at[sent_block], got_ctx.at[chip, slot], send_sem.at[5], got_sem.at[group], peer
                ).start()

        @pl.when(is_middle)
        def _():
            got_stat[group, chip] = chip_stat[group, chip]
            got_ctx[chip, slot, :] = chip_ctx[block(chip), :]

    def merge_chips(group):
        pl.when(is_middle)(functools.partial(own_rows, group))

    def own_rows(group):
        first_pair, count = groups[group]
        mode = SHARES[group]
        part_rows, _, block, slot = slices(first_pair, count)
        each = part_rows + stat_rows // 4
        await_copy(fin_ref.at[0, pl.ds(0, (chips - 1) * each)], got_sem.at[group])
        stats = [got_stat[group, source] for source in range(chips)]
        top = stats[0][0:1]
        for stat in stats[1:]:
            top = jnp.maximum(top, stat[0:1])
        total = context = None
        for source, stat in enumerate(stats):
            factor = jnp.exp(stat[0:1] - top)
            part_total = stat[1:2] * factor
            part_context = got_ctx[source, slot, :].astype(jnp.float32) * factor
            total = part_total if total is None else total + part_total
            context = part_context if context is None else context + part_context
        fin_ref[core, block(chip), :] = (context / total).astype(jnp.bfloat16)
        own = fin_ref.at[core, block(chip)]
        stride = {"direct": 1, "relay": 2, "column": 4}[mode]
        sem = 7 if mode == "direct" else 6
        offset = lax.rem(me, stride)

        @pl.loop(0, n // stride)
        def _(step):
            peer = stride * step + offset

            @pl.when(peer != me)
            def _():
                remote(own, own, send_sem.at[sem], fin_sem.at[group], peer).start()

    def group_rows(group):
        first_pair, count = groups[group]
        return slice(first_pair * lanes, (first_pair + count) * lanes)

    def await_middle(ref, unit, amount, sem):
        @pl.when(is_middle)
        def _():
            await_copy(ref.at[pl.ds(0, unit * (amount - 1))], sem)

        @pl.when(jnp.logical_not(is_middle))
        def _():
            await_copy(ref.at[pl.ds(0, unit * amount)], sem)

    def await_slices(group, amount):
        unit = groups[group][1] * lanes // len(owners)
        await_middle(fin_ref.at[0], unit, amount, fin_sem.at[group])

    def side_rows(group, which):
        first_pair, count = groups[group]
        span = count * lanes // 2
        return pl.ds(pl.multiple_of(first_pair * lanes + which * span, 16), span)

    def cross(group):
        await_slices(group, levels // 2)
        block = fin_ref.at[core, side_rows(group, side)]
        remote(block, block, send_sem.at[9], side_sem.at[group], me + 2 - 4 * side).start()

    def relay(group):
        if SHARES[group] == "column":
            await_copy(fin_ref.at[0, pl.ds(0, groups[group][1] * lanes // 2)], side_sem.at[group])
        else:
            await_slices(group, len(owners))
        block = fin_ref.at[core, group_rows(group)]
        remote(block, block, send_sem.at[8], both_sem.at[group], partner).start()

    stages = {
        "K": project_keys,
        "V": project_values,
        "B": await_barrier,
        "Q": spread_queries,
        "W": relay_queries,
        "Y": await_queries,
        "A": attend,
        "M": merge_cores,
        "C": merge_chips,
        "X": cross,
        "R": relay,
    }
    for stage in PLAN:
        stages[stage[0]](int(stage[1:]))

    def await_both(group):
        await_copy(fin_ref.at[0, group_rows(group)], both_sem.at[group])

    small[2].wait()
    direct = [group for group, mode in enumerate(SHARES) if mode == "direct"]
    for group in range(direct[0]):
        await_both(group)

    def attended(begin, stop):
        context = jnp.concatenate([fin_ref[0, begin:stop, :], fin_ref[1, begin:stop, :]], axis=1)
        return jnp.dot(wout_ref[:, begin:stop], context, preferred_element_type=jnp.float32)

    late_row = groups[direct[0]][0] * lanes
    total = attended(0, late_row)
    for group in direct:
        await_slices(group, 2 * len(owners))
    total = total + attended(late_row, width)
    total = total.astype(jnp.bfloat16)
    for step in range(steps):
        out_ref[step] = total[:, step * per_step : (step + 1) * per_step]

    def sent(amount, sem):
        await_copy(q_ref.at[pl.ds(0, amount // 2)], send_sem.at[sem])

    share_rows = {mode: 0 for mode in SHARES}
    for (_, count), shared in zip(groups, SHARES):
        share_rows[shared] += count * lanes // len(owners)
    await_copy(q_ref.at[pl.ds(0, rows * (chips - 1))], send_sem.at[0])
    await_copy(q_ref.at[pl.ds(0, rows * chips)], send_sem.at[1])
    await_copy(stat_ref.at[0], send_sem.at[2])
    await_copy(ctx_ref.at[0], send_sem.at[3])
    @pl.when(is_middle)
    def _():
        await_copy(chip_stat.at[:, pl.ds(0, len(owners) - 1)], send_sem.at[4])

    @pl.when(jnp.logical_not(is_middle))
    def _():
        await_copy(chip_stat.at[:, pl.ds(0, len(owners))], send_sem.at[4])

    await_middle(fin_ref.at[0], width // len(owners), len(owners), send_sem.at[5])

    @pl.when(is_middle)
    def _():
        sent((levels - 1) * share_rows["column"] + (chips - 1) * share_rows["relay"], 6)
        sent((n - 1) * share_rows["direct"], 7)

    sent(late_row, 8)
    sent(share_rows["column"] * len(owners) // 2, 9)


def paired_local(n, frames, dec_states, w_query, w_keyval, w_output, head_slope, lengths, positions):
    steps, frame_count, width = frames.shape
    per_step = dec_states.shape[1]
    tokens = steps * per_step
    heads = head_slope.shape[0]
    lanes = 2 * (width // heads)
    pairs = heads // 2
    rows = w_query.shape[1]
    keys = steps * frame_count
    part = 2 * lanes
    chips = n // 2
    groups = len(GROUPS)
    vmem = pl.BlockSpec(memory_space=pltpu.VMEM)
    hbm = pl.BlockSpec(memory_space=pltpu.HBM)
    out = pl.pallas_call(
        functools.partial(paired_kernel, n),
        out_shape=pltpu.VMEM((steps, rows, per_step), jnp.bfloat16),
        in_specs=[hbm] * 8,
        out_specs=vmem,
        scratch_shapes=[
            pltpu.VMEM((1, tokens), jnp.int32),
            pltpu.SMEM((heads,), jnp.float32),
            pltpu.SMEM(lengths.shape, jnp.int32),
            pltpu.VMEM((tokens, width), jnp.bfloat16),
            pltpu.VMEM((rows, width), jnp.bfloat16),
            pltpu.VMEM((rows, width), jnp.bfloat16),
            pltpu.VMEM((steps, frame_count, width), jnp.bfloat16),
            pltpu.VMEM((2 * width // part, width, part), jnp.bfloat16),
            pltpu.VMEM((pairs, keys, lanes), jnp.bfloat16),
            pltpu.VMEM((keys, lanes), jnp.bfloat16),
            pltpu.VMEM((pairs, lanes, keys), jnp.bfloat16),
            pltpu.VMEM((width, tokens), jnp.bfloat16),
            pltpu.VMEM((2, width, per_step), jnp.bfloat16),
            pltpu.VMEM((2, groups, 8, per_step), jnp.float32),
            pltpu.VMEM((width, per_step), jnp.bfloat16),
            pltpu.VMEM((groups, 8, per_step), jnp.float32),
            pltpu.VMEM((width, per_step), jnp.bfloat16),
            pltpu.VMEM((groups, chips, 2, per_step), jnp.float32),
            pltpu.VMEM((chips, 2 * width // chips, per_step), jnp.bfloat16),
            pltpu.VMEM((groups, chips, 2, per_step), jnp.float32),
            pltpu.VMEM((2, width, per_step), jnp.bfloat16),
            pltpu.SemaphoreType.DMA((6,)),
            pltpu.SemaphoreType.DMA((steps,)),
            pltpu.SemaphoreType.DMA((2 * width // part,)),
            pltpu.SemaphoreType.DMA((10,)),
            pltpu.SemaphoreType.DMA((chips,)),
            pltpu.SemaphoreType.DMA((2,)),
            pltpu.SemaphoreType.DMA((groups,)),
            pltpu.SemaphoreType.DMA((groups,)),
            pltpu.SemaphoreType.DMA((groups,)),
            pltpu.SemaphoreType.DMA((groups,)),
            pltpu.SemaphoreType.DMA((groups,)),
        ],
        compiler_params=pltpu.CompilerParams(
            collective_id=0, has_side_effects=True, vmem_limit_bytes=40 * 1024 * 1024
        ),
    )(
        *(
            pltpu.with_memory_space_constraint(value, pltpu.HBM)
            for value in (
                positions.reshape(1, tokens),
                head_slope,
                lengths,
                dec_states.reshape(tokens, width),
                w_query.T,
                w_output.T,
                frames,
                w_keyval,
            )
        )
    )
    return out.transpose(0, 2, 1)


def fits_pairs(n, frames, dec_states, w_query, head_slope):
    steps, frame_count, width = frames.shape
    per_step, heads = dec_states.shape[1], head_slope.shape[0]
    size = width // heads
    chips = n // 2
    return (
        steps == 2
        and n % 4 == 0
        and heads % 4 == 0
        and heads // 2 == sum(count for _, count in GROUPS)
        and n % 16 == 0
        and size == 64
        and per_step == 2 * size
        and frame_count % 128 == 0
        and w_query.shape[1] % 16 == 0
        and (2 * size) % (16 * chips) == 0
    )


def local(n, frames, dec_states, w_query, w_keyval, w_output, head_slope, lengths, positions):
    paired = fits_pairs(n, frames, dec_states, w_query, head_slope)
    run = paired_local if paired else plain_local
    return run(n, frames, dec_states, w_query, w_keyval, w_output, head_slope, lengths, positions)


def solution(mesh):
    return jax.shard_map(
        functools.partial(local, mesh.shape["seq"]),
        mesh=mesh,
        in_specs=(
            P("grp", "seq", None),
            P(None, "grp", None),
            P(None, "seq"),
            P(),
            P(None, "seq"),
            P(),
            P("grp", None),
            P(None, "grp"),
        ),
        out_specs=P(None, "grp", "seq"),
        check_vma=False,
    )
```
